256 devices in a mesh: cp: 32 (over x, y, core), tp: 8 (over z).
Axes of the slice: x: 4, y: 4, z: 8, core: 2. Of those that a mesh axis runs over, the one named last changes fastest.
Arguments:
- hidden: bfloat16 [16384, 4096], P('cp', 'tp'), may hold values from -9 to 9
- lengths: int32 [64], replicated, may hold values from 1 to 512, 16384 in all
- targets: int32 [64], replicated, may hold values from 0 to 128255
- norm_gain: float32 [4096], replicated, may hold values from 0.25 to 1.75
- lm_weight: bfloat16 [4096, 128256], P('cp', 'tp'), may hold values from -16 to 16, as said below
Outputs:
- target_logprob: float32 [64], replicated
The draws below stay inside these ranges and needn't reach their ends.
Inputs may be any that keep to these rules, and one draw needn't show every extreme that they name: `lm_weight`: most entries are of order 3 / sqrt(4096). The lengths sum to 16384, and one prompt has exactly 512 positions.
All inputs are finite; a program needn't handle non-finite values.
Results may differ from the reference program's by a relative error of at most 0.00058.
Values may be sent and summed in bfloat16 or wider, within the bound.
No kernel may reach another device: no remote copies, remote signals or barrier semaphores. Data moves between devices by JAX's collectives and lax.ppermute only.
A program may use at most 64 MiB of HBM per device.

```python
import math
import jax
import jax.numpy as jnp
import numpy as np
from jax import lax

D = 4096
VOCAB = 128256
B = 64
TOTAL = 16384
MOST = 512


def draw_hidden(key, part):
    sample = jax.random.normal(jax.random.fold_in(key, 31), (TOTAL, D), jnp.float32)
    sample = jnp.clip(sample, -6.0, 6.0)
    return sample.astype(jnp.bfloat16)


def draw_lm_weight(key, part):
    weights = jax.random.normal(jax.random.fold_in(key, 11), (D, VOCAB), jnp.float32) * (3.0 / math.sqrt(D))
    return jnp.clip(weights, -16.0, 16.0).astype(jnp.bfloat16)


def place_ends(values, key, low, largest):
    longest = values.shape.index(max(values.shape))
    spots = []
    for shift in (0, 1):
        where = [jax.random.randint(jax.random.fold_in(key, axis), (), 0, length) for axis, length in enumerate(values.shape)]
        where[longest] = (where[longest] + shift) % values.shape[longest]
        spots.append(tuple(where))
    return values.at[spots[0]].set(low).at[spots[1]].set(largest)


def length_profile(count, total, most, slope):
    weights = [(1 << 20) // math.isqrt(grade ** slope) + 1 for grade in range(2, count + 1)]
    spare, holding = total - most - (count - 1), [1] * (count - 1)
    while spare > 0:
        movable = [i for i in range(count - 1) if holding[i] < most]
        pool, remaining = sum([weights[i] for i in movable]), spare
        for i in movable:
            extra = min(most - holding[i], max(1, remaining * weights[i] // pool), spare)
            holding[i] = holding[i] + extra
            spare = spare - extra
    return np.array([most] + holding)


def ragged_sizes(key, number_of, total, bound, lean):
    if number_of == 2:
        one = jax.random.randint(key, (), max(1, total - bound), min(bound, total - 1) + 1)
        return jnp.stack([one, total - one])
    sizes = jnp.asarray(length_profile(number_of, total, bound, lean), jnp.int32)
    pairs = (number_of - 1) // 2
    donor, receiver = sizes[1:1 + 2 * pairs:2], sizes[2:2 + 2 * pairs:2]
    margin = jnp.minimum(donor - 1, bound - receiver)
    shifted = jax.random.randint(jax.random.fold_in(key, 1), (pairs,), 0, 1 << 20) % (margin + 1)
    sizes = sizes.at[1:1 + 2 * pairs:2].set(donor - shifted).at[2:2 + 2 * pairs:2].set(receiver + shifted)
    return sizes[jax.random.permutation(jax.random.fold_in(key, 2), number_of)]


def setup_inputs(seed: int = 0) -> dict:
    key_of = jax.random.split(jax.random.key(seed), 6)
    return {
        "hidden": draw_hidden(jax.random.fold_in(key_of[5], 71), 0),
        "lengths": ragged_sizes(key_of[1], B, TOTAL, MOST, 2).astype(jnp.int32),
        "targets": place_ends(jax.random.randint(key_of[2], (B,), 0, VOCAB), jax.random.fold_in(key_of[2], 1), 0, VOCAB - 1).astype(jnp.int32),
        "norm_gain": jnp.clip(1.0 + 0.15 * jax.random.normal(key_of[3], (D,), jnp.float32), 0.25, 1.75),
        "lm_weight": draw_lm_weight(jax.random.fold_in(key_of[5], 71), 0),
    }


def reference(hidden, lengths, targets, norm_gain, lm_weight):
    ends = (jnp.cumsum(lengths) - 1).astype(jnp.int32)
    last_rows = jnp.take(hidden, ends, axis=0).astype(jnp.float32)
    mean_sq = lax.optimization_barrier(jnp.mean(last_rows * last_rows, axis=1, keepdims=True))
    normed = (last_rows * norm_gain[None, :] / jnp.sqrt(mean_sq + 1e-05)).astype(jnp.bfloat16)
    logits = jnp.dot(normed, lm_weight, preferred_element_type=jnp.float32)
    top = lax.optimization_barrier(jnp.max(logits, axis=1))
    total = lax.optimization_barrier(jnp.sum(jnp.exp(logits - top[:, None]), axis=1))
    picked = jnp.take_along_axis(logits, targets[:, None].astype(jnp.int32), axis=1)[:, 0]
    return picked - top - jnp.log(total)
```

```python
import functools

import jax
import jax.numpy as jnp
from jax import lax
from jax.experimental import pallas as pl
from jax.experimental.pallas import tpu as pltpu
from jax.sharding import Mesh
from jax.sharding import PartitionSpec as P

CHIPS = ("x", "y")
CP = ("x", "y", "c")
ALL = ("x", "y", "c", "z")
SLOTS = 8
BLOCK = 512
NEG = -1e30

VMEM = pl.BlockSpec(memory_space=pltpu.VMEM)
SMEM = pl.BlockSpec(memory_space=pltpu.SMEM)
ANY = pl.BlockSpec(memory_space=pl.ANY)


def iota(shape, dim):
    return lax.broadcasted_iota(jnp.int32, shape, dim).astype(jnp.float32)


def total(x, axis):
    return jnp.sum(x, axis=axis, keepdims=True)


def place():
    return (lax.axis_index("x") * lax.axis_size("y") + lax.axis_index("y")) * lax.axis_size(
        "c"
    ) + lax.axis_index("c")


def as_column(row):
    n = row.shape[1]
    return total(jnp.where(iota((n, n), 0) == iota((n, n), 1), row, 0.0), 1)


def ends_of(lengths_ref):
    row = lengths_ref[...].astype(jnp.float32)
    n = row.shape[1]
    down, across = iota((n, n), 0), iota((n, n), 1)
    column = total(jnp.where(across <= down, row, 0.0), 1) - 1.0
    return total(jnp.where(down <= across, as_column(row), 0.0), 0) - 1.0, column


def pick_kernel(lengths_ref, first_ref, hidden_ref, out_ref, most_ref):
    n = lengths_ref.shape[1]
    rows = hidden_ref.shape[0]
    ends, _ = ends_of(lengths_ref)
    base = (place() * rows).astype(jnp.float32)
    owned = (ends >= base) & (ends < base + rows)
    before = total(jnp.where(ends < base, 1.0, 0.0), 1)
    slot = iota((1, n), 1) - before - first_ref[0, 0].astype(jnp.float32)
    wanted = owned & (slot == iota((SLOTS, n), 0))
    at = total(jnp.where(wanted, ends - base + 1.0, 0.0), 1) - 1.0
    selector = (at == iota((SLOTS, rows), 1)).astype(jnp.bfloat16)
    picked = jnp.dot(selector, hidden_ref[...], preferred_element_type=jnp.float32)
    picked = picked.astype(jnp.bfloat16)
    for peer in range(out_ref.shape[0]):
        out_ref[peer] = picked
    owners = iota((32, n), 0)
    counts = total(jnp.where(jnp.floor(ends / rows) == owners, 1.0, 0.0), 1)
    most_ref[0, 0] = jnp.max(counts).astype(jnp.int32)


def norm_kernel(rows_ref, gain_ref, out_ref):
    parts, _, width = rows_ref.shape
    squares = jnp.zeros((SLOTS, 1), jnp.float32)
    for part in range(parts):
        values = rows_ref[part].astype(jnp.float32)
        squares = squares + total(values * values, 1)
    scale = jnp.sqrt(squares / (parts * width) + 1e-05)
    chips, cores, _, block = out_ref.shape
    for chip in range(chips):
        part, at = divmod(chip * block, width)
        values = rows_ref[part, :, at : at + block].astype(jnp.float32)
        gain = gain_ref[:, chip * block : (chip + 1) * block]
        normed = (values * gain / scale).astype(jnp.bfloat16)
        for core in range(cores):
            out_ref[chip, core] = normed


def rows_in_order(lengths_ref, first_ref, found_ref):
    n = lengths_ref.shape[1]
    places = found_ref.shape[0]
    rows = 512
    ends_row, ends = ends_of(lengths_ref)
    owner = jnp.floor(ends / rows)
    before = total(jnp.where(ends_row < owner * rows, 1.0, 0.0), 1)
    slot = iota((n, 1), 0) - before - first_ref[0, 0].astype(jnp.float32)
    inside = (slot >= 0.0) & (slot < SLOTS)
    at = jnp.where(inside, owner * SLOTS + slot, -1.0)
    selector = (at == iota((n, places), 1)).astype(jnp.bfloat16)
    return jnp.dot(selector, found_ref[...], preferred_element_type=jnp.float32)


def order_kernel(lengths_ref, first_ref, found_ref, more_ref, out_ref):
    rows = rows_in_order(lengths_ref, first_ref, found_ref)
    out_ref[...] = more_ref[...] + rows.astype(jnp.bfloat16)


def split_kernel(weight_ref, keep_ref, send_ref, sems):
    core = lax.axis_index("c")
    half = keep_ref.shape[0]
    spare = weight_ref.shape[0] - half
    copies = [
        pltpu.make_async_copy(
            weight_ref.at[pl.ds(pl.multiple_of(which * spare, 16), half)], ref, sems.at[k]
        )
        for k, (which, ref) in enumerate(((1 - core, send_ref), (core, keep_ref)))
    ]
    for copy in copies:
        copy.start()
    for copy in copies:
        copy.wait()


def head_kernel(lengths_ref, first_ref, found_ref, more_ref, keep_ref, other_ref, out_ref):
    rows = rows_in_order(lengths_ref, first_ref, found_ref).astype(jnp.bfloat16) + more_ref[...]
    width = keep_ref.shape[1]
    low, high = rows[:, :width], rows[:, width:]
    first = lax.axis_index("c") == 0
    left = jnp.concatenate([jnp.where(first, low, high), jnp.where(first, high, low)], axis=1)
    for block in range(out_ref.shape[0]):
        span = slice(block * BLOCK, (block + 1) * BLOCK)
        weight = jnp.concatenate([keep_ref[span, :], other_ref[span, :]], axis=1)
        part = lax.dot_general(
            left, weight, (((1,), (1,)), ((), ())), preferred_element_type=jnp.float32
        )
        out_ref[block] = part.astype(out_ref.dtype)


def stats_kernel(spare, vocab, logits_ref, targets_ref, out_ref):
    logits = logits_ref[...]
    n, block = logits.shape
    core = lax.axis_index("c")
    chip = lax.axis_index("x") * lax.axis_size("y") + lax.axis_index("y")
    start = (core * spare + chip * block).astype(jnp.float32)
    column = iota((1, block), 1) + start
    half = vocab - spare
    valid = column >= (core * half).astype(jnp.float32)
    shift = (lax.axis_index("z") * vocab).astype(jnp.float32)
    wanted = as_column(targets_ref[...].astype(jnp.float32)) - shift
    found = total(jnp.where(valid & (column == wanted), logits, 0.0), 1)
    logits = jnp.where(valid, logits, NEG)
    top = jnp.max(logits, axis=1, keepdims=True)
    both = top + jnp.log(total(jnp.exp(logits - top), 1))
    down, across = iota((n, 2 * n), 0), iota((n, 2 * n), 1)
    line = jnp.where(across == down, both, 0.0) + jnp.where(across == down + n, found, 0.0)
    out_ref[...] = jnp.broadcast_to(total(line, 0)[None], out_ref.shape)


def join_kernel(found_ref, out_ref):
    n = out_ref.shape[1]
    lines = found_ref[:, 0, :]
    top = jnp.max(lines, axis=0, keepdims=True)
    both = top + jnp.log(total(jnp.exp(lines - top), 0))
    chosen = total(lines, 0)
    out_ref[...] = chosen[:, n:] - both[:, :n]


def shape(dims, dtype):
    return jax.ShapeDtypeStruct(dims, dtype)


def exchange(x, axes):
    return lax.all_to_all(x, axes, split_axis=0, concat_axis=0, tiled=True)


def gathered(lengths, first, hidden, gain):
    peers = lax.axis_size("z")
    chips, cores = lax.axis_size(CHIPS), lax.axis_size("c")
    rows, most = pl.pallas_call(
        pick_kernel,
        out_shape=(shape((peers, SLOTS, hidden.shape[1]), hidden.dtype), shape((1, 1), jnp.int32)),
        in_specs=[VMEM, SMEM, VMEM],
        out_specs=(VMEM, SMEM),
        name="pick",
    )(lengths, first, hidden)
    rows = exchange(rows, "z")
    width = gain.shape[1] // chips
    normed = pl.pallas_call(
        norm_kernel,
        out_shape=shape((chips, cores, SLOTS, width), jnp.bfloat16),
        in_specs=[VMEM, VMEM],
        out_specs=VMEM,
        name="norm",
    )(rows, gain)
    return exchange(normed.reshape(chips * cores * SLOTS, width), CP), most


def local(hidden, lengths, targets, norm_gain, lm_weight):
    n = lengths.shape[0]
    lengths, targets, gain = lengths[None], targets[None], norm_gain[None]
    weight = lm_weight.T
    vocab, depth = weight.shape
    chips = lax.axis_size(CHIPS)
    half = chips * BLOCK
    start = jnp.zeros((1, 1), jnp.int32)
    found, most = gathered(lengths, start, hidden, gain)

    def again(state):
        first, more = state
        found, _ = gathered(lengths, first, hidden, gain)
        more = pl.pallas_call(
            order_kernel,
            out_shape=shape(more.shape, more.dtype),
            in_specs=[VMEM, SMEM, VMEM, VMEM],
            out_specs=VMEM,
            name="order",
        )(lengths, first, found, more)
        return first + SLOTS, more

    _, more = lax.while_loop(
        lambda state: state[0][0, 0] < most[0, 0],
        again,
        (start + SLOTS, jnp.zeros((n, found.shape[1]), jnp.bfloat16)),
    )
    keep, send = pl.pallas_call(
        split_kernel,
        out_shape=(shape((half, depth), weight.dtype),) * 2,
        in_specs=[ANY],
        out_specs=(VMEM, VMEM),
        scratch_shapes=[pltpu.SemaphoreType.DMA((2,))],
        name="split",
    )(weight)
    other = lax.ppermute(send, "c", [(0, 1), (1, 0)])
    parts = pl.pallas_call(
        head_kernel,
        out_shape=shape((chips, n, BLOCK), jnp.float32),
        in_specs=[VMEM, SMEM, VMEM, VMEM, VMEM, VMEM],
        out_specs=VMEM,
        name="head",
    )(lengths, start, found, more, keep, other)
    logits = jnp.sum(exchange(parts.astype(jnp.float16), CHIPS).astype(jnp.float32), axis=0)
    line = pl.pallas_call(
        functools.partial(stats_kernel, vocab - half, vocab),
        out_shape=shape((lax.axis_size(ALL), 1, 2 * n), jnp.float32),
        in_specs=[VMEM, VMEM],
        out_specs=VMEM,
        name="stats",
    )(logits, targets)
    lines = exchange(line, ALL)
    out = pl.pallas_call(
        join_kernel,
        out_shape=shape((1, n), jnp.float32),
        in_specs=[VMEM],
        out_specs=VMEM,
        name="join",
    )(lines)
    return out[0]


def solution(mesh):
    split = Mesh(mesh.devices.reshape(4, 4, 2, mesh.shape["tp"]), ALL)
    return jax.shard_map(
        local,
        mesh=split,
        in_specs=(P(CP, "z"), P(), P(), P(), P(CP, "z")),
        out_specs=P(),
        check_vma=False,
    )
```

```python
import functools

import jax
import jax.numpy as jnp
from jax import lax
from jax.experimental import pallas as pl
from jax.experimental.pallas import tpu as pltpu
from jax.sharding import Mesh
from jax.sharding import PartitionSpec as P


CHIPS = ("x", "y")
CP = ("x", "y", "c")
ALL = ("x", "y", "c", "z")
SLOTS = 8
BLOCK = 512
NEG = -1e30

VMEM = pl.BlockSpec(memory_space=pltpu.VMEM)
SMEM = pl.BlockSpec(memory_space=pltpu.SMEM)
ANY = pl.BlockSpec(memory_space=pl.ANY)
MIB = 1 << 20


def limit(mib):
    return pltpu.CompilerParams(vmem_limit_bytes=mib * MIB)


def iota(shape, dim):
    return lax.broadcasted_iota(jnp.int32, shape, dim).astype(jnp.float32)


def total(x, axis):
    return jnp.sum(x, axis=axis, keepdims=True)


def place():
    return (lax.axis_index("x") * lax.axis_size("y") + lax.axis_index("y")) * lax.axis_size(
        "c"
    ) + lax.axis_index("c")


def as_column(row):
    n = row.shape[1]
    return total(jnp.where(iota((n, n), 0) == iota((n, n), 1), row, 0.0), 1)


def ends_of(lengths_ref):
    row = lengths_ref[...].astype(jnp.float32)
    n = row.shape[1]
    down, across = iota((n, n), 0), iota((n, n), 1)
    column = total(jnp.where(across <= down, row, 0.0), 1) - 1.0
    return total(jnp.where(down <= across, as_column(row), 0.0), 0) - 1.0, column


def pick_kernel(lengths_ref, first_ref, hidden_ref, out_ref, most_ref):
    n = lengths_ref.shape[1]
    rows = hidden_ref.shape[0]
    ends, _ = ends_of(lengths_ref)
    base = (place() * rows).astype(jnp.float32)
    owned = (ends >= base) & (ends < base + rows)
    before = total(jnp.where(ends < base, 1.0, 0.0), 1)
    slot = iota((1, n), 1) - before - first_ref[0, 0].astype(jnp.float32)
    wanted = owned & (slot == iota((SLOTS, n), 0))
    at = total(jnp.where(wanted, ends - base + 1.0, 0.0), 1) - 1.0
    selector = (at == iota((SLOTS, rows), 1)).astype(jnp.bfloat16)
    picked = jnp.dot(selector, hidden_ref[...], preferred_element_type=jnp.float32)
    picked = picked.astype(jnp.bfloat16)
    for peer in range(out_ref.shape[0]):
        out_ref[peer] = picked
    owners = iota((32, n), 0)
    counts = total(jnp.where(jnp.floor(ends / rows) == owners, 1.0, 0.0), 1)
    most_ref[0, 0] = jnp.max(counts).astype(jnp.int32)


def norm_kernel(rows_ref, gain_ref, out_ref):
    parts, _, width = rows_ref.shape
    squares = jnp.zeros((SLOTS, 1), jnp.float32)
    for part in range(parts):
        values = rows_ref[part].astype(jnp.float32)
        squares = squares + total(values * values, 1)
    scale = jnp.sqrt(squares / (parts * width) + 1e-05)
    chips, cores, _, block = out_ref.shape
    for chip in range(chips):
        part, at = divmod(chip * block, width)
        values = rows_ref[part, :, at : at + block].astype(jnp.float32)
        gain = gain_ref[:, chip * block : (chip + 1) * block]
        normed = (values * gain / scale).astype(jnp.bfloat16)
        for core in range(cores):
            out_ref[chip, core] = normed


def rows_in_order(lengths_ref, first_ref, found_ref):
    n = lengths_ref.shape[1]
    places = found_ref.shape[0]
    rows = 512
    ends_row, ends = ends_of(lengths_ref)
    owner = jnp.floor(ends / rows)
    before = total(jnp.where(ends_row < owner * rows, 1.0, 0.0), 1)
    slot = iota((n, 1), 0) - before - first_ref[0, 0].astype(jnp.float32)
    inside = (slot >= 0.0) & (slot < SLOTS)
    at = jnp.where(inside, owner * SLOTS + slot, -1.0)
    selector = (at == iota((n, places), 1)).astype(jnp.bfloat16)
    return jnp.dot(selector, found_ref[...], preferred_element_type=jnp.float32)


def order_kernel(lengths_ref, first_ref, found_ref, more_ref, out_ref):
    rows = rows_in_order(lengths_ref, first_ref, found_ref)
    out_ref[...] = more_ref[...] + rows.astype(jnp.bfloat16)


def split_kernel(weight_ref, send_ref, sem):
    half = send_ref.shape[0]
    start = (1 - lax.axis_index("c")) * (weight_ref.shape[0] - half)
    copy = pltpu.make_async_copy(
        weight_ref.at[pl.ds(pl.multiple_of(start, 16), half)], send_ref, sem
    )
    copy.start()
    copy.wait()


def head_kernel(lengths_ref, first_ref, found_ref, more_ref, weight_ref, other_ref, out_ref):
    rows = rows_in_order(lengths_ref, first_ref, found_ref).astype(jnp.bfloat16) + more_ref[...]
    width = other_ref.shape[1]
    start = lax.axis_index("c") * (weight_ref.shape[0] - other_ref.shape[0])
    low, high = rows[:, :width], rows[:, width:]
    first = lax.axis_index("c") == 0
    left = jnp.concatenate([jnp.where(first, low, high), jnp.where(first, high, low)], axis=1)
    for block in range(out_ref.shape[0]):
        own = weight_ref[pl.ds(pl.multiple_of(start + block * BLOCK, 16), BLOCK), :]
        other = other_ref[block * BLOCK : (block + 1) * BLOCK, :]
        weight = jnp.concatenate([own, other], axis=1)
        part = lax.dot_general(
            left, weight, (((1,), (1,)), ((), ())), preferred_element_type=jnp.float32
        )
        out_ref[block] = part.astype(out_ref.dtype)


def stats_kernel(spare, vocab, logits_ref, targets_ref, out_ref):
    logits = logits_ref[...]
    n, block = logits.shape
    core = lax.axis_index("c")
    chip = lax.axis_index("x") * lax.axis_size("y") + lax.axis_index("y")
    start = (core * spare + chip * block).astype(jnp.float32)
    column = iota((1, block), 1) + start
    half = vocab - spare
    valid = column >= (core * half).astype(jnp.float32)
    shift = (lax.axis_index("z") * vocab).astype(jnp.float32)
    wanted = as_column(targets_ref[...].astype(jnp.float32)) - shift
    found = total(jnp.where(valid & (column == wanted), logits, 0.0), 1)
    logits = jnp.where(valid, logits, NEG)
    top = jnp.max(logits, axis=1, keepdims=True)
    both = top + jnp.log(total(jnp.exp(logits - top), 1))
    down, across = iota((n, 2 * n), 0), iota((n, 2 * n), 1)
    line = jnp.where(across == down, both, 0.0) + jnp.where(across == down + n, found, 0.0)
    out_ref[...] = jnp.broadcast_to(total(line, 0)[None], out_ref.shape)


def join_kernel(found_ref, out_ref):
    n = out_ref.shape[1]
    lines = found_ref[:, 0, :]
    top = jnp.max(lines, axis=0, keepdims=True)
    both = top + jnp.log(total(jnp.exp(lines - top), 0))
    chosen = total(lines, 0)
    out_ref[...] = chosen[:, n:] - both[:, :n]


def shape(dims, dtype):
    return jax.ShapeDtypeStruct(dims, dtype)


def exchange(x, axes):
    return lax.all_to_all(x, axes, split_axis=0, concat_axis=0, tiled=True)


def picked(lengths, first, hidden):
    return pl.pallas_call(
        pick_kernel,
        out_shape=(
            shape((lax.axis_size("z"), SLOTS, hidden.shape[1]), hidden.dtype),
            shape((1, 1), jnp.int32),
        ),
        in_specs=[VMEM, SMEM, VMEM],
        out_specs=(VMEM, SMEM),
        compiler_params=limit(4),
        name="pick",
    )(lengths, first, hidden)


def spread(rows, gain):
    chips, cores = lax.axis_size(CHIPS), lax.axis_size("c")
    width = gain.shape[1] // chips
    rows = exchange(rows, "z")
    normed = pl.pallas_call(
        norm_kernel,
        out_shape=shape((chips, cores, SLOTS, width), jnp.bfloat16),
        in_specs=[VMEM, VMEM],
        out_specs=VMEM,
        compiler_params=limit(4),
        name="norm",
    )(rows, gain)
    return exchange(normed.reshape(chips * cores * SLOTS, width), CP)


def local(hidden, lengths, targets, norm_gain, lm_weight):
    n = lengths.shape[0]
    lengths, targets, gain = lengths[None], targets[None], norm_gain[None]
    weight = lm_weight.T
    vocab, depth = weight.shape
    chips = lax.axis_size(CHIPS)
    half = chips * BLOCK
    start = jnp.zeros((1, 1), jnp.int32)
    rows, most = picked(lengths, start, hidden)

    def again(state):
        first, more = state
        found = spread(picked(lengths, first, hidden)[0], gain)
        more = pl.pallas_call(
            order_kernel,
            out_shape=shape(more.shape, more.dtype),
            in_specs=[VMEM, SMEM, VMEM, VMEM],
            out_specs=VMEM,
            compiler_params=limit(4),
            name="order",
        )(lengths, first, found, more)
        return first + SLOTS, more

    _, more = lax.while_loop(
        lambda state: state[0][0, 0] < most[0, 0],
        again,
        (start + SLOTS, jnp.zeros((n, gain.shape[1] // chips), jnp.bfloat16)),
    )
    rows, weight, more = lax.optimization_barrier((rows, weight, more))
    found = spread(rows, gain)
    send = pl.pallas_call(
        split_kernel,
        out_shape=pltpu.VMEM((half, depth), weight.dtype),
        in_specs=[ANY],
        out_specs=VMEM,
        scratch_shapes=[pltpu.SemaphoreType.DMA(())],
        cost_estimate=pl.CostEstimate(flops=10**9, bytes_accessed=4 * MIB, transcendentals=0),
        compiler_params=limit(8),
        name="split",
    )(pltpu.with_memory_space_constraint(weight, pltpu.HBM))
    other = lax.ppermute(send, "c", [(0, 1), (1, 0)])
    parts = pl.pallas_call(
        head_kernel,
        out_shape=shape((chips, n, BLOCK), jnp.float32),
        in_specs=[VMEM, SMEM, VMEM, VMEM, VMEM, VMEM],
        out_specs=VMEM,
        compiler_params=limit(16),
        name="head",
    )(lengths, start, found, more, weight, other)
    logits = jnp.sum(exchange(parts.astype(jnp.float16), CHIPS).astype(jnp.float32), axis=0)
    line = pl.pallas_call(
        functools.partial(stats_kernel, vocab - half, vocab),
        out_shape=shape((lax.axis_size(ALL), 1, 2 * n), jnp.float32),
        in_specs=[VMEM, VMEM],
        out_specs=VMEM,
        compiler_params=limit(4),
        name="stats",
    )(logits, targets)
    lines = exchange(line, ALL)
    out = pl.pallas_call(
        join_kernel,
        out_shape=shape((1, n), jnp.float32),
        in_specs=[VMEM],
        out_specs=VMEM,
        compiler_params=limit(4),
        name="join",
    )(lines)
    return out[0]


def solution(mesh):
    split = Mesh(mesh.devices.reshape(4, 4, 2, mesh.shape["tp"]), ALL)
    return jax.shard_map(
        local,
        mesh=split,
        in_specs=(P(CP, "z"), P(), P(), P(), P(CP, "z")),
        out_specs=P(),
        check_vma=False,
    )
```

```python
import functools

import jax
import jax.numpy as jnp
from jax import lax
from jax.experimental import pallas as pl
from jax.experimental.pallas import tpu as pltpu
from jax.sharding import Mesh
from jax.sharding import PartitionSpec as P


CHIPS = ("x", "y")
CP = ("x", "y", "c")
ALL = ("x", "y", "c", "z")
SLOTS = 8
BLOCK = 512
NEG = -1e30

VMEM = pl.BlockSpec(memory_space=pltpu.VMEM)
SMEM = pl.BlockSpec(memory_space=pltpu.SMEM)
HBM = pl.BlockSpec(memory_space=pltpu.HBM)
MIB = 1 << 20


def limit(mib):
    return pltpu.CompilerParams(vmem_limit_bytes=mib * MIB)


def iota(shape, dim):
    return lax.broadcasted_iota(jnp.int32, shape, dim).astype(jnp.float32)


def total(x, axis):
    return jnp.sum(x, axis=axis, keepdims=True)


def place():
    return (lax.axis_index("x") * lax.axis_size("y") + lax.axis_index("y")) * lax.axis_size(
        "c"
    ) + lax.axis_index("c")


def as_column(row):
    n = row.shape[1]
    return total(jnp.where(iota((n, n), 0) == iota((n, n), 1), row, 0.0), 1)


def ends_of(lengths_ref):
    row = lengths_ref[...].astype(jnp.float32)
    n = row.shape[1]
    down, across = iota((n, n), 0), iota((n, n), 1)
    column = total(jnp.where(across <= down, row, 0.0), 1) - 1.0
    return total(jnp.where(down <= across, as_column(row), 0.0), 0) - 1.0, column


def pick_kernel(lengths_ref, first_ref, hidden_ref, out_ref, most_ref):
    n = lengths_ref.shape[1]
    rows = hidden_ref.shape[0]
    ends, _ = ends_of(lengths_ref)
    base = (place() * rows).astype(jnp.float32)
    owned = (ends >= base) & (ends < base + rows)
    before = total(jnp.where(ends < base, 1.0, 0.0), 1)
    slot = iota((1, n), 1) - before - first_ref[0, 0].astype(jnp.float32)
    wanted = owned & (slot == iota((SLOTS, n), 0))
    at = total(jnp.where(wanted, ends - base + 1.0, 0.0), 1) - 1.0
    selector = (at == iota((SLOTS, rows), 1)).astype(jnp.bfloat16)
    owners = iota((32, n), 0)
    counts = total(jnp.where(jnp.floor(ends / rows) == owners, 1.0, 0.0), 1)
    most_ref[0, 0] = jnp.max(counts).astype(jnp.int32)
    picked = jnp.dot(selector, hidden_ref[...], preferred_element_type=jnp.float32)
    picked = picked.astype(jnp.bfloat16)
    for peer in range(out_ref.shape[0]):
        out_ref[peer] = picked


def half_of(weight_ref, half, core):
    start = core * (weight_ref.shape[0] - half)
    return weight_ref.at[pl.ds(pl.multiple_of(start, 16), half)]


def begin_kernel(
    lengths_ref, first_ref, hidden_ref, weight_ref, out_ref, most_ref, send_ref, held, sems
):
    source = half_of(weight_ref, send_ref.shape[0], 1 - lax.axis_index("c"))
    rows = pltpu.make_async_copy(hidden_ref, held, sems.at[0])
    swap = pltpu.make_async_copy(source, send_ref, sems.at[1])
    rows.start()
    swap.start()
    rows.wait()
    pick_kernel(lengths_ref, first_ref, held, out_ref, most_ref)
    swap.wait()


def norm_kernel(rows_ref, gain_ref, out_ref):
    parts, _, width = rows_ref.shape
    squares = jnp.zeros((SLOTS, 1), jnp.float32)
    for part in range(parts):
        values = rows_ref[part].astype(jnp.float32)
        squares = squares + total(values * values, 1)
    scale = jnp.sqrt(squares / (parts * width) + 1e-05)
    chips, cores, _, block = out_ref.shape
    for chip in range(chips):
        part, at = divmod(chip * block, width)
        values = rows_ref[part, :, at : at + block].astype(jnp.float32)
        gain = gain_ref[:, chip * block : (chip + 1) * block]
        normed = (values * gain / scale).astype(jnp.bfloat16)
        for core in range(cores):
            out_ref[chip, core] = normed


def rows_in_order(lengths_ref, first_ref, found_ref):
    n = lengths_ref.shape[1]
    places = found_ref.shape[0]
    rows = 512
    ends_row, ends = ends_of(lengths_ref)
    owner = jnp.floor(ends / rows)
    before = total(jnp.where(ends_row < owner * rows, 1.0, 0.0), 1)
    slot = iota((n, 1), 0) - before - first_ref[0, 0].astype(jnp.float32)
    inside = (slot >= 0.0) & (slot < SLOTS)
    at = jnp.where(inside, owner * SLOTS + slot, -1.0)
    selector = (at == iota((n, places), 1)).astype(jnp.bfloat16)
    return jnp.dot(selector, found_ref[...], preferred_element_type=jnp.float32)


def order_kernel(lengths_ref, first_ref, found_ref, more_ref, out_ref):
    rows = rows_in_order(lengths_ref, first_ref, found_ref)
    out_ref[...] = more_ref[...] + rows.astype(jnp.bfloat16)


def keep_kernel(weight_ref, keep_ref, sem):
    copy = pltpu.make_async_copy(
        half_of(weight_ref, keep_ref.shape[0], lax.axis_index("c")), keep_ref, sem
    )
    copy.start()
    copy.wait()


def head_kernel(lengths_ref, first_ref, found_ref, more_ref, keep_ref, other_ref, out_ref):
    rows = rows_in_order(lengths_ref, first_ref, found_ref).astype(jnp.bfloat16) + more_ref[...]
    width = keep_ref.shape[1]
    low, high = rows[:, :width], rows[:, width:]
    first = lax.axis_index("c") == 0
    left = jnp.concatenate([jnp.where(first, low, high), jnp.where(first, high, low)], axis=1)
    for block in range(out_ref.shape[0]):
        span = slice(block * BLOCK, (block + 1) * BLOCK)
        weight = jnp.concatenate([keep_ref[span, :], other_ref[span, :]], axis=1)
        part = lax.dot_general(
            left, weight, (((1,), (1,)), ((), ())), preferred_element_type=jnp.float32
        )
        out_ref[block] = part.astype(out_ref.dtype)


def stats_kernel(spare, vocab, logits_ref, targets_ref, out_ref):
    logits = logits_ref[...]
    n, block = logits.shape
    core = lax.axis_index("c")
    chip = lax.axis_index("x") * lax.axis_size("y") + lax.axis_index("y")
    start = (core * spare + chip * block).astype(jnp.float32)
    column = iota((1, block), 1) + start
    half = vocab - spare
    valid = column >= (core * half).astype(jnp.float32)
    shift = (lax.axis_index("z") * vocab).astype(jnp.float32)
    wanted = as_column(targets_ref[...].astype(jnp.float32)) - shift
    found = total(jnp.where(valid & (column == wanted), logits, 0.0), 1)
    logits = jnp.where(valid, logits, NEG)
    top = jnp.max(logits, axis=1, keepdims=True)
    both = top + jnp.log(total(jnp.exp(logits - top), 1))
    down, across = iota((n, 2 * n), 0), iota((n, 2 * n), 1)
    line = jnp.where(across == down, both, 0.0) + jnp.where(across == down + n, found, 0.0)
    out_ref[...] = jnp.broadcast_to(total(line, 0), out_ref.shape)


def join_kernel(found_ref, out_ref):
    n = out_ref.shape[1]
    lines = found_ref[...]
    top = jnp.max(lines, axis=0, keepdims=True)
    both = top + jnp.log(total(jnp.exp(lines - top), 0))
    chosen = total(lines, 0)
    out_ref[...] = chosen[:, n:] - both[:, :n]


def shape(dims, dtype):
    return jax.ShapeDtypeStruct(dims, dtype)


def in_hbm(x):
    return pltpu.with_memory_space_constraint(x, pltpu.HBM)


def exchange(x, axes):
    return lax.all_to_all(x, axes, split_axis=0, concat_axis=0, tiled=True)


def picked(lengths, first, hidden):
    return pl.pallas_call(
        pick_kernel,
        out_shape=(
            shape((lax.axis_size("z"), SLOTS, hidden.shape[1]), hidden.dtype),
            shape((1, 1), jnp.int32),
        ),
        in_specs=[VMEM, SMEM, VMEM],
        out_specs=(VMEM, SMEM),
        compiler_params=limit(4),
        name="pick",
    )(lengths, first, hidden)


def spread(rows, gain):
    chips, cores = lax.axis_size(CHIPS), lax.axis_size("c")
    width = gain.shape[1] // chips
    rows = exchange(rows, "z")
    normed = pl.pallas_call(
        norm_kernel,
        out_shape=shape((chips, cores, SLOTS, width), jnp.bfloat16),
        in_specs=[VMEM, VMEM],
        out_specs=VMEM,
        compiler_params=limit(4),
        name="norm",
    )(rows, gain)
    return exchange(normed.reshape(chips * cores * SLOTS, width), CP)


def local(hidden, lengths, targets, norm_gain, lm_weight):
    n = lengths.shape[0]
    lengths, targets, gain = lengths[None], targets[None], norm_gain[None]
    weight = lm_weight.T
    vocab, depth = weight.shape
    chips = lax.axis_size(CHIPS)
    half = chips * BLOCK
    start = jnp.zeros((1, 1), jnp.int32)
    rows, most, send = pl.pallas_call(
        begin_kernel,
        out_shape=(
            pltpu.VMEM((lax.axis_size("z"), SLOTS, hidden.shape[1]), hidden.dtype),
            shape((1, 1), jnp.int32),
            pltpu.VMEM((half, depth), weight.dtype),
        ),
        in_specs=[VMEM, SMEM, HBM, HBM],
        out_specs=(VMEM, SMEM, VMEM),
        scratch_shapes=[pltpu.VMEM(hidden.shape, hidden.dtype), pltpu.SemaphoreType.DMA((2,))],
        compiler_params=limit(8),
        name="begin",
    )(lengths, start, in_hbm(hidden), in_hbm(weight))
    other = lax.ppermute(send, "c", [(0, 1), (1, 0)])

    def again(state):
        first, more = state
        found = spread(picked(lengths, first, hidden)[0], gain)
        more = pl.pallas_call(
            order_kernel,
            out_shape=shape(more.shape, more.dtype),
            in_specs=[VMEM, SMEM, VMEM, VMEM],
            out_specs=VMEM,
            compiler_params=limit(4),
            name="order",
        )(lengths, first, found, more)
        return first + SLOTS, more

    _, more = lax.while_loop(
        lambda state: state[0][0, 0] < most[0, 0],
        again,
        (start + SLOTS, jnp.zeros((n, gain.shape[1] // chips), jnp.bfloat16)),
    )
    rows, weight, more = lax.optimization_barrier((rows, weight, more))
    found = spread(rows, gain)
    keep = pl.pallas_call(
        keep_kernel,
        out_shape=pltpu.VMEM((half, depth), weight.dtype),
        in_specs=[HBM],
        out_specs=VMEM,
        scratch_shapes=[pltpu.SemaphoreType.DMA(())],
        compiler_params=limit(8),
        name="half",
    )(in_hbm(weight))
    parts = pl.pallas_call(
        head_kernel,
        out_shape=shape((chips, n, BLOCK), jnp.float32),
        in_specs=[VMEM, SMEM, VMEM, VMEM, VMEM, VMEM],
        out_specs=VMEM,
        compiler_params=limit(16),
        name="head",
    )(lengths, start, found, more, keep, other)
    logits = jnp.sum(exchange(parts.astype(jnp.float16), CHIPS).astype(jnp.float32), axis=0)
    line = pl.pallas_call(
        functools.partial(stats_kernel, vocab - half, vocab),
        out_shape=shape((lax.axis_size(ALL), 2 * n), jnp.float32),
        in_specs=[VMEM, VMEM],
        out_specs=VMEM,
        compiler_params=limit(4),
        name="stats",
    )(logits, targets)
    lines = exchange(line, ALL)
    out = pl.pallas_call(
        join_kernel,
        out_shape=shape((1, n), jnp.float32),
        in_specs=[VMEM],
        out_specs=VMEM,
        compiler_params=limit(4),
        name="join",
    )(lines)
    return out[0]


def solution(mesh):
    split = Mesh(mesh.devices.reshape(4, 4, 2, mesh.shape["tp"]), ALL)
    return jax.shard_map(
        local,
        mesh=split,
        in_specs=(P(CP, "z"), P(), P(), P(), P(CP, "z")),
        out_specs=P(),
        check_vma=False,
    )
```

```python
import functools

import jax
import jax.numpy as jnp
from jax import lax
from jax.experimental import pallas as pl
from jax.experimental.pallas import tpu as pltpu
from jax.sharding import Mesh
from jax.sharding import PartitionSpec as P


CHIPS = ("x", "y")
CP = ("x", "y", "c")
ALL = ("x", "y", "c", "z")
SLOTS = 8
BLOCK = 512
PIECES = 8
NEG = -1e30

VMEM = pl.BlockSpec(memory_space=pltpu.VMEM)
SMEM = pl.BlockSpec(memory_space=pltpu.SMEM)
HBM = pl.BlockSpec(memory_space=pltpu.HBM)
MIB = 1 << 20


def limit(mib):
    return pltpu.CompilerParams(vmem_limit_bytes=mib * MIB)


def iota(shape, dim):
    return lax.broadcasted_iota(jnp.int32, shape, dim).astype(jnp.float32)


def total(x, axis):
    return jnp.sum(x, axis=axis, keepdims=True)


def place():
    return (lax.axis_index("x") * lax.axis_size("y") + lax.axis_index("y")) * lax.axis_size(
        "c"
    ) + lax.axis_index("c")


def as_column(row):
    n = row.shape[1]
    return total(jnp.where(iota((n, n), 0) == iota((n, n), 1), row, 0.0), 1)


def ends_of(lengths_ref):
    row = lengths_ref[...].astype(jnp.float32)
    n = row.shape[1]
    down, across = iota((n, n), 0), iota((n, n), 1)
    column = total(jnp.where(across <= down, row, 0.0), 1) - 1.0
    return total(jnp.where(down <= across, as_column(row), 0.0), 0) - 1.0, column


def pick_kernel(lengths_ref, *refs):
    *first_ref, hidden_ref, out_ref, most_ref, held, sem = refs
    rows = pltpu.make_async_copy(hidden_ref, held, sem)
    rows.start()
    n, rows_here = lengths_ref.shape[1], held.shape[0]
    ends, _ = ends_of(lengths_ref)
    base = (place() * rows_here).astype(jnp.float32)
    owned = (ends >= base) & (ends < base + rows_here)
    before = total(jnp.where(ends < base, 1.0, 0.0), 1)
    slot = iota((1, n), 1) - before
    if first_ref:
        slot = slot - first_ref[0][0, 0].astype(jnp.float32)
    wanted = owned & (slot == iota((SLOTS, n), 0))
    at = total(jnp.where(wanted, ends - base + 1.0, 0.0), 1) - 1.0
    selector = (at == iota((SLOTS, rows_here), 1)).astype(jnp.bfloat16)
    counts = total(jnp.where(jnp.floor(ends / rows_here) == iota((32, n), 0), 1.0, 0.0), 1)
    most_ref[0, 0] = jnp.max(counts).astype(jnp.int32)
    rows.wait()
    picked = jnp.dot(selector, held[...], preferred_element_type=jnp.float32)
    picked = picked.astype(jnp.bfloat16)
    for peer in range(out_ref.shape[0]):
        out_ref[peer] = picked


def norm_kernel(rows_ref, gain_ref, out_ref):
    parts, _, width = rows_ref.shape
    squares = jnp.zeros((SLOTS, 1), jnp.float32)
    for part in range(parts):
        values = rows_ref[part].astype(jnp.float32)
        squares = squares + total(values * values, 1)
    scale = jnp.sqrt(squares / (parts * width) + 1e-05)
    chips, cores, _, block = out_ref.shape
    for chip in range(chips):
        part, at = divmod(chip * block, width)
        values = rows_ref[part, :, at : at + block].astype(jnp.float32)
        gain = gain_ref[:, chip * block : (chip + 1) * block]
        normed = (values * gain / scale).astype(jnp.bfloat16)
        for core in range(cores):
            out_ref[chip, core] = normed


def rows_in_order(lengths_ref, found_ref, first=0.0):
    n = lengths_ref.shape[1]
    places = found_ref.shape[0]
    rows = 512
    ends_row, ends = ends_of(lengths_ref)
    owner = jnp.floor(ends / rows)
    before = total(jnp.where(ends_row < owner * rows, 1.0, 0.0), 1)
    slot = iota((n, 1), 0) - before - first
    inside = (slot >= 0.0) & (slot < SLOTS)
    at = jnp.where(inside, owner * SLOTS + slot, -1.0)
    selector = (at == iota((n, places), 1)).astype(jnp.bfloat16)
    return jnp.dot(selector, found_ref[...], preferred_element_type=jnp.float32)


def order_kernel(lengths_ref, first_ref, found_ref, more_ref, out_ref):
    first = first_ref[0, 0].astype(jnp.float32)
    rows = rows_in_order(lengths_ref, found_ref, first)
    out_ref[...] = more_ref[...] + rows.astype(jnp.bfloat16)


def half_kernel(weight_ref, keep_ref, sem):
    half = keep_ref.shape[0]
    start = lax.axis_index("c") * (weight_ref.shape[0] - half)
    copy = pltpu.make_async_copy(
        weight_ref.at[pl.ds(pl.multiple_of(start, 16), half)], keep_ref, sem
    )
    copy.start()
    copy.wait()


def head_kernel(lengths_ref, found_ref, more_ref, keep_ref, other_ref, out_ref, held, sems):
    half, width = keep_ref.shape
    first = lax.axis_index("c") == 0
    start = lax.axis_index("c") * (other_ref.shape[0] - half)
    piece = half // PIECES
    copies = []
    for k in range(PIECES):
        rows = pl.ds(pl.multiple_of(start + k * piece, 16), piece)
        copy = pltpu.make_async_copy(other_ref.at[rows], held.at[k], sems.at[k])
        copy.start()
        copies.append(copy)
    rows = rows_in_order(lengths_ref, found_ref).astype(jnp.bfloat16) + more_ref[...]
    low, high = rows[:, :width], rows[:, width:]
    left = jnp.concatenate([jnp.where(first, low, high), jnp.where(first, high, low)], axis=1)
    for block in range(out_ref.shape[0]):
        at = block * BLOCK
        k, inside = divmod(at, piece)
        if inside == 0:
            copies[k].wait()
        weight = jnp.concatenate(
            [keep_ref[at : at + BLOCK, :], held[k, inside : inside + BLOCK, :]], axis=1
        )
        part = lax.dot_general(
            left, weight, (((1,), (1,)), ((), ())), preferred_element_type=jnp.float32
        )
        out_ref[block] = part.astype(out_ref.dtype)


def stats_kernel(spare, vocab, logits_ref, targets_ref, out_ref):
    logits = logits_ref[...]
    n, block = logits.shape
    core = lax.axis_index("c")
    chip = lax.axis_index("x") * lax.axis_size("y") + lax.axis_index("y")
    start = (core * spare + chip * block).astype(jnp.float32)
    column = iota((1, block), 1) + start
    half = vocab - spare
    valid = column >= (core * half).astype(jnp.float32)
    shift = (lax.axis_index("z") * vocab).astype(jnp.float32)
    wanted = as_column(targets_ref[...].astype(jnp.float32)) - shift
    found = total(jnp.where(valid & (column == wanted), logits, 0.0), 1)
    logits = jnp.where(valid, logits, NEG)
    top = jnp.max(logits, axis=1, keepdims=True)
    both = top + jnp.log(total(jnp.exp(logits - top), 1))
    down, across = iota((n, 2 * n), 0), iota((n, 2 * n), 1)
    line = jnp.where(across == down, both, 0.0) + jnp.where(across == down + n, found, 0.0)
    out_ref[...] = jnp.broadcast_to(total(line, 0), out_ref.shape)


def join_kernel(found_ref, out_ref):
    n = out_ref.shape[1]
    lines = found_ref[...]
    top = jnp.max(lines, axis=0, keepdims=True)
    both = top + jnp.log(total(jnp.exp(lines - top), 0))
    chosen = total(lines, 0)
    out_ref[...] = chosen[:, n:] - both[:, :n]


def shape(dims, dtype):
    return jax.ShapeDtypeStruct(dims, dtype)


def in_hbm(x):
    return pltpu.with_memory_space_constraint(x, pltpu.HBM)


def exchange(x, axes):
    return lax.all_to_all(x, axes, split_axis=0, concat_axis=0, tiled=True)


def own_half(weight, half):
    return pl.pallas_call(
        half_kernel,
        out_shape=shape((half, weight.shape[1]), weight.dtype),
        in_specs=[HBM],
        out_specs=VMEM,
        scratch_shapes=[pltpu.SemaphoreType.DMA(())],
        compiler_params=limit(8),
        name="half",
    )(in_hbm(weight))


def picked(lengths, first, hidden):
    return pl.pallas_call(
        pick_kernel,
        out_shape=(
            shape((lax.axis_size("z"), SLOTS, hidden.shape[1]), hidden.dtype),
            shape((1, 1), jnp.int32),
        ),
        in_specs=[VMEM] + [SMEM] * len(first) + [HBM],
        out_specs=(VMEM, SMEM),
        scratch_shapes=[pltpu.VMEM(hidden.shape, hidden.dtype), pltpu.SemaphoreType.DMA(())],
        compiler_params=limit(4),
        name="pick",
    )(lengths, *first, in_hbm(hidden))


def spread(rows, gain):
    chips, cores = lax.axis_size(CHIPS), lax.axis_size("c")
    width = gain.shape[1] // chips
    rows = exchange(rows, "z")
    normed = pl.pallas_call(
        norm_kernel,
        out_shape=shape((chips, cores, SLOTS, width), jnp.bfloat16),
        in_specs=[VMEM, VMEM],
        out_specs=VMEM,
        compiler_params=limit(4),
        name="norm",
    )(rows, gain)
    return exchange(normed.reshape(chips * cores * SLOTS, width), CP)


def local(hidden, lengths, targets, norm_gain, lm_weight):
    n = lengths.shape[0]
    lengths, targets, gain = lengths[None], targets[None], norm_gain[None]
    weight = lm_weight.T
    vocab, depth = weight.shape
    chips = lax.axis_size(CHIPS)
    half = chips * BLOCK
    start = jnp.zeros((1, 1), jnp.int32)
    rows, most = picked(lengths, (), hidden)

    def again(state):
        first, more = state
        found = spread(picked(lengths, (first,), hidden)[0], gain)
        more = pl.pallas_call(
            order_kernel,
            out_shape=shape(more.shape, more.dtype),
            in_specs=[VMEM, SMEM, VMEM, VMEM],
            out_specs=VMEM,
            compiler_params=limit(4),
            name="order",
        )(lengths, first, found, more)
        return first + SLOTS, more

    _, more = lax.while_loop(
        lambda state: state[0][0, 0] < most[0, 0],
        again,
        (start + SLOTS, jnp.zeros((n, gain.shape[1] // chips), jnp.bfloat16)),
    )
    rows, weight, more = lax.optimization_barrier((rows, weight, more))
    found = spread(rows, gain)
    other = lax.ppermute(weight, "c", [(0, 1), (1, 0)])
    keep = own_half(weight, half)
    parts = pl.pallas_call(
        head_kernel,
        out_shape=shape((chips, n, BLOCK), jnp.float32),
        in_specs=[VMEM] * 4 + [HBM],
        out_specs=VMEM,
        scratch_shapes=[
            pltpu.VMEM((PIECES, half // PIECES, depth), weight.dtype),
            pltpu.SemaphoreType.DMA((PIECES,)),
        ],
        compiler_params=limit(16),
        name="head",
    )(lengths, found, more, keep, in_hbm(other))
    logits = jnp.sum(exchange(parts.astype(jnp.float16), CHIPS).astype(jnp.float32), axis=0)
    line = pl.pallas_call(
        functools.partial(stats_kernel, vocab - half, vocab),
        out_shape=shape((lax.axis_size(ALL), 2 * n), jnp.float32),
        in_specs=[VMEM, VMEM],
        out_specs=VMEM,
        compiler_params=limit(4),
        name="stats",
    )(logits, targets)
    lines = exchange(line, ALL)
    out = pl.pallas_call(
        join_kernel,
        out_shape=shape((1, n), jnp.float32),
        in_specs=[VMEM],
        out_specs=VMEM,
        compiler_params=limit(4),
        name="join",
    )(lines)
    return out[0]


def solution(mesh):
    split = Mesh(mesh.devices.reshape(4, 4, 2, mesh.shape["tp"]), ALL)
    return jax.shard_map(
        local,
        mesh=split,
        in_specs=(P(CP, "z"), P(), P(), P(), P(CP, "z")),
        out_specs=P(),
        check_vma=False,
    )
```

```python
import functools

import jax
import jax.numpy as jnp
from jax import lax
from jax.experimental import pallas as pl
from jax.experimental.pallas import tpu as pltpu
from jax.sharding import Mesh
from jax.sharding import PartitionSpec as P

CHIPS = ("x", "y")
CP = ("x", "y", "c")
ALL = ("x", "y", "c", "z")
SLOTS = 8
BLOCK = 512
PIECES = 4
NEG = -1e30

VMEM = pl.BlockSpec(memory_space=pltpu.VMEM)
HBM = pl.BlockSpec(memory_space=pltpu.HBM)
SMEM = pl.BlockSpec(memory_space=pltpu.SMEM)
MIB = 1 << 20


def limit(mib):
    return pltpu.CompilerParams(vmem_limit_bytes=mib * MIB)


def iota(shape, dim):
    return lax.broadcasted_iota(jnp.int32, shape, dim).astype(jnp.float32)


def total(x, axis):
    return jnp.sum(x, axis=axis, keepdims=True)


def place():
    return (lax.axis_index("x") * lax.axis_size("y") + lax.axis_index("y")) * lax.axis_size(
        "c"
    ) + lax.axis_index("c")


def as_column(row):
    n = row.shape[1]
    return total(jnp.where(iota((n, n), 0) == iota((n, n), 1), row, 0.0), 1)


def ends_of(lengths_ref):
    row = lengths_ref[...].astype(jnp.float32)
    n = row.shape[1]
    down, across = iota((n, n), 0), iota((n, n), 1)
    column = total(jnp.where(across <= down, row, 0.0), 1) - 1.0
    return total(jnp.where(down <= across, as_column(row), 0.0), 0) - 1.0, column


def pick_kernel(lengths_ref, *refs):
    *first_ref, hidden_ref, out_ref, most_ref = refs
    n, rows_here = lengths_ref.shape[1], hidden_ref.shape[0]
    ends, _ = ends_of(lengths_ref)
    base = (place() * rows_here).astype(jnp.float32)
    owned = (ends >= base) & (ends < base + rows_here)
    before = total(jnp.where(ends < base, 1.0, 0.0), 1)
    slot = iota((1, n), 1) - before
    if first_ref:
        slot = slot - first_ref[0][0, 0].astype(jnp.float32)
    wanted = owned & (slot == iota((SLOTS, n), 0))
    at = total(jnp.where(wanted, ends - base + 1.0, 0.0), 1) - 1.0
    selector = (at == iota((SLOTS, rows_here), 1)).astype(jnp.bfloat16)
    counts = total(jnp.where(jnp.floor(ends / rows_here) == iota((32, n), 0), 1.0, 0.0), 1)
    most_ref[0, 0] = jnp.max(counts).astype(jnp.int32)
    picked = jnp.dot(selector, hidden_ref[...], preferred_element_type=jnp.float32)
    picked = picked.astype(jnp.bfloat16)
    for peer in range(out_ref.shape[0]):
        out_ref[peer] = picked


def norm_kernel(rows_ref, gain_ref, out_ref):
    parts, _, width = rows_ref.shape
    squares = jnp.zeros((SLOTS, 1), jnp.float32)
    for part in range(parts):
        values = rows_ref[part].astype(jnp.float32)
        squares = squares + total(values * values, 1)
    scale = jnp.sqrt(squares / (parts * width) + 1e-05)
    chips, cores, _, block = out_ref.shape
    for chip in range(chips):
        part, at = divmod(chip * block, width)
        values = rows_ref[part, :, at : at + block].astype(jnp.float32)
        gain = gain_ref[:, chip * block : (chip + 1) * block]
        normed = (values * gain / scale).astype(jnp.bfloat16)
        for core in range(cores):
            out_ref[chip, core] = normed


def rows_in_order(lengths_ref, found_ref, first=0.0):
    n = lengths_ref.shape[1]
    places = found_ref.shape[0]
    rows = 512
    ends_row, ends = ends_of(lengths_ref)
    owner = jnp.floor(ends / rows)
    before = total(jnp.where(ends_row < owner * rows, 1.0, 0.0), 1)
    slot = iota((n, 1), 0) - before - first
    inside = (slot >= 0.0) & (slot < SLOTS)
    at = jnp.where(inside, owner * SLOTS + slot, -1.0)
    selector = (at == iota((n, places), 1)).astype(jnp.bfloat16)
    return jnp.dot(selector, found_ref[...], preferred_element_type=jnp.float32)


def order_kernel(lengths_ref, first_ref, found_ref, more_ref, next_ref, out_ref):
    next_ref[0, 0] = first_ref[0, 0] + SLOTS
    first = first_ref[0, 0].astype(jnp.float32)
    rows = rows_in_order(lengths_ref, found_ref, first)
    out_ref[...] = more_ref[...] + rows.astype(jnp.bfloat16)


def head_kernel(lengths_ref, found_ref, more_ref, weight_ref, other_ref, out_ref, own, sems):
    width = weight_ref.shape[1]
    blocks = out_ref.shape[0]
    pieces, piece, _ = own.shape
    start = lax.axis_index("c") * (weight_ref.shape[0] - blocks * BLOCK)
    first = lax.axis_index("c") == 0

    def span(at, count):
        return pl.ds(pl.multiple_of(start + at, 16), count)

    def product(left, right):
        return lax.dot_general(
            left, right, (((1,), (1,)), ((), ())), preferred_element_type=jnp.float32
        )

    copies = [
        pltpu.make_async_copy(weight_ref.at[span(k * piece, piece)], own.at[k], sems.at[k])
        for k in range(pieces)
    ]
    for copy in copies:
        copy.start()
    rows = rows_in_order(lengths_ref, found_ref).astype(jnp.bfloat16) + more_ref[...]
    low, high = rows[:, :width], rows[:, width:]
    here, there = jnp.where(first, low, high), jnp.where(first, high, low)
    for block in range(blocks):
        out_ref[block] = product(there, other_ref[span(block * BLOCK, BLOCK), :])
    for block in range(blocks):
        k, at = divmod(block * BLOCK, piece)
        if at == 0:
            copies[k].wait()
        out_ref[block] += product(here, own[k, at : at + BLOCK, :])


def stats_kernel(spare, vocab, logits_ref, targets_ref, out_ref):
    logits = logits_ref[...]
    n, block = logits.shape
    core = lax.axis_index("c")
    chip = lax.axis_index("x") * lax.axis_size("y") + lax.axis_index("y")
    start = (core * spare + chip * block).astype(jnp.float32)
    column = iota((1, block), 1) + start
    half = vocab - spare
    valid = column >= (core * half).astype(jnp.float32)
    shift = (lax.axis_index("z") * vocab).astype(jnp.float32)
    wanted = as_column(targets_ref[...].astype(jnp.float32)) - shift
    found = total(jnp.where(valid & (column == wanted), logits, 0.0), 1)
    logits = jnp.where(valid, logits, NEG)
    top = jnp.max(logits, axis=1, keepdims=True)
    both = top + jnp.log(total(jnp.exp(logits - top), 1))
    down, across = iota((n, 2 * n), 0), iota((n, 2 * n), 1)
    line = jnp.where(across == down, both, 0.0) + jnp.where(across == down + n, found, 0.0)
    out_ref[...] = jnp.broadcast_to(total(line, 0), out_ref.shape)


def join_kernel(found_ref, out_ref):
    n = out_ref.shape[1]
    lines = found_ref[...]
    top = jnp.max(lines, axis=0, keepdims=True)
    both = top + jnp.log(total(jnp.exp(lines - top), 0))
    chosen = total(lines, 0)
    out_ref[...] = chosen[:, n:] - both[:, :n]


def shape(dims, dtype):
    return jax.ShapeDtypeStruct(dims, dtype)


def in_hbm(x):
    return pltpu.with_memory_space_constraint(x, pltpu.HBM)


def exchange(x, axes):
    return lax.all_to_all(x, axes, split_axis=0, concat_axis=0, tiled=True)


def picked(lengths, first, hidden):
    return pl.pallas_call(
        pick_kernel,
        out_shape=(
            shape((lax.axis_size("z"), SLOTS, hidden.shape[1]), hidden.dtype),
            shape((1, 1), jnp.int32),
        ),
        in_specs=[VMEM] + [SMEM] * len(first) + [VMEM],
        out_specs=(VMEM, SMEM),
        compiler_params=limit(4),
        name="pick",
    )(lengths, *first, hidden)


def spread(rows, gain, after=()):
    chips, cores = lax.axis_size(CHIPS), lax.axis_size("c")
    width = gain.shape[1] // chips
    rows, after = lax.optimization_barrier((exchange(rows, "z"), after))
    normed = pl.pallas_call(
        norm_kernel,
        out_shape=shape((chips, cores, SLOTS, width), jnp.bfloat16),
        in_specs=[VMEM, VMEM],
        out_specs=VMEM,
        compiler_params=limit(4),
        name="norm",
    )(rows, gain)
    return exchange(normed.reshape(chips * cores * SLOTS, width), CP), after


def local(hidden, lengths, targets, norm_gain, lm_weight):
    n = lengths.shape[0]
    lengths, targets, gain = lengths[None], targets[None], norm_gain[None]
    weight = lm_weight.T
    vocab, depth = weight.shape
    chips = lax.axis_size(CHIPS)
    half = chips * BLOCK
    start = jnp.zeros((1, 1), jnp.int32)
    rows, most = picked(lengths, (), hidden)
    other = lax.ppermute(weight, "c", [(0, 1), (1, 0)])

    def again(state):
        first, more = state
        found = spread(picked(lengths, (first,), hidden)[0], gain)[0]
        return pl.pallas_call(
            order_kernel,
            out_shape=(shape(first.shape, first.dtype), shape(more.shape, more.dtype)),
            in_specs=[VMEM, SMEM, VMEM, VMEM],
            out_specs=(SMEM, VMEM),
            input_output_aliases={1: 0, 3: 1},
            compiler_params=limit(4),
            name="order",
        )(lengths, first, found, more)

    _, more = lax.while_loop(
        lambda state: state[0][0, 0] < most[0, 0],
        again,
        (start + SLOTS, jnp.zeros((n, gain.shape[1] // chips), jnp.bfloat16)),
    )
    rows, more = lax.optimization_barrier((rows, more))
    found, other = spread(rows, gain, other)
    parts = pl.pallas_call(
        head_kernel,
        out_shape=shape((chips, n, BLOCK), jnp.float32),
        in_specs=[VMEM] * 3 + [HBM, VMEM],
        out_specs=VMEM,
        scratch_shapes=[
            pltpu.VMEM((PIECES, half // PIECES, depth), weight.dtype),
            pltpu.SemaphoreType.DMA((PIECES,)),
        ],
        compiler_params=limit(16),
        name="head",
    )(lengths, found, more, in_hbm(weight), other)
    logits = jnp.sum(exchange(parts.astype(jnp.float16), CHIPS).astype(jnp.float32), axis=0)
    line = pl.pallas_call(
        functools.partial(stats_kernel, vocab - half, vocab),
        out_shape=shape((lax.axis_size(ALL), 2 * n), jnp.float32),
        in_specs=[VMEM, VMEM],
        out_specs=VMEM,
        compiler_params=limit(4),
        name="stats",
    )(logits, targets)
    lines = exchange(line, ALL)
    out = pl.pallas_call(
        join_kernel,
        out_shape=shape((1, n), jnp.float32),
        in_specs=[VMEM],
        out_specs=VMEM,
        compiler_params=limit(4),
        name="join",
    )(lines)
    return out[0]


def solution(mesh):
    split = Mesh(mesh.devices.reshape(4, 4, 2, mesh.shape["tp"]), ALL)
    return jax.shard_map(
        local,
        mesh=split,
        in_specs=(P(CP, "z"), P(), P(), P(), P(CP, "z")),
        out_specs=P(),
        check_vma=False,
    )
```

```python
import functools

import jax
import jax.numpy as jnp
from jax import lax
from jax.experimental import pallas as pl
from jax.experimental.pallas import tpu as pltpu
from jax.sharding import Mesh
from jax.sharding import PartitionSpec as P

CHIPS = ("x", "y")
CP = ("x", "y", "c")
ALL = ("x", "y", "c", "z")
SLOTS = 8
BLOCK = 512
NEG = -1e30

VMEM = pl.BlockSpec(memory_space=pltpu.VMEM)
SMEM = pl.BlockSpec(memory_space=pltpu.SMEM)
MIB = 1 << 20


def limit(mib):
    return pltpu.CompilerParams(vmem_limit_bytes=mib * MIB)


def iota(shape, dim):
    return lax.broadcasted_iota(jnp.int32, shape, dim).astype(jnp.float32)


def total(x, axis):
    return jnp.sum(x, axis=axis, keepdims=True)


def place():
    return (lax.axis_index("x") * lax.axis_size("y") + lax.axis_index("y")) * lax.axis_size(
        "c"
    ) + lax.axis_index("c")


def as_column(row):
    n = row.shape[1]
    return total(jnp.where(iota((n, n), 0) == iota((n, n), 1), row, 0.0), 1)


def ends_of(lengths_ref):
    row = lengths_ref[...].astype(jnp.float32)
    n = row.shape[1]
    down, across = iota((n, n), 0), iota((n, n), 1)
    column = total(jnp.where(across <= down, row, 0.0), 1) - 1.0
    return total(jnp.where(down <= across, as_column(row), 0.0), 0) - 1.0, column


def pick_kernel(lengths_ref, *refs):
    *first_ref, hidden_ref, out_ref, most_ref = refs
    n, rows_here = lengths_ref.shape[1], hidden_ref.shape[0]
    ends, _ = ends_of(lengths_ref)
    base = (place() * rows_here).astype(jnp.float32)
    owned = (ends >= base) & (ends < base + rows_here)
    before = total(jnp.where(ends < base, 1.0, 0.0), 1)
    slot = iota((1, n), 1) - before
    if first_ref:
        slot = slot - first_ref[0][0, 0].astype(jnp.float32)
    wanted = owned & (slot == iota((SLOTS, n), 0))
    at = total(jnp.where(wanted, ends - base + 1.0, 0.0), 1) - 1.0
    selector = (at == iota((SLOTS, rows_here), 1)).astype(jnp.bfloat16)
    counts = total(jnp.where(jnp.floor(ends / rows_here) == iota((32, n), 0), 1.0, 0.0), 1)
    most_ref[0, 0] = jnp.max(counts).astype(jnp.int32)
    picked = jnp.dot(selector, hidden_ref[...], preferred_element_type=jnp.float32)
    picked = picked.astype(jnp.bfloat16)
    for peer in range(out_ref.shape[0]):
        out_ref[peer] = picked


def norm_kernel(rows_ref, gain_ref, out_ref):
    parts, _, width = rows_ref.shape
    squares = jnp.zeros((SLOTS, 1), jnp.float32)
    for part in range(parts):
        values = rows_ref[part].astype(jnp.float32)
        squares = squares + total(values * values, 1)
    scale = jnp.sqrt(squares / (parts * width) + 1e-05)
    chips, cores, _, block = out_ref.shape
    for chip in range(chips):
        part, at = divmod(chip * block, width)
        values = rows_ref[part, :, at : at + block].astype(jnp.float32)
        gain = gain_ref[:, chip * block : (chip + 1) * block]
        normed = (values * gain / scale).astype(jnp.bfloat16)
        for core in range(cores):
            out_ref[chip, core] = normed


def rows_in_order(lengths_ref, found_ref, first=0.0):
    n = lengths_ref.shape[1]
    places = found_ref.shape[0]
    rows = 512
    ends_row, ends = ends_of(lengths_ref)
    owner = jnp.floor(ends / rows)
    before = total(jnp.where(ends_row < owner * rows, 1.0, 0.0), 1)
    slot = iota((n, 1), 0) - before - first
    inside = (slot >= 0.0) & (slot < SLOTS)
    at = jnp.where(inside, owner * SLOTS + slot, -1.0)
    selector = (at == iota((n, places), 1)).astype(jnp.bfloat16)
    return jnp.dot(selector, found_ref[...], preferred_element_type=jnp.float32)


def order_kernel(lengths_ref, first_ref, found_ref, more_ref, next_ref, out_ref):
    next_ref[0, 0] = first_ref[0, 0] + SLOTS
    first = first_ref[0, 0].astype(jnp.float32)
    rows = rows_in_order(lengths_ref, found_ref, first)
    out_ref[...] = more_ref[...] + rows.astype(jnp.bfloat16)


def head_kernel(lengths_ref, found_ref, more_ref, weight_ref, other_ref, out_ref):
    width = weight_ref.shape[1]
    blocks = out_ref.shape[0]
    start = lax.axis_index("c") * (weight_ref.shape[0] - blocks * BLOCK)
    first = lax.axis_index("c") == 0
    rows = rows_in_order(lengths_ref, found_ref).astype(jnp.bfloat16) + more_ref[...]
    low, high = rows[:, :width], rows[:, width:]
    left = jnp.concatenate([jnp.where(first, low, high), jnp.where(first, high, low)], axis=1)
    for block in range(blocks):
        span = pl.ds(pl.multiple_of(start + block * BLOCK, 16), BLOCK)
        weight = jnp.concatenate([weight_ref[span, :], other_ref[span, :]], axis=1)
        part = lax.dot_general(
            left, weight, (((1,), (1,)), ((), ())), preferred_element_type=jnp.float32
        )
        out_ref[block] = part.astype(out_ref.dtype)


def stats_kernel(spare, vocab, logits_ref, targets_ref, out_ref):
    logits = logits_ref[...]
    n, block = logits.shape
    core = lax.axis_index("c")
    chip = lax.axis_index("x") * lax.axis_size("y") + lax.axis_index("y")
    start = (core * spare + chip * block).astype(jnp.float32)
    column = iota((1, block), 1) + start
    half = vocab - spare
    valid = column >= (core * half).astype(jnp.float32)
    shift = (lax.axis_index("z") * vocab).astype(jnp.float32)
    wanted = as_column(targets_ref[...].astype(jnp.float32)) - shift
    found = total(jnp.where(valid & (column == wanted), logits, 0.0), 1)
    logits = jnp.where(valid, logits, NEG)
    top = jnp.max(logits, axis=1, keepdims=True)
    both = top + jnp.log(total(jnp.exp(logits - top), 1))
    down, across = iota((n, 2 * n), 0), iota((n, 2 * n), 1)
    line = jnp.where(across == down, both, 0.0) + jnp.where(across == down + n, found, 0.0)
    out_ref[...] = jnp.broadcast_to(total(line, 0), out_ref.shape)


def join_kernel(found_ref, out_ref):
    n = out_ref.shape[1]
    lines = found_ref[...]
    top = jnp.max(lines, axis=0, keepdims=True)
    both = top + jnp.log(total(jnp.exp(lines - top), 0))
    chosen = total(lines, 0)
    out_ref[...] = chosen[:, n:] - both[:, :n]


def shape(dims, dtype):
    return jax.ShapeDtypeStruct(dims, dtype)


def exchange(x, axes):
    return lax.all_to_all(x, axes, split_axis=0, concat_axis=0, tiled=True)


def picked(lengths, first, hidden):
    return pl.pallas_call(
        pick_kernel,
        out_shape=(
            shape((lax.axis_size("z"), SLOTS, hidden.shape[1]), hidden.dtype),
            shape((1, 1), jnp.int32),
        ),
        in_specs=[VMEM] + [SMEM] * len(first) + [VMEM],
        out_specs=(VMEM, SMEM),
        compiler_params=limit(4),
        name="pick",
    )(lengths, *first, hidden)


def spread(rows, gain, after=()):
    chips, cores = lax.axis_size(CHIPS), lax.axis_size("c")
    width = gain.shape[1] // chips
    rows, after = lax.optimization_barrier((exchange(rows, "z"), after))
    normed = pl.pallas_call(
        norm_kernel,
        out_shape=shape((chips, cores, SLOTS, width), jnp.bfloat16),
        in_specs=[VMEM, VMEM],
        out_specs=VMEM,
        compiler_params=limit(4),
        name="norm",
    )(rows, gain)
    return exchange(normed.reshape(chips * cores * SLOTS, width), CP), after


def local(hidden, lengths, targets, norm_gain, lm_weight):
    n = lengths.shape[0]
    lengths, targets, gain = lengths[None], targets[None], norm_gain[None]
    weight = lm_weight.T
    vocab, depth = weight.shape
    chips = lax.axis_size(CHIPS)
    half = chips * BLOCK
    start = jnp.zeros((1, 1), jnp.int32)
    rows, most = picked(lengths, (), hidden)
    other = lax.ppermute(weight, "c", [(0, 1), (1, 0)])

    def again(state):
        first, more = state
        found = spread(picked(lengths, (first,), hidden)[0], gain)[0]
        return pl.pallas_call(
            order_kernel,
            out_shape=(shape(first.shape, first.dtype), shape(more.shape, more.dtype)),
            in_specs=[VMEM, SMEM, VMEM, VMEM],
            out_specs=(SMEM, VMEM),
            input_output_aliases={1: 0, 3: 1},
            compiler_params=limit(4),
            name="order",
        )(lengths, first, found, more)

    _, more = lax.while_loop(
        lambda state: state[0][0, 0] < most[0, 0],
        again,
        (start + SLOTS, jnp.zeros((n, gain.shape[1] // chips), jnp.bfloat16)),
    )
    rows, more, weight = lax.optimization_barrier((rows, more, weight))
    own = lax.ppermute(weight, "c", [(0, 0), (1, 1)])
    found, (own, other) = spread(rows, gain, (own, other))
    parts = pl.pallas_call(
        head_kernel,
        out_shape=shape((chips, n, BLOCK), jnp.float32),
        in_specs=[VMEM] * 5,
        out_specs=VMEM,
        compiler_params=limit(16),
        name="head",
    )(lengths, found, more, own, other)
    logits = jnp.sum(exchange(parts.astype(jnp.float16), CHIPS).astype(jnp.float32), axis=0)
    line = pl.pallas_call(
        functools.partial(stats_kernel, vocab - half, vocab),
        out_shape=shape((lax.axis_size(ALL), 2 * n), jnp.float32),
        in_specs=[VMEM, VMEM],
        out_specs=VMEM,
        compiler_params=limit(4),
        name="stats",
    )(logits, targets)
    lines = exchange(line, ALL)
    out = pl.pallas_call(
        join_kernel,
        out_shape=shape((1, n), jnp.float32),
        in_specs=[VMEM],
        out_specs=VMEM,
        compiler_params=limit(4),
        name="join",
    )(lines)
    return out[0]


def solution(mesh):
    split = Mesh(mesh.devices.reshape(4, 4, 2, mesh.shape["tp"]), ALL)
    return jax.shard_map(
        local,
        mesh=split,
        in_specs=(P(CP, "z"), P(), P(), P(), P(CP, "z")),
        out_specs=P(),
        check_vma=False,
    )
```

```python
import functools

import jax
import jax.numpy as jnp
from jax import lax
from jax.experimental import pallas as pl
from jax.experimental.pallas import tpu as pltpu
from jax.sharding import Mesh
from jax.sharding import PartitionSpec as P

CHIPS = ("x", "y")
CP = ("x", "y", "c")
ALL = ("x", "y", "c", "z")
SLOTS = 8
BLOCK = 512
NEG = -1e30

VMEM = pl.BlockSpec(memory_space=pltpu.VMEM)
SMEM = pl.BlockSpec(memory_space=pltpu.SMEM)
MIB = 1 << 20


def limit(mib):
    return pltpu.CompilerParams(vmem_limit_bytes=mib * MIB)


def iota(shape, dim):
    return lax.broadcasted_iota(jnp.int32, shape, dim).astype(jnp.float32)


def total(x, axis):
    return jnp.sum(x, axis=axis, keepdims=True)


def place():
    return (lax.axis_index("x") * lax.axis_size("y") + lax.axis_index("y")) * lax.axis_size(
        "c"
    ) + lax.axis_index("c")


def as_column(row):
    n = row.shape[1]
    return total(jnp.where(iota((n, n), 0) == iota((n, n), 1), row, 0.0), 1)


def ends_of(lengths_ref):
    row = lengths_ref[...].astype(jnp.float32)
    n = row.shape[1]
    down, across = iota((n, n), 0), iota((n, n), 1)
    column = total(jnp.where(across <= down, row, 0.0), 1) - 1.0
    return total(jnp.where(down <= across, as_column(row), 0.0), 0) - 1.0, column


def pick_kernel(lengths_ref, *refs):
    *first_ref, hidden_ref, out_ref, most_ref = refs
    n, rows_here = lengths_ref.shape[1], hidden_ref.shape[0]
    ends, _ = ends_of(lengths_ref)
    base = (place() * rows_here).astype(jnp.float32)
    owned = (ends >= base) & (ends < base + rows_here)
    before = total(jnp.where(ends < base, 1.0, 0.0), 1)
    slot = iota((1, n), 1) - before
    if first_ref:
        slot = slot - first_ref[0][0, 0].astype(jnp.float32)
    wanted = owned & (slot == iota((SLOTS, n), 0))
    at = total(jnp.where(wanted, ends - base + 1.0, 0.0), 1) - 1.0
    selector = (at == iota((SLOTS, rows_here), 1)).astype(jnp.bfloat16)
    counts = total(jnp.where(jnp.floor(ends / rows_here) == iota((32, n), 0), 1.0, 0.0), 1)
    most_ref[0, 0] = jnp.max(counts).astype(jnp.int32)
    picked = jnp.dot(selector, hidden_ref[...], preferred_element_type=jnp.float32)
    picked = picked.astype(jnp.bfloat16)
    for peer in range(out_ref.shape[0]):
        out_ref[peer] = picked


def norm_kernel(rows_ref, gain_ref, out_ref):
    parts, _, width = rows_ref.shape
    squares = jnp.zeros((SLOTS, 1), jnp.float32)
    for part in range(parts):
        values = rows_ref[part].astype(jnp.float32)
        squares = squares + total(values * values, 1)
    scale = jnp.sqrt(squares / (parts * width) + 1e-05)
    chips, cores, _, block = out_ref.shape
    for chip in range(chips):
        part, at = divmod(chip * block, width)
        values = rows_ref[part, :, at : at + block].astype(jnp.float32)
        gain = gain_ref[:, chip * block : (chip + 1) * block]
        normed = (values * gain / scale).astype(jnp.bfloat16)
        for core in range(cores):
            out_ref[chip, core] = normed


def rows_in_order(lengths_ref, found_ref, first=0.0):
    n = lengths_ref.shape[1]
    places = found_ref.shape[0]
    rows = 512
    ends_row, ends = ends_of(lengths_ref)
    owner = jnp.floor(ends / rows)
    before = total(jnp.where(ends_row < owner * rows, 1.0, 0.0), 1)
    slot = iota((n, 1), 0) - before - first
    inside = (slot >= 0.0) & (slot < SLOTS)
    at = jnp.where(inside, owner * SLOTS + slot, -1.0)
    selector = (at == iota((n, places), 1)).astype(jnp.bfloat16)
    return jnp.dot(selector, found_ref[...], preferred_element_type=jnp.float32)


def order_kernel(lengths_ref, first_ref, found_ref, more_ref, next_ref, out_ref):
    next_ref[0, 0] = first_ref[0, 0] + SLOTS
    first = first_ref[0, 0].astype(jnp.float32)
    rows = rows_in_order(lengths_ref, found_ref, first)
    out_ref[...] = more_ref[...] + rows.astype(jnp.bfloat16)


def head_kernel(lengths_ref, found_ref, more_ref, weight_ref, other_ref, out_ref):
    width = weight_ref.shape[1]
    blocks = out_ref.shape[0]
    start = lax.axis_index("c") * (weight_ref.shape[0] - blocks * BLOCK)
    first = lax.axis_index("c") == 0
    rows = rows_in_order(lengths_ref, found_ref).astype(jnp.bfloat16) + more_ref[...]
    low, high = rows[:, :width], rows[:, width:]
    left = jnp.concatenate([jnp.where(first, low, high), jnp.where(first, high, low)], axis=1)
    for block in range(blocks):
        span = pl.ds(pl.multiple_of(start + block * BLOCK, 16), BLOCK)
        weight = jnp.concatenate([weight_ref[span, :], other_ref[span, :]], axis=1)
        part = lax.dot_general(
            left, weight, (((1,), (1,)), ((), ())), preferred_element_type=jnp.float32
        )
        out_ref[block] = part.astype(out_ref.dtype)


def stats_kernel(spare, vocab, logits_ref, targets_ref, out_ref):
    logits = logits_ref[...]
    n, block = logits.shape
    core = lax.axis_index("c")
    chip = lax.axis_index("x") * lax.axis_size("y") + lax.axis_index("y")
    start = (core * spare + chip * block).astype(jnp.float32)
    column = iota((1, block), 1) + start
    half = vocab - spare
    valid = column >= (core * half).astype(jnp.float32)
    shift = (lax.axis_index("z") * vocab).astype(jnp.float32)
    wanted = as_column(targets_ref[...].astype(jnp.float32)) - shift
    found = total(jnp.where(valid & (column == wanted), logits, 0.0), 1)
    logits = jnp.where(valid, logits, NEG)
    top = jnp.max(logits, axis=1, keepdims=True)
    both = top + jnp.log(total(jnp.exp(logits - top), 1))
    down, across = iota((n, 2 * n), 0), iota((n, 2 * n), 1)
    line = jnp.where(across == down, both, 0.0) + jnp.where(across == down + n, found, 0.0)
    out_ref[...] = jnp.broadcast_to(total(line, 0), out_ref.shape)


def join_kernel(found_ref, out_ref):
    n = out_ref.shape[1]
    lines = found_ref[...]
    top = jnp.max(lines, axis=0, keepdims=True)
    both = top + jnp.log(total(jnp.exp(lines - top), 0))
    chosen = total(lines, 0)
    out_ref[...] = chosen[:, n:] - both[:, :n]


def shape(dims, dtype):
    return jax.ShapeDtypeStruct(dims, dtype)


def exchange(x, axes):
    return lax.all_to_all(x, axes, split_axis=0, concat_axis=0, tiled=True)


def picked(lengths, first, hidden):
    return pl.pallas_call(
        pick_kernel,
        out_shape=(
            shape((lax.axis_size("z"), SLOTS, hidden.shape[1]), hidden.dtype),
            shape((1, 1), jnp.int32),
        ),
        in_specs=[VMEM] + [SMEM] * len(first) + [VMEM],
        out_specs=(VMEM, SMEM),
        compiler_params=limit(4),
        cost_estimate=pl.CostEstimate(flops=10**10, bytes_accessed=1 << 25, transcendentals=0),
        name="pick",
    )(lengths, *first, hidden)


def spread(rows, gain, after=()):
    chips, cores = lax.axis_size(CHIPS), lax.axis_size("c")
    width = gain.shape[1] // chips
    rows, after = lax.optimization_barrier((exchange(rows, "z"), after))
    normed = pl.pallas_call(
        norm_kernel,
        out_shape=shape((chips, cores, SLOTS, width), jnp.bfloat16),
        in_specs=[VMEM, VMEM],
        out_specs=VMEM,
        compiler_params=limit(4),
        cost_estimate=pl.CostEstimate(flops=10**10, bytes_accessed=1 << 25, transcendentals=0),
        name="norm",
    )(rows, gain)
    return exchange(normed.reshape(chips * cores * SLOTS, width), CP), after


def local(hidden, lengths, targets, norm_gain, lm_weight):
    n = lengths.shape[0]
    lengths, targets, gain = lengths[None], targets[None], norm_gain[None]
    weight = lm_weight.T
    vocab, depth = weight.shape
    chips = lax.axis_size(CHIPS)
    half = chips * BLOCK
    start = jnp.zeros((1, 1), jnp.int32)
    rows, most = picked(lengths, (), hidden)

    def again(state):
        first, more = state
        found = spread(picked(lengths, (first,), hidden)[0], gain)[0]
        return pl.pallas_call(
            order_kernel,
            out_shape=(shape(first.shape, first.dtype), shape(more.shape, more.dtype)),
            in_specs=[VMEM, SMEM, VMEM, VMEM],
            out_specs=(SMEM, VMEM),
            input_output_aliases={1: 0, 3: 1},
            compiler_params=limit(4),
            name="order",
        )(lengths, first, found, more)

    _, more = lax.while_loop(
        lambda state: state[0][0, 0] < most[0, 0],
        again,
        (start + SLOTS, jnp.zeros((n, gain.shape[1] // chips), jnp.bfloat16)),
    )
    rows, more, weight = lax.optimization_barrier((rows, more, weight))
    found, weight = spread(rows, gain, weight)
    other = lax.ppermute(weight, "c", [(0, 1), (1, 0)])
    own = weight
    parts = pl.pallas_call(
        head_kernel,
        out_shape=shape((chips, n, BLOCK), jnp.float32),
        in_specs=[VMEM] * 5,
        out_specs=VMEM,
        compiler_params=limit(16),
        name="head",
    )(lengths, found, more, own, other)
    logits = jnp.sum(exchange(parts.astype(jnp.float16), CHIPS).astype(jnp.float32), axis=0)
    line = pl.pallas_call(
        functools.partial(stats_kernel, vocab - half, vocab),
        out_shape=shape((lax.axis_size(ALL), 2 * n), jnp.float32),
        in_specs=[VMEM, VMEM],
        out_specs=VMEM,
        compiler_params=limit(4),
        name="stats",
    )(logits, targets)
    lines = exchange(line, ALL)
    out = pl.pallas_call(
        join_kernel,
        out_shape=shape((1, n), jnp.float32),
        in_specs=[VMEM],
        out_specs=VMEM,
        compiler_params=limit(4),
        name="join",
    )(lines)
    return out[0]


def solution(mesh):
    split = Mesh(mesh.devices.reshape(4, 4, 2, mesh.shape["tp"]), ALL)
    return jax.shard_map(
        local,
        mesh=split,
        in_specs=(P(CP, "z"), P(), P(), P(), P(CP, "z")),
        out_specs=P(),
        check_vma=False,
    )
```

```python
import functools

import jax
import jax.numpy as jnp
from jax import lax
from jax.experimental import pallas as pl
from jax.experimental.pallas import tpu as pltpu
from jax.sharding import Mesh
from jax.sharding import PartitionSpec as P

CHIPS = ("x", "y")
CP = ("x", "y", "c")
ALL = ("x", "y", "c", "z")
SLOTS = 8
BLOCK = 512
NEG = -1e30

VMEM = pl.BlockSpec(memory_space=pltpu.VMEM)
HBM = pl.BlockSpec(memory_space=pltpu.HBM)
SMEM = pl.BlockSpec(memory_space=pltpu.SMEM)
MIB = 1 << 20


def limit(mib):
    return pltpu.CompilerParams(vmem_limit_bytes=mib * MIB)


def iota(shape, dim):
    return lax.broadcasted_iota(jnp.int32, shape, dim).astype(jnp.float32)


def total(x, axis):
    return jnp.sum(x, axis=axis, keepdims=True)


def place():
    return (lax.axis_index("x") * lax.axis_size("y") + lax.axis_index("y")) * lax.axis_size(
        "c"
    ) + lax.axis_index("c")


def as_column(row):
    n = row.shape[1]
    return total(jnp.where(iota((n, n), 0) == iota((n, n), 1), row, 0.0), 1)


def ends_of(lengths_ref):
    row = lengths_ref[...].astype(jnp.float32)
    n = row.shape[1]
    down, across = iota((n, n), 0), iota((n, n), 1)
    column = total(jnp.where(across <= down, row, 0.0), 1) - 1.0
    return total(jnp.where(down <= across, as_column(row), 0.0), 0) - 1.0, column


def pick_kernel(lengths_ref, *refs):
    *first_ref, hidden_ref, out_ref, more_ref, lengths, hidden, flag, sems = refs
    small = pltpu.make_async_copy(lengths_ref, lengths, sems.at[0])
    large = pltpu.make_async_copy(hidden_ref, hidden, sems.at[1])
    small.start()
    large.start()
    first = first_ref[0][0, 0] if first_ref else jnp.int32(0)
    small.wait()
    n, rows_here = lengths.shape[1], hidden.shape[0]
    ends, _ = ends_of(lengths)
    counts = total(jnp.where(jnp.floor(ends / rows_here) == iota((32, n), 0), 1.0, 0.0), 1)
    most = jnp.max(counts).astype(jnp.int32)
    flag[0, 0] = (most > first + SLOTS).astype(jnp.int32)
    tell = pltpu.make_async_copy(flag, more_ref, sems.at[2])
    tell.start()
    base = (place() * rows_here).astype(jnp.float32)
    owned = (ends >= base) & (ends < base + rows_here)
    before = total(jnp.where(ends < base, 1.0, 0.0), 1)
    slot = iota((1, n), 1) - before - first.astype(jnp.float32)
    wanted = owned & (slot == iota((SLOTS, n), 0))
    at = total(jnp.where(wanted, ends - base + 1.0, 0.0), 1) - 1.0
    selector = (at == iota((SLOTS, rows_here), 1)).astype(jnp.bfloat16)
    large.wait()
    picked = jnp.dot(selector, hidden[...], preferred_element_type=jnp.float32)
    picked = picked.astype(jnp.bfloat16)
    for peer in range(out_ref.shape[0]):
        out_ref[peer] = picked
    tell.wait()


def norm_kernel(rows_ref, gain_ref, out_ref):
    parts, _, width = rows_ref.shape
    squares = jnp.zeros((SLOTS, 1), jnp.float32)
    for part in range(parts):
        values = rows_ref[part].astype(jnp.float32)
        squares = squares + total(values * values, 1)
    scale = jnp.sqrt(squares / (parts * width) + 1e-05)
    chips, cores, _, block = out_ref.shape
    for chip in range(chips):
        part, at = divmod(chip * block, width)
        values = rows_ref[part, :, at : at + block].astype(jnp.float32)
        gain = gain_ref[:, chip * block : (chip + 1) * block]
        normed = (values * gain / scale).astype(jnp.bfloat16)
        for core in range(cores):
            out_ref[chip, core] = normed


def rows_in_order(lengths_ref, found_ref, first=0.0):
    n = lengths_ref.shape[1]
    places = found_ref.shape[0]
    rows = 512
    ends_row, ends = ends_of(lengths_ref)
    owner = jnp.floor(ends / rows)
    before = total(jnp.where(ends_row < owner * rows, 1.0, 0.0), 1)
    slot = iota((n, 1), 0) - before - first
    inside = (slot >= 0.0) & (slot < SLOTS)
    at = jnp.where(inside, owner * SLOTS + slot, -1.0)
    selector = (at == iota((n, places), 1)).astype(jnp.bfloat16)
    return jnp.dot(selector, found_ref[...], preferred_element_type=jnp.float32)


def order_kernel(lengths_ref, first_ref, found_ref, more_ref, next_ref, out_ref):
    next_ref[0, 0] = first_ref[0, 0] + SLOTS
    first = first_ref[0, 0].astype(jnp.float32)
    rows = rows_in_order(lengths_ref, found_ref, first)
    out_ref[...] = more_ref[...] + rows.astype(jnp.bfloat16)


def head_kernel(lengths_ref, found_ref, more_ref, weight_ref, other_ref, out_ref):
    width = weight_ref.shape[1]
    blocks = out_ref.shape[0]
    start = lax.axis_index("c") * (weight_ref.shape[0] - blocks * BLOCK)
    first = lax.axis_index("c") == 0
    rows = rows_in_order(lengths_ref, found_ref).astype(jnp.bfloat16) + more_ref[...]
    low, high = rows[:, :width], rows[:, width:]
    left = jnp.concatenate([jnp.where(first, low, high), jnp.where(first, high, low)], axis=1)
    for block in range(blocks):
        span = pl.ds(pl.multiple_of(start + block * BLOCK, 16), BLOCK)
        weight = jnp.concatenate([weight_ref[span, :], other_ref[span, :]], axis=1)
        part = lax.dot_general(
            left, weight, (((1,), (1,)), ((), ())), preferred_element_type=jnp.float32
        )
        out_ref[block] = part.astype(out_ref.dtype)


def stats_kernel(spare, vocab, logits_ref, targets_ref, out_ref):
    logits = logits_ref[...]
    n, block = logits.shape
    core = lax.axis_index("c")
    chip = lax.axis_index("x") * lax.axis_size("y") + lax.axis_index("y")
    start = (core * spare + chip * block).astype(jnp.float32)
    column = iota((1, block), 1) + start
    half = vocab - spare
    valid = column >= (core * half).astype(jnp.float32)
    shift = (lax.axis_index("z") * vocab).astype(jnp.float32)
    wanted = as_column(targets_ref[...].astype(jnp.float32)) - shift
    found = total(jnp.where(valid & (column == wanted), logits, 0.0), 1)
    logits = jnp.where(valid, logits, NEG)
    top = jnp.max(logits, axis=1, keepdims=True)
    both = top + jnp.log(total(jnp.exp(logits - top), 1))
    down, across = iota((n, 2 * n), 0), iota((n, 2 * n), 1)
    line = jnp.where(across == down, both, 0.0) + jnp.where(across == down + n, found, 0.0)
    out_ref[...] = jnp.broadcast_to(total(line, 0), out_ref.shape)


def join_kernel(found_ref, out_ref):
    n = out_ref.shape[1]
    lines = found_ref[...]
    top = jnp.max(lines, axis=0, keepdims=True)
    both = top + jnp.log(total(jnp.exp(lines - top), 0))
    chosen = total(lines, 0)
    out_ref[...] = chosen[:, n:] - both[:, :n]


def shape(dims, dtype):
    return jax.ShapeDtypeStruct(dims, dtype)


def in_hbm(x):
    return pltpu.with_memory_space_constraint(x, pltpu.HBM)


def exchange(x, axes):
    return lax.all_to_all(x, axes, split_axis=0, concat_axis=0, tiled=True)


def picked(lengths, first, hidden):
    return pl.pallas_call(
        pick_kernel,
        out_shape=(
            shape((lax.axis_size("z"), SLOTS, hidden.shape[1]), hidden.dtype),
            shape((1, 1), jnp.int32),
        ),
        in_specs=[HBM] + [SMEM] * len(first) + [HBM],
        out_specs=(VMEM, HBM),
        scratch_shapes=[
            pltpu.VMEM(lengths.shape, lengths.dtype),
            pltpu.VMEM(hidden.shape, hidden.dtype),
            pltpu.SMEM((1, 1), jnp.int32),
            pltpu.SemaphoreType.DMA((3,)),
        ],
        compiler_params=limit(4),
        cost_estimate=pl.CostEstimate(flops=10**10, bytes_accessed=1 << 25, transcendentals=0),
        name="pick",
    )(in_hbm(lengths), *first, in_hbm(hidden))


def spread(rows, gain, after=()):
    chips, cores = lax.axis_size(CHIPS), lax.axis_size("c")
    width = gain.shape[1] // chips
    rows, after = lax.optimization_barrier((exchange(rows, "z"), after))
    normed = pl.pallas_call(
        norm_kernel,
        out_shape=shape((chips, cores, SLOTS, width), jnp.bfloat16),
        in_specs=[VMEM, VMEM],
        out_specs=VMEM,
        compiler_params=limit(4),
        cost_estimate=pl.CostEstimate(flops=10**10, bytes_accessed=1 << 25, transcendentals=0),
        name="norm",
    )(rows, gain)
    return exchange(normed.reshape(chips * cores * SLOTS, width), CP), after


def local(hidden, lengths, targets, norm_gain, lm_weight):
    n = lengths.shape[0]
    lengths, targets, gain = lengths[None], targets[None], norm_gain[None]
    weight = lm_weight.T
    vocab, depth = weight.shape
    chips = lax.axis_size(CHIPS)
    half = chips * BLOCK
    start = jnp.zeros((1, 1), jnp.int32)
    rows, some = picked(lengths, (), hidden)

    def again(state):
        _, first, more = state
        rows, some = picked(lengths, (first,), hidden)
        found = spread(rows, gain)[0]
        first, more = pl.pallas_call(
            order_kernel,
            out_shape=(shape(first.shape, first.dtype), shape(more.shape, more.dtype)),
            in_specs=[VMEM, SMEM, VMEM, VMEM],
            out_specs=(SMEM, VMEM),
            input_output_aliases={1: 0, 3: 1},
            compiler_params=limit(4),
            name="order",
        )(lengths, first, found, more)
        return some, first, more

    _, _, more = lax.while_loop(
        lambda state: state[0][0, 0] != 0,
        again,
        (some, start + SLOTS, jnp.zeros((n, gain.shape[1] // chips), jnp.bfloat16)),
    )
    rows, more, weight = lax.optimization_barrier((rows, more, weight))
    found, weight = spread(rows, gain, weight)
    other = lax.ppermute(weight, "c", [(0, 1), (1, 0)])
    own = weight
    parts = pl.pallas_call(
        head_kernel,
        out_shape=shape((chips, n, BLOCK), jnp.float32),
        in_specs=[VMEM] * 5,
        out_specs=VMEM,
        compiler_params=limit(16),
        name="head",
    )(lengths, found, more, own, other)
    logits = jnp.sum(exchange(parts.astype(jnp.float16), CHIPS).astype(jnp.float32), axis=0)
    line = pl.pallas_call(
        functools.partial(stats_kernel, vocab - half, vocab),
        out_shape=shape((lax.axis_size(ALL), 2 * n), jnp.float32),
        in_specs=[VMEM, VMEM],
        out_specs=VMEM,
        compiler_params=limit(4),
        name="stats",
    )(logits, targets)
    lines = exchange(line, ALL)
    out = pl.pallas_call(
        join_kernel,
        out_shape=shape((1, n), jnp.float32),
        in_specs=[VMEM],
        out_specs=VMEM,
        compiler_params=limit(4),
        name="join",
    )(lines)
    return out[0]


def solution(mesh):
    split = Mesh(mesh.devices.reshape(4, 4, 2, mesh.shape["tp"]), ALL)
    return jax.shard_map(
        local,
        mesh=split,
        in_specs=(P(CP, "z"), P(), P(), P(), P(CP, "z")),
        out_specs=P(),
        check_vma=False,
    )
```

```python
import functools

import jax
import jax.numpy as jnp
from jax import lax
from jax.experimental import pallas as pl
from jax.experimental.pallas import tpu as pltpu
from jax.sharding import Mesh
from jax.sharding import PartitionSpec as P

CHIPS = ("x", "y")
CP = ("x", "y", "c")
ALL = ("x", "y", "c", "z")
SLOTS = 8
BLOCK = 512
NEG = -1e30

VMEM = pl.BlockSpec(memory_space=pltpu.VMEM)
HBM = pl.BlockSpec(memory_space=pltpu.HBM)
SMEM = pl.BlockSpec(memory_space=pltpu.SMEM)
MIB = 1 << 20


def limit(mib):
    return pltpu.CompilerParams(vmem_limit_bytes=mib * MIB)


def iota(shape, dim):
    return lax.broadcasted_iota(jnp.int32, shape, dim).astype(jnp.float32)


def total(x, axis):
    return jnp.sum(x, axis=axis, keepdims=True)


def place():
    return (lax.axis_index("x") * lax.axis_size("y") + lax.axis_index("y")) * lax.axis_size(
        "c"
    ) + lax.axis_index("c")


def as_column(row):
    n = row.shape[1]
    return total(jnp.where(iota((n, n), 0) == iota((n, n), 1), row, 0.0), 1)


def ends_of(lengths_ref):
    row = lengths_ref[...].astype(jnp.float32)
    n = row.shape[1]
    down, across = iota((n, n), 0), iota((n, n), 1)
    column = total(jnp.where(across <= down, row, 0.0), 1) - 1.0
    return total(jnp.where(down <= across, as_column(row), 0.0), 0) - 1.0, column


def pick_kernel(lengths_ref, *refs):
    *first_ref, hidden_ref, out_ref, more_ref, lengths, hidden, sems = refs
    small = pltpu.make_async_copy(lengths_ref, lengths, sems.at[0])
    large = pltpu.make_async_copy(hidden_ref, hidden, sems.at[1])
    small.start()
    large.start()
    first = first_ref[0][0, 0] if first_ref else jnp.int32(0)
    small.wait()
    n, rows_here = lengths.shape[1], hidden.shape[0]
    ends, _ = ends_of(lengths)
    counts = total(jnp.where(jnp.floor(ends / rows_here) == iota((32, n), 0), 1.0, 0.0), 1)
    most = jnp.max(counts).astype(jnp.int32)
    more_ref[0, 0] = (most > first + SLOTS).astype(jnp.int32)
    base = (place() * rows_here).astype(jnp.float32)
    owned = (ends >= base) & (ends < base + rows_here)
    before = total(jnp.where(ends < base, 1.0, 0.0), 1)
    slot = iota((1, n), 1) - before - first.astype(jnp.float32)
    wanted = owned & (slot == iota((SLOTS, n), 0))
    at = total(jnp.where(wanted, ends - base + 1.0, 0.0), 1) - 1.0
    selector = (at == iota((SLOTS, rows_here), 1)).astype(jnp.bfloat16)
    large.wait()
    picked = jnp.dot(selector, hidden[...], preferred_element_type=jnp.float32)
    picked = picked.astype(jnp.bfloat16)
    for peer in range(out_ref.shape[0]):
        out_ref[peer] = picked


def norm_kernel(rows_ref, gain_ref, out_ref):
    parts, _, width = rows_ref.shape
    squares = jnp.zeros((SLOTS, 1), jnp.float32)
    for part in range(parts):
        values = rows_ref[part].astype(jnp.float32)
        squares = squares + total(values * values, 1)
    scale = jnp.sqrt(squares / (parts * width) + 1e-05)
    chips, cores, _, block = out_ref.shape
    for chip in range(chips):
        part, at = divmod(chip * block, width)
        values = rows_ref[part, :, at : at + block].astype(jnp.float32)
        gain = gain_ref[:, chip * block : (chip + 1) * block]
        normed = (values * gain / scale).astype(jnp.bfloat16)
        for core in range(cores):
            out_ref[chip, core] = normed


def rows_in_order(lengths_ref, found_ref, first=0.0):
    n = lengths_ref.shape[1]
    places = found_ref.shape[0]
    rows = 512
    ends_row, ends = ends_of(lengths_ref)
    owner = jnp.floor(ends / rows)
    before = total(jnp.where(ends_row < owner * rows, 1.0, 0.0), 1)
    slot = iota((n, 1), 0) - before - first
    inside = (slot >= 0.0) & (slot < SLOTS)
    at = jnp.where(inside, owner * SLOTS + slot, -1.0)
    selector = (at == iota((n, places), 1)).astype(jnp.bfloat16)
    return jnp.dot(selector, found_ref[...], preferred_element_type=jnp.float32)


def order_kernel(lengths_ref, first_ref, found_ref, more_ref, next_ref, out_ref):
    next_ref[0, 0] = first_ref[0, 0] + SLOTS
    first = first_ref[0, 0].astype(jnp.float32)
    rows = rows_in_order(lengths_ref, found_ref, first)
    out_ref[...] = more_ref[...] + rows.astype(jnp.bfloat16)


def head_kernel(lengths_ref, found_ref, more_ref, weight_ref, other_ref, out_ref):
    width = weight_ref.shape[1]
    blocks = out_ref.shape[0]
    start = lax.axis_index("c") * (weight_ref.shape[0] - blocks * BLOCK)
    first = lax.axis_index("c") == 0
    rows = rows_in_order(lengths_ref, found_ref).astype(jnp.bfloat16) + more_ref[...]
    low, high = rows[:, :width], rows[:, width:]
    left = jnp.concatenate([jnp.where(first, low, high), jnp.where(first, high, low)], axis=1)
    for block in range(blocks):
        span = pl.ds(pl.multiple_of(start + block * BLOCK, 16), BLOCK)
        weight = jnp.concatenate([weight_ref[span, :], other_ref[span, :]], axis=1)
        part = lax.dot_general(
            left, weight, (((1,), (1,)), ((), ())), preferred_element_type=jnp.float32
        )
        out_ref[block] = part.astype(out_ref.dtype)


def stats_kernel(spare, vocab, logits_ref, targets_ref, out_ref):
    logits = logits_ref[...]
    n, block = logits.shape
    core = lax.axis_index("c")
    chip = lax.axis_index("x") * lax.axis_size("y") + lax.axis_index("y")
    start = (core * spare + chip * block).astype(jnp.float32)
    column = iota((1, block), 1) + start
    half = vocab - spare
    valid = column >= (core * half).astype(jnp.float32)
    shift = (lax.axis_index("z") * vocab).astype(jnp.float32)
    wanted = as_column(targets_ref[...].astype(jnp.float32)) - shift
    found = total(jnp.where(valid & (column == wanted), logits, 0.0), 1)
    logits = jnp.where(valid, logits, NEG)
    top = jnp.max(logits, axis=1, keepdims=True)
    both = top + jnp.log(total(jnp.exp(logits - top), 1))
    down, across = iota((n, 2 * n), 0), iota((n, 2 * n), 1)
    line = jnp.where(across == down, both, 0.0) + jnp.where(across == down + n, found, 0.0)
    out_ref[...] = jnp.broadcast_to(total(line, 0), out_ref.shape)


def join_kernel(found_ref, out_ref):
    n = out_ref.shape[1]
    lines = found_ref[...]
    top = jnp.max(lines, axis=0, keepdims=True)
    both = top + jnp.log(total(jnp.exp(lines - top), 0))
    chosen = total(lines, 0)
    out_ref[...] = chosen[:, n:] - both[:, :n]


def shape(dims, dtype):
    return jax.ShapeDtypeStruct(dims, dtype)


def in_hbm(x):
    return pltpu.with_memory_space_constraint(x, pltpu.HBM)


def exchange(x, axes):
    return lax.all_to_all(x, axes, split_axis=0, concat_axis=0, tiled=True)


def picked(lengths, first, hidden):
    return pl.pallas_call(
        pick_kernel,
        out_shape=(
            shape((lax.axis_size("z"), SLOTS, hidden.shape[1]), hidden.dtype),
            pltpu.SMEM((1, 1), jnp.int32),
        ),
        in_specs=[HBM] + [SMEM] * len(first) + [HBM],
        out_specs=(VMEM, SMEM),
        scratch_shapes=[
            pltpu.VMEM(lengths.shape, lengths.dtype),
            pltpu.VMEM(hidden.shape, hidden.dtype),
            pltpu.SemaphoreType.DMA((2,)),
        ],
        compiler_params=limit(4),
        cost_estimate=pl.CostEstimate(flops=10**10, bytes_accessed=1 << 25, transcendentals=0),
        name="pick",
    )(in_hbm(lengths), *first, in_hbm(hidden))


def spread(rows, gain, after=()):
    chips, cores = lax.axis_size(CHIPS), lax.axis_size("c")
    width = gain.shape[1] // chips
    rows, after = lax.optimization_barrier((exchange(rows, "z"), after))
    normed = pl.pallas_call(
        norm_kernel,
        out_shape=shape((chips, cores, SLOTS, width), jnp.bfloat16),
        in_specs=[VMEM, VMEM],
        out_specs=VMEM,
        compiler_params=limit(4),
        cost_estimate=pl.CostEstimate(flops=10**10, bytes_accessed=1 << 25, transcendentals=0),
        name="norm",
    )(rows, gain)
    return exchange(normed.reshape(chips * cores * SLOTS, width), CP), after


def local(hidden, lengths, targets, norm_gain, lm_weight):
    n = lengths.shape[0]
    lengths, targets, gain = lengths[None], targets[None], norm_gain[None]
    weight = lm_weight.T
    vocab, depth = weight.shape
    chips = lax.axis_size(CHIPS)
    half = chips * BLOCK
    start = jnp.zeros((1, 1), jnp.int32)
    rows, some = picked(lengths, (), hidden)

    def again(state):
        _, first, more = state
        rows, some = picked(lengths, (first,), hidden)
        found = spread(rows, gain)[0]
        first, more = pl.pallas_call(
            order_kernel,
            out_shape=(shape(first.shape, first.dtype), shape(more.shape, more.dtype)),
            in_specs=[VMEM, SMEM, VMEM, VMEM],
            out_specs=(SMEM, VMEM),
            input_output_aliases={1: 0, 3: 1},
            compiler_params=limit(4),
            name="order",
        )(lengths, first, found, more)
        return some[0, 0], first, more

    _, _, more = lax.while_loop(
        lambda state: state[0] != 0,
        again,
        (some[0, 0], start + SLOTS, jnp.zeros((n, gain.shape[1] // chips), jnp.bfloat16)),
    )
    rows, more, weight = lax.optimization_barrier((rows, more, weight))
    found, weight = spread(rows, gain, weight)
    other = lax.ppermute(weight, "c", [(0, 1), (1, 0)])
    own = weight
    parts = pl.pallas_call(
        head_kernel,
        out_shape=shape((chips, n, BLOCK), jnp.float32),
        in_specs=[VMEM] * 5,
        out_specs=VMEM,
        compiler_params=limit(16),
        name="head",
    )(lengths, found, more, own, other)
    logits = jnp.sum(exchange(parts.astype(jnp.float16), CHIPS).astype(jnp.float32), axis=0)
    line = pl.pallas_call(
        functools.partial(stats_kernel, vocab - half, vocab),
        out_shape=shape((lax.axis_size(ALL), 2 * n), jnp.float32),
        in_specs=[VMEM, VMEM],
        out_specs=VMEM,
        compiler_params=limit(4),
        name="stats",
    )(logits, targets)
    lines = exchange(line, ALL)
    out = pl.pallas_call(
        join_kernel,
        out_shape=shape((1, n), jnp.float32),
        in_specs=[VMEM],
        out_specs=VMEM,
        compiler_params=limit(4),
        name="join",
    )(lines)
    return out[0]


def solution(mesh):
    split = Mesh(mesh.devices.reshape(4, 4, 2, mesh.shape["tp"]), ALL)
    return jax.shard_map(
        local,
        mesh=split,
        in_specs=(P(CP, "z"), P(), P(), P(), P(CP, "z")),
        out_specs=P(),
        check_vma=False,
    )
```

```python
import functools

import jax
import jax.numpy as jnp
from jax import lax
from jax.experimental import pallas as pl
from jax.experimental.pallas import tpu as pltpu
from jax.sharding import Mesh
from jax.sharding import PartitionSpec as P

CHIPS = ("x", "y")
LINE = ("c", "z")
CP = ("x", "y", "c")
ALL = ("x", "y", "c", "z")
SLOTS = 8
BLOCK = 512
NEG = -1e30

VMEM = pl.BlockSpec(memory_space=pltpu.VMEM)
HBM = pl.BlockSpec(memory_space=pltpu.HBM)
SMEM = pl.BlockSpec(memory_space=pltpu.SMEM)
MIB = 1 << 20


def limit(mib):
    return pltpu.CompilerParams(vmem_limit_bytes=mib * MIB)


def iota(shape, dim):
    return lax.broadcasted_iota(jnp.int32, shape, dim).astype(jnp.float32)


def total(x, axis):
    return jnp.sum(x, axis=axis, keepdims=True)


def place():
    return (lax.axis_index("x") * lax.axis_size("y") + lax.axis_index("y")) * lax.axis_size(
        "c"
    ) + lax.axis_index("c")


def as_column(row):
    n = row.shape[1]
    return total(jnp.where(iota((n, n), 0) == iota((n, n), 1), row, 0.0), 1)


def ends_of(lengths_ref):
    row = lengths_ref[...].astype(jnp.float32)
    n = row.shape[1]
    down, across = iota((n, n), 0), iota((n, n), 1)
    column = total(jnp.where(across <= down, row, 0.0), 1) - 1.0
    return total(jnp.where(down <= across, as_column(row), 0.0), 0) - 1.0, column


def pick_kernel(lengths_ref, *refs):
    *first_ref, hidden_ref, out_ref, more_ref, lengths, hidden, sems = refs
    small = pltpu.make_async_copy(lengths_ref, lengths, sems.at[0])
    large = pltpu.make_async_copy(hidden_ref, hidden, sems.at[1])
    small.start()
    large.start()
    first = first_ref[0][0, 0] if first_ref else jnp.int32(0)
    small.wait()
    n, rows_here = lengths.shape[1], hidden.shape[0]
    ends, _ = ends_of(lengths)
    counts = total(jnp.where(jnp.floor(ends / rows_here) == iota((32, n), 0), 1.0, 0.0), 1)
    most = jnp.max(counts).astype(jnp.int32)
    more_ref[0, 0] = (most > first + SLOTS).astype(jnp.int32)
    base = (place() * rows_here).astype(jnp.float32)
    owned = (ends >= base) & (ends < base + rows_here)
    before = total(jnp.where(ends < base, 1.0, 0.0), 1)
    slot = iota((1, n), 1) - before - first.astype(jnp.float32)
    wanted = owned & (slot == iota((SLOTS, n), 0))
    at = total(jnp.where(wanted, ends - base + 1.0, 0.0), 1) - 1.0
    selector = (at == iota((SLOTS, rows_here), 1)).astype(jnp.bfloat16)
    large.wait()
    picked = jnp.dot(selector, hidden[...], preferred_element_type=jnp.float32)
    picked = picked.astype(jnp.bfloat16)
    for peer in range(out_ref.shape[0]):
        out_ref[peer] = picked


def norm_kernel(rows_ref, gain_ref, out_ref):
    cores, parts, _, width = rows_ref.shape
    chips, _, block = out_ref.shape
    for core in range(cores):
        squares = jnp.zeros((SLOTS, 1), jnp.float32)
        for part in range(parts):
            values = rows_ref[core, part].astype(jnp.float32)
            squares = squares + total(values * values, 1)
        scale = jnp.sqrt(squares / (parts * width) + 1e-05)
        for chip in range(chips):
            part, at = divmod(chip * block, width)
            values = rows_ref[core, part, :, at : at + block].astype(jnp.float32)
            gain = gain_ref[:, chip * block : (chip + 1) * block]
            normed = (values * gain / scale).astype(jnp.bfloat16)
            out_ref[chip, core * SLOTS : (core + 1) * SLOTS] = normed


def rows_in_order(lengths_ref, found_ref, first=0.0):
    n = lengths_ref.shape[1]
    places = found_ref.shape[0]
    rows = 512
    ends_row, ends = ends_of(lengths_ref)
    owner = jnp.floor(ends / rows)
    before = total(jnp.where(ends_row < owner * rows, 1.0, 0.0), 1)
    slot = iota((n, 1), 0) - before - first
    inside = (slot >= 0.0) & (slot < SLOTS)
    at = jnp.where(inside, owner * SLOTS + slot, -1.0)
    selector = (at == iota((n, places), 1)).astype(jnp.bfloat16)
    return jnp.dot(selector, found_ref[...], preferred_element_type=jnp.float32)


def order_kernel(lengths_ref, first_ref, found_ref, more_ref, next_ref, out_ref):
    next_ref[0, 0] = first_ref[0, 0] + SLOTS
    first = first_ref[0, 0].astype(jnp.float32)
    rows = rows_in_order(lengths_ref, found_ref, first)
    out_ref[...] = more_ref[...] + rows.astype(jnp.bfloat16)


def head_kernel(lengths_ref, found_ref, more_ref, weight_ref, other_ref, out_ref):
    width = weight_ref.shape[1]
    blocks = out_ref.shape[0]
    start = lax.axis_index("c") * (weight_ref.shape[0] - blocks * BLOCK)
    first = lax.axis_index("c") == 0
    rows = rows_in_order(lengths_ref, found_ref).astype(jnp.bfloat16) + more_ref[...]
    low, high = rows[:, :width], rows[:, width:]
    left = jnp.concatenate([jnp.where(first, low, high), jnp.where(first, high, low)], axis=1)
    for block in range(blocks):
        span = pl.ds(pl.multiple_of(start + block * BLOCK, 16), BLOCK)
        weight = jnp.concatenate([weight_ref[span, :], other_ref[span, :]], axis=1)
        part = lax.dot_general(
            left, weight, (((1,), (1,)), ((), ())), preferred_element_type=jnp.float32
        )
        out_ref[block] = part.astype(out_ref.dtype)


def stats_kernel(spare, vocab, logits_ref, targets_ref, out_ref):
    logits = logits_ref[...]
    n, block = logits.shape
    core = lax.axis_index("c")
    chip = lax.axis_index("x") * lax.axis_size("y") + lax.axis_index("y")
    start = (core * spare + chip * block).astype(jnp.float32)
    column = iota((1, block), 1) + start
    half = vocab - spare
    valid = column >= (core * half).astype(jnp.float32)
    shift = (lax.axis_index("z") * vocab).astype(jnp.float32)
    wanted = as_column(targets_ref[...].astype(jnp.float32)) - shift
    found = total(jnp.where(valid & (column == wanted), logits, 0.0), 1)
    logits = jnp.where(valid, logits, NEG)
    top = jnp.max(logits, axis=1, keepdims=True)
    both = top + jnp.log(total(jnp.exp(logits - top), 1))
    down, across = iota((n, 2 * n), 0), iota((n, 2 * n), 1)
    line = jnp.where(across == down, both, 0.0) + jnp.where(across == down + n, found, 0.0)
    out_ref[...] = jnp.broadcast_to(total(line, 0), out_ref.shape)


def join_kernel(found_ref, out_ref):
    n = out_ref.shape[1]
    lines = found_ref[...]
    top = jnp.max(lines, axis=0, keepdims=True)
    both = top + jnp.log(total(jnp.exp(lines - top), 0))
    chosen = total(lines, 0)
    out_ref[...] = chosen[:, n:] - both[:, :n]


def shape(dims, dtype):
    return jax.ShapeDtypeStruct(dims, dtype)


def in_hbm(x):
    return pltpu.with_memory_space_constraint(x, pltpu.HBM)


def exchange(x, axes):
    return lax.all_to_all(x, axes, split_axis=0, concat_axis=0, tiled=True)


def picked(lengths, first, hidden):
    return pl.pallas_call(
        pick_kernel,
        out_shape=(
            shape((lax.axis_size(LINE), SLOTS, hidden.shape[1]), hidden.dtype),
            pltpu.SMEM((1, 1), jnp.int32),
        ),
        in_specs=[HBM] + [SMEM] * len(first) + [HBM],
        out_specs=(VMEM, SMEM),
        scratch_shapes=[
            pltpu.VMEM(lengths.shape, lengths.dtype),
            pltpu.VMEM(hidden.shape, hidden.dtype),
            pltpu.SemaphoreType.DMA((2,)),
        ],
        compiler_params=limit(4),
        cost_estimate=pl.CostEstimate(flops=10**10, bytes_accessed=1 << 25, transcendentals=0),
        name="pick",
    )(in_hbm(lengths), *first, in_hbm(hidden))


def spread(rows, gain, after=()):
    chips, cores = lax.axis_size(CHIPS), lax.axis_size("c")
    width = gain.shape[1] // chips
    rows, after = lax.optimization_barrier((exchange(rows, LINE), after))
    rows = rows.reshape(cores, -1, *rows.shape[1:])
    normed = pl.pallas_call(
        norm_kernel,
        out_shape=shape((chips, cores * SLOTS, width), jnp.bfloat16),
        in_specs=[VMEM, VMEM],
        out_specs=VMEM,
        compiler_params=limit(4),
        cost_estimate=pl.CostEstimate(flops=10**10, bytes_accessed=1 << 25, transcendentals=0),
        name="norm",
    )(rows, gain)
    return exchange(normed.reshape(chips * cores * SLOTS, width), CHIPS), after


def local(hidden, lengths, targets, norm_gain, lm_weight):
    n = lengths.shape[0]
    lengths, targets, gain = lengths[None], targets[None], norm_gain[None]
    weight = lm_weight.T
    vocab, depth = weight.shape
    chips = lax.axis_size(CHIPS)
    half = chips * BLOCK
    start = jnp.zeros((1, 1), jnp.int32)
    rows, some = picked(lengths, (), hidden)

    def again(state):
        _, first, more = state
        rows, some = picked(lengths, (first,), hidden)
        found = spread(rows, gain)[0]
        first, more = pl.pallas_call(
            order_kernel,
            out_shape=(shape(first.shape, first.dtype), shape(more.shape, more.dtype)),
            in_specs=[VMEM, SMEM, VMEM, VMEM],
            out_specs=(SMEM, VMEM),
            input_output_aliases={1: 0, 3: 1},
            compiler_params=limit(4),
            name="order",
        )(lengths, first, found, more)
        return some[0, 0], first, more

    _, _, more = lax.while_loop(
        lambda state: state[0] != 0,
        again,
        (some[0, 0], start + SLOTS, jnp.zeros((n, gain.shape[1] // chips), jnp.bfloat16)),
    )
    rows, more, weight = lax.optimization_barrier((rows, more, weight))
    found, weight = spread(rows, gain, weight)
    other = lax.ppermute(weight, "c", [(0, 1), (1, 0)])
    own = weight
    parts = pl.pallas_call(
        head_kernel,
        out_shape=shape((chips, n, BLOCK), jnp.float32),
        in_specs=[VMEM] * 5,
        out_specs=VMEM,
        compiler_params=limit(16),
        name="head",
    )(lengths, found, more, own, other)
    logits = jnp.sum(exchange(parts.astype(jnp.float16), CHIPS).astype(jnp.float32), axis=0)
    line = pl.pallas_call(
        functools.partial(stats_kernel, vocab - half, vocab),
        out_shape=shape((lax.axis_size(ALL), 2 * n), jnp.float32),
        in_specs=[VMEM, VMEM],
        out_specs=VMEM,
        compiler_params=limit(4),
        name="stats",
    )(logits, targets)
    lines = exchange(line, ALL)
    out = pl.pallas_call(
        join_kernel,
        out_shape=shape((1, n), jnp.float32),
        in_specs=[VMEM],
        out_specs=VMEM,
        compiler_params=limit(4),
        name="join",
    )(lines)
    return out[0]


def solution(mesh):
    split = Mesh(mesh.devices.reshape(4, 4, 2, mesh.shape["tp"]), ALL)
    return jax.shard_map(
        local,
        mesh=split,
        in_specs=(P(CP, "z"), P(), P(), P(), P(CP, "z")),
        out_specs=P(),
        check_vma=False,
    )
```

```python
import functools

import jax
import jax.numpy as jnp
from jax import lax
from jax.experimental import pallas as pl
from jax.experimental.pallas import tpu as pltpu
from jax.sharding import Mesh
from jax.sharding import PartitionSpec as P

CHIPS = ("x", "y")
CP = ("x", "y", "c")
ALL = ("x", "y", "c", "z")
SLOTS = 8
ORDER = [5, 6, 7, 0, 1, 2, 3, 4]
BLOCK = 512
NEG = -1e30

VMEM = pl.BlockSpec(memory_space=pltpu.VMEM)
HBM = pl.BlockSpec(memory_space=pltpu.HBM)
SMEM = pl.BlockSpec(memory_space=pltpu.SMEM)
MIB = 1 << 20


def limit(mib):
    return pltpu.CompilerParams(vmem_limit_bytes=mib * MIB)


def iota(shape, dim):
    return lax.broadcasted_iota(jnp.int32, shape, dim).astype(jnp.float32)


def total(x, axis):
    return jnp.sum(x, axis=axis, keepdims=True)


def place():
    return (lax.axis_index("x") * lax.axis_size("y") + lax.axis_index("y")) * lax.axis_size(
        "c"
    ) + lax.axis_index("c")


def as_column(row):
    n = row.shape[1]
    return total(jnp.where(iota((n, n), 0) == iota((n, n), 1), row, 0.0), 1)


def ends_of(lengths_ref):
    row = lengths_ref[...].astype(jnp.float32)
    n = row.shape[1]
    down, across = iota((n, n), 0), iota((n, n), 1)
    column = total(jnp.where(across <= down, row, 0.0), 1) - 1.0
    return total(jnp.where(down <= across, as_column(row), 0.0), 0) - 1.0, column


def pick_kernel(lengths_ref, *refs):
    *first_ref, hidden_ref, out_ref, more_ref, lengths, hidden, sems = refs
    small = pltpu.make_async_copy(lengths_ref, lengths, sems.at[0])
    large = pltpu.make_async_copy(hidden_ref, hidden, sems.at[1])
    small.start()
    large.start()
    first = first_ref[0][0, 0] if first_ref else jnp.int32(0)
    small.wait()
    n, rows_here = lengths.shape[1], hidden.shape[0]
    ends, _ = ends_of(lengths)
    counts = total(jnp.where(jnp.floor(ends / rows_here) == iota((32, n), 0), 1.0, 0.0), 1)
    most = jnp.max(counts).astype(jnp.int32)
    more_ref[0, 0] = (most > first + SLOTS).astype(jnp.int32)
    base = (place() * rows_here).astype(jnp.float32)
    owned = (ends >= base) & (ends < base + rows_here)
    before = total(jnp.where(ends < base, 1.0, 0.0), 1)
    slot = iota((1, n), 1) - before - first.astype(jnp.float32)
    wanted = owned & (slot == iota((SLOTS, n), 0))
    at = total(jnp.where(wanted, ends - base + 1.0, 0.0), 1) - 1.0
    selector = (at == iota((SLOTS, rows_here), 1)).astype(jnp.bfloat16)
    large.wait()
    picked = jnp.dot(selector, hidden[...], preferred_element_type=jnp.float32)
    picked = picked.astype(jnp.bfloat16)
    for peer in range(out_ref.shape[0]):
        out_ref[peer] = picked


def norm_kernel(rows_ref, gain_ref, out_ref):
    parts, _, width = rows_ref.shape
    squares = jnp.zeros((SLOTS, 1), jnp.float32)
    for part in range(parts):
        values = rows_ref[part].astype(jnp.float32)
        squares = squares + total(values * values, 1)
    scale = jnp.sqrt(squares / (parts * width) + 1e-05)
    chips, cores, _, block = out_ref.shape
    for chip in range(chips):
        part, at = divmod(chip * block, width)
        part = ORDER.index(part)
        values = rows_ref[part, :, at : at + block].astype(jnp.float32)
        gain = gain_ref[:, chip * block : (chip + 1) * block]
        normed = (values * gain / scale).astype(jnp.bfloat16)
        for core in range(cores):
            out_ref[chip, core] = normed


def rows_in_order(lengths_ref, found_ref, first=0.0):
    n = lengths_ref.shape[1]
    places = found_ref.shape[0]
    rows = 512
    ends_row, ends = ends_of(lengths_ref)
    owner = jnp.floor(ends / rows)
    before = total(jnp.where(ends_row < owner * rows, 1.0, 0.0), 1)
    slot = iota((n, 1), 0) - before - first
    inside = (slot >= 0.0) & (slot < SLOTS)
    at = jnp.where(inside, owner * SLOTS + slot, -1.0)
    selector = (at == iota((n, places), 1)).astype(jnp.bfloat16)
    return jnp.dot(selector, found_ref[...], preferred_element_type=jnp.float32)


def order_kernel(lengths_ref, first_ref, found_ref, more_ref, next_ref, out_ref):
    next_ref[0, 0] = first_ref[0, 0] + SLOTS
    first = first_ref[0, 0].astype(jnp.float32)
    rows = rows_in_order(lengths_ref, found_ref, first)
    out_ref[...] = more_ref[...] + rows.astype(jnp.bfloat16)


def head_kernel(lengths_ref, found_ref, more_ref, weight_ref, other_ref, out_ref):
    width = weight_ref.shape[1]
    blocks = out_ref.shape[0]
    start = lax.axis_index("c") * (weight_ref.shape[0] - blocks * BLOCK)
    first = lax.axis_index("c") == 0
    rows = rows_in_order(lengths_ref, found_ref).astype(jnp.bfloat16) + more_ref[...]
    low, high = rows[:, :width], rows[:, width:]
    left = jnp.concatenate([jnp.where(first, low, high), jnp.where(first, high, low)], axis=1)
    for block in range(blocks):
        span = pl.ds(pl.multiple_of(start + block * BLOCK, 16), BLOCK)
        weight = jnp.concatenate([weight_ref[span, :], other_ref[span, :]], axis=1)
        part = lax.dot_general(
            left, weight, (((1,), (1,)), ((), ())), preferred_element_type=jnp.float32
        )
        out_ref[block] = part.astype(out_ref.dtype)


def stats_kernel(spare, vocab, logits_ref, targets_ref, out_ref):
    logits = logits_ref[...]
    n, block = logits.shape
    core = lax.axis_index("c")
    chip = lax.axis_index("x") * lax.axis_size("y") + lax.axis_index("y")
    start = (core * spare + chip * block).astype(jnp.float32)
    column = iota((1, block), 1) + start
    half = vocab - spare
    valid = column >= (core * half).astype(jnp.float32)
    shift = (lax.axis_index("z") * vocab).astype(jnp.float32)
    wanted = as_column(targets_ref[...].astype(jnp.float32)) - shift
    found = total(jnp.where(valid & (column == wanted), logits, 0.0), 1)
    logits = jnp.where(valid, logits, NEG)
    top = jnp.max(logits, axis=1, keepdims=True)
    both = top + jnp.log(total(jnp.exp(logits - top), 1))
    down, across = iota((n, 2 * n), 0), iota((n, 2 * n), 1)
    line = jnp.where(across == down, both, 0.0) + jnp.where(across == down + n, found, 0.0)
    out_ref[...] = jnp.broadcast_to(total(line, 0), out_ref.shape)


def join_kernel(found_ref, out_ref):
    n = out_ref.shape[1]
    lines = found_ref[...]
    top = jnp.max(lines, axis=0, keepdims=True)
    both = top + jnp.log(total(jnp.exp(lines - top), 0))
    chosen = total(lines, 0)
    out_ref[...] = chosen[:, n:] - both[:, :n]


def shape(dims, dtype):
    return jax.ShapeDtypeStruct(dims, dtype)


def in_hbm(x):
    return pltpu.with_memory_space_constraint(x, pltpu.HBM)


def exchange(x, axes, groups=None):
    return lax.all_to_all(
        x, axes, split_axis=0, concat_axis=0, tiled=True, axis_index_groups=groups
    )


def picked(lengths, first, hidden):
    return pl.pallas_call(
        pick_kernel,
        out_shape=(
            shape((lax.axis_size("z"), SLOTS, hidden.shape[1]), hidden.dtype),
            pltpu.SMEM((1, 1), jnp.int32),
        ),
        in_specs=[HBM] + [SMEM] * len(first) + [HBM],
        out_specs=(VMEM, SMEM),
        scratch_shapes=[
            pltpu.VMEM(lengths.shape, lengths.dtype),
            pltpu.VMEM(hidden.shape, hidden.dtype),
            pltpu.SemaphoreType.DMA((2,)),
        ],
        compiler_params=limit(4),
        cost_estimate=pl.CostEstimate(flops=10**10, bytes_accessed=1 << 25, transcendentals=0),
        name="pick",
    )(in_hbm(lengths), *first, in_hbm(hidden))


def spread(rows, gain, after=()):
    chips, cores = lax.axis_size(CHIPS), lax.axis_size("c")
    width = gain.shape[1] // chips
    rows, after = lax.optimization_barrier((exchange(rows, "z", [ORDER]), after))
    normed = pl.pallas_call(
        norm_kernel,
        out_shape=shape((chips, cores, SLOTS, width), jnp.bfloat16),
        in_specs=[VMEM, VMEM],
        out_specs=VMEM,
        compiler_params=limit(4),
        cost_estimate=pl.CostEstimate(flops=10**10, bytes_accessed=1 << 25, transcendentals=0),
        name="norm",
    )(rows, gain)
    return exchange(normed.reshape(chips * cores * SLOTS, width), CP), after


def local(hidden, lengths, targets, norm_gain, lm_weight):
    n = lengths.shape[0]
    lengths, targets, gain = lengths[None], targets[None], norm_gain[None]
    weight = lm_weight.T
    vocab, depth = weight.shape
    chips = lax.axis_size(CHIPS)
    half = chips * BLOCK
    start = jnp.zeros((1, 1), jnp.int32)
    rows, some = picked(lengths, (), hidden)

    def again(state):
        _, first, more = state
        rows, some = picked(lengths, (first,), hidden)
        found = spread(rows, gain)[0]
        first, more = pl.pallas_call(
            order_kernel,
            out_shape=(shape(first.shape, first.dtype), shape(more.shape, more.dtype)),
            in_specs=[VMEM, SMEM, VMEM, VMEM],
            out_specs=(SMEM, VMEM),
            input_output_aliases={1: 0, 3: 1},
            compiler_params=limit(4),
            name="order",
        )(lengths, first, found, more)
        return some[0, 0], first, more

    _, _, more = lax.while_loop(
        lambda state: state[0] != 0,
        again,
        (some[0, 0], start + SLOTS, jnp.zeros((n, gain.shape[1] // chips), jnp.bfloat16)),
    )
    rows, more, weight = lax.optimization_barrier((rows, more, weight))
    found, weight = spread(rows, gain, weight)
    other = lax.ppermute(weight, "c", [(0, 1), (1, 0)])
    own = weight
    parts = pl.pallas_call(
        head_kernel,
        out_shape=shape((chips, n, BLOCK), jnp.float32),
        in_specs=[VMEM] * 5,
        out_specs=VMEM,
        compiler_params=limit(16),
        name="head",
    )(lengths, found, more, own, other)
    logits = jnp.sum(exchange(parts.astype(jnp.float16), CHIPS).astype(jnp.float32), axis=0)
    line = pl.pallas_call(
        functools.partial(stats_kernel, vocab - half, vocab),
        out_shape=shape((lax.axis_size(ALL), 2 * n), jnp.float32),
        in_specs=[VMEM, VMEM],
        out_specs=VMEM,
        compiler_params=limit(4),
        name="stats",
    )(logits, targets)
    lines = exchange(line, ALL)
    out = pl.pallas_call(
        join_kernel,
        out_shape=shape((1, n), jnp.float32),
        in_specs=[VMEM],
        out_specs=VMEM,
        compiler_params=limit(4),
        name="join",
    )(lines)
    return out[0]


def solution(mesh):
    split = Mesh(mesh.devices.reshape(4, 4, 2, mesh.shape["tp"]), ALL)
    return jax.shard_map(
        local,
        mesh=split,
        in_specs=(P(CP, "z"), P(), P(), P(), P(CP, "z")),
        out_specs=P(),
        check_vma=False,
    )
```

```python
import functools

import jax
import jax.numpy as jnp
from jax import lax
from jax.experimental import pallas as pl
from jax.experimental.pallas import tpu as pltpu
from jax.sharding import Mesh
from jax.sharding import PartitionSpec as P

SLOTS = 8
SIDE = 4
CHIPS = SIDE * SIDE
CORES = 2
DEEP = 8
BLOCK = 512
NEG = -1e30

VMEM = pl.BlockSpec(memory_space=pltpu.VMEM)
HBM = pl.BlockSpec(memory_space=pltpu.HBM)
SMEM = pl.BlockSpec(memory_space=pltpu.SMEM)
MIB = 1 << 20


def limit(mib):
    return pltpu.CompilerParams(vmem_limit_bytes=mib * MIB)


def iota(shape, dim):
    return lax.broadcasted_iota(jnp.int32, shape, dim).astype(jnp.float32)


def total(x, axis):
    return jnp.sum(x, axis=axis, keepdims=True)


def chip_rank(chip):
    x, y = chip // SIDE, chip % SIDE
    return (x + SIDE // 2) % SIDE * SIDE + (y + SIDE // 2) % SIDE


PLANE = sorted(range(CHIPS), key=chip_rank)
COLUMN = [(k + DEEP // 2) % DEEP for k in range(DEEP)]
BOTH = [chip * CORES + core for chip in PLANE for core in (1, 0)]
EACH = [[chip * CORES + core for chip in PLANE] for core in (0, 1)]
WHOLE = [place * DEEP + z for place in BOTH for z in COLUMN]
PAIRS = [(place, place ^ 1) for place in range(CHIPS * CORES)]


def core_index():
    return lax.axis_index("q") & 1


def chip_index():
    return lax.axis_index("q") >> 1


def modulo(x, n):
    return x - n * jnp.floor(x / n)


def place_rank(place):
    chip = jnp.floor(place / CORES)
    x, y = jnp.floor(chip / SIDE), modulo(chip, SIDE)
    x, y = modulo(x + SIDE // 2, SIDE), modulo(y + SIDE // 2, SIDE)
    return (x * SIDE + y) * CORES + (1.0 - modulo(place, CORES))


def as_column(row):
    n = row.shape[1]
    return total(jnp.where(iota((n, n), 0) == iota((n, n), 1), row, 0.0), 1)


def ends_of(lengths_ref):
    row = lengths_ref[...].astype(jnp.float32)
    n = row.shape[1]
    down, across = iota((n, n), 0), iota((n, n), 1)
    column = total(jnp.where(across <= down, row, 0.0), 1) - 1.0
    return total(jnp.where(down <= across, as_column(row), 0.0), 0) - 1.0, column


def pick_kernel(lengths_ref, *refs):
    *first_ref, hidden_ref, out_ref, more_ref, lengths, hidden, sems = refs
    small = pltpu.make_async_copy(lengths_ref, lengths, sems.at[0])
    large = pltpu.make_async_copy(hidden_ref, hidden, sems.at[1])
    small.start()
    large.start()
    first = first_ref[0][0, 0] if first_ref else jnp.int32(0)
    small.wait()
    n, rows_here = lengths.shape[1], hidden.shape[0]
    ends, _ = ends_of(lengths)
    counts = total(jnp.where(jnp.floor(ends / rows_here) == iota((32, n), 0), 1.0, 0.0), 1)
    most = jnp.max(counts).astype(jnp.int32)
    more_ref[0, 0] = (most > first + SLOTS).astype(jnp.int32)
    base = (lax.axis_index("q") * rows_here).astype(jnp.float32)
    owned = (ends >= base) & (ends < base + rows_here)
    before = total(jnp.where(ends < base, 1.0, 0.0), 1)
    slot = iota((1, n), 1) - before - first.astype(jnp.float32)
    wanted = owned & (slot == iota((SLOTS, n), 0))
    at = total(jnp.where(wanted, ends - base + 1.0, 0.0), 1) - 1.0
    selector = (at == iota((SLOTS, rows_here), 1)).astype(jnp.bfloat16)
    large.wait()
    picked = jnp.dot(selector, hidden[...], preferred_element_type=jnp.float32)
    picked = picked.astype(jnp.bfloat16)
    for peer in range(out_ref.shape[0]):
        out_ref[peer] = picked


def norm_kernel(rows_ref, gain_ref, out_ref):
    parts, _, width = rows_ref.shape
    squares = jnp.zeros((SLOTS, 1), jnp.float32)
    for part in range(parts):
        values = rows_ref[part].astype(jnp.float32)
        squares = squares + total(values * values, 1)
    scale = jnp.sqrt(squares / (parts * width) + 1e-05)
    chips, cores, _, block = out_ref.shape
    for rank, chip in enumerate(PLANE):
        part, at = divmod(chip * block, width)
        part = COLUMN.index(part)
        values = rows_ref[part, :, at : at + block].astype(jnp.float32)
        gain = gain_ref[:, chip * block : (chip + 1) * block]
        normed = (values * gain / scale).astype(jnp.bfloat16)
        for core in range(cores):
            out_ref[rank, core] = normed


def rows_in_order(lengths_ref, found_ref, first=0.0):
    n = lengths_ref.shape[1]
    places = found_ref.shape[0]
    rows = 512
    ends_row, ends = ends_of(lengths_ref)
    owner = jnp.floor(ends / rows)
    before = total(jnp.where(ends_row < owner * rows, 1.0, 0.0), 1)
    slot = iota((n, 1), 0) - before - first
    inside = (slot >= 0.0) & (slot < SLOTS)
    at = jnp.where(inside, place_rank(owner) * SLOTS + slot, -1.0)
    selector = (at == iota((n, places), 1)).astype(jnp.bfloat16)
    return jnp.dot(selector, found_ref[...], preferred_element_type=jnp.float32)


def order_kernel(lengths_ref, first_ref, found_ref, more_ref, next_ref, out_ref):
    next_ref[0, 0] = first_ref[0, 0] + SLOTS
    first = first_ref[0, 0].astype(jnp.float32)
    rows = rows_in_order(lengths_ref, found_ref, first)
    out_ref[...] = more_ref[...] + rows.astype(jnp.bfloat16)


def head_kernel(lengths_ref, found_ref, more_ref, weight_ref, other_ref, out_ref):
    width = weight_ref.shape[1]
    blocks = out_ref.shape[0]
    start = core_index() * (weight_ref.shape[0] - blocks * BLOCK)
    first = core_index() == 0
    rows = rows_in_order(lengths_ref, found_ref).astype(jnp.bfloat16) + more_ref[...]
    low, high = rows[:, :width], rows[:, width:]
    left = jnp.concatenate([jnp.where(first, low, high), jnp.where(first, high, low)], axis=1)
    for block in range(blocks):
        span = pl.ds(pl.multiple_of(start + block * BLOCK, 16), BLOCK)
        weight = jnp.concatenate([weight_ref[span, :], other_ref[span, :]], axis=1)
        part = lax.dot_general(
            left, weight, (((1,), (1,)), ((), ())), preferred_element_type=jnp.float32
        )
        out_ref[block] = part.astype(out_ref.dtype)


def stats_kernel(spare, vocab, logits_ref, targets_ref, out_ref):
    logits = logits_ref[...]
    n, block = logits.shape
    core = core_index()
    chip = chip_index()
    x, y = chip >> 2, chip & (SIDE - 1)
    rank = ((x + SIDE // 2) & (SIDE - 1)) * SIDE + ((y + SIDE // 2) & (SIDE - 1))
    start = (core * spare + rank * block).astype(jnp.float32)
    column = iota((1, block), 1) + start
    half = vocab - spare
    valid = column >= (core * half).astype(jnp.float32)
    shift = (lax.axis_index("z") * vocab).astype(jnp.float32)
    wanted = as_column(targets_ref[...].astype(jnp.float32)) - shift
    found = total(jnp.where(valid & (column == wanted), logits, 0.0), 1)
    logits = jnp.where(valid, logits, NEG)
    top = jnp.max(logits, axis=1, keepdims=True)
    both = top + jnp.log(total(jnp.exp(logits - top), 1))
    down, across = iota((n, 2 * n), 0), iota((n, 2 * n), 1)
    line = jnp.where(across == down, both, 0.0) + jnp.where(across == down + n, found, 0.0)
    out_ref[...] = jnp.broadcast_to(total(line, 0), out_ref.shape)


def join_kernel(found_ref, out_ref):
    n = out_ref.shape[1]
    lines = found_ref[...]
    top = jnp.max(lines, axis=0, keepdims=True)
    both = top + jnp.log(total(jnp.exp(lines - top), 0))
    chosen = total(lines, 0)
    out_ref[...] = chosen[:, n:] - both[:, :n]


def shape(dims, dtype):
    return jax.ShapeDtypeStruct(dims, dtype)


def in_hbm(x):
    return pltpu.with_memory_space_constraint(x, pltpu.HBM)


def exchange(x, axis, groups):
    return lax.all_to_all(
        x, axis, split_axis=0, concat_axis=0, tiled=True, axis_index_groups=groups
    )


def picked(lengths, first, hidden):
    return pl.pallas_call(
        pick_kernel,
        out_shape=(
            shape((DEEP, SLOTS, hidden.shape[1]), hidden.dtype),
            pltpu.SMEM((1, 1), jnp.int32),
        ),
        in_specs=[HBM] + [SMEM] * len(first) + [HBM],
        out_specs=(VMEM, SMEM),
        scratch_shapes=[
            pltpu.VMEM(lengths.shape, lengths.dtype),
            pltpu.VMEM(hidden.shape, hidden.dtype),
            pltpu.SemaphoreType.DMA((2,)),
        ],
        compiler_params=limit(4),
        cost_estimate=pl.CostEstimate(flops=10**10, bytes_accessed=1 << 25, transcendentals=0),
        name="pick",
    )(in_hbm(lengths), *first, in_hbm(hidden))


def spread(rows, gain, after=()):
    chips, cores = CHIPS, CORES
    width = gain.shape[1] // chips
    rows, after = lax.optimization_barrier((exchange(rows, "z", [COLUMN]), after))
    normed = pl.pallas_call(
        norm_kernel,
        out_shape=shape((chips, cores, SLOTS, width), jnp.bfloat16),
        in_specs=[VMEM, VMEM],
        out_specs=VMEM,
        compiler_params=limit(4),
        cost_estimate=pl.CostEstimate(flops=10**10, bytes_accessed=1 << 25, transcendentals=0),
        name="norm",
    )(rows, gain)
    return exchange(normed.reshape(chips * cores * SLOTS, width), "q", [BOTH]), after


def local(hidden, lengths, targets, norm_gain, lm_weight):
    n = lengths.shape[0]
    lengths, targets, gain = lengths[None], targets[None], norm_gain[None]
    weight = lm_weight.T
    vocab, depth = weight.shape
    chips = CHIPS
    half = chips * BLOCK
    start = jnp.zeros((1, 1), jnp.int32)
    rows, some = picked(lengths, (), hidden)

    def again(state):
        _, first, more = state
        rows, some = picked(lengths, (first,), hidden)
        found = spread(rows, gain)[0]
        first, more = pl.pallas_call(
            order_kernel,
            out_shape=(shape(first.shape, first.dtype), shape(more.shape, more.dtype)),
            in_specs=[VMEM, SMEM, VMEM, VMEM],
            out_specs=(SMEM, VMEM),
            input_output_aliases={1: 0, 3: 1},
            compiler_params=limit(4),
            name="order",
        )(lengths, first, found, more)
        return some[0, 0], first, more

    _, _, more = lax.while_loop(
        lambda state: state[0] != 0,
        again,
        (some[0, 0], start + SLOTS, jnp.zeros((n, gain.shape[1] // chips), jnp.bfloat16)),
    )
    rows, more, weight = lax.optimization_barrier((rows, more, weight))
    found, weight = spread(rows, gain, weight)
    other = lax.ppermute(weight, "q", PAIRS)
    own = weight
    parts = pl.pallas_call(
        head_kernel,
        out_shape=shape((chips, n, BLOCK), jnp.float32),
        in_specs=[VMEM] * 5,
        out_specs=VMEM,
        compiler_params=limit(16),
        name="head",
    )(lengths, found, more, own, other)
    logits = jnp.sum(exchange(parts.astype(jnp.float16), "q", EACH).astype(jnp.float32), axis=0)
    return pl.pallas_call(
        functools.partial(stats_kernel, vocab - half, vocab),
        out_shape=shape((len(WHOLE), 2 * n), jnp.float32),
        in_specs=[VMEM, VMEM],
        out_specs=VMEM,
        compiler_params=limit(4),
        name="stats",
    )(logits, targets)


def joined(line):
    n = line.shape[1] // 2
    out = pl.pallas_call(
        join_kernel,
        out_shape=shape((1, n), jnp.float32),
        in_specs=[VMEM],
        out_specs=VMEM,
        compiler_params=limit(4),
        name="join",
    )(exchange(line, "d", [WHOLE]))
    return out[0]


def solution(mesh):
    devices = mesh.devices.reshape(CHIPS * CORES, DEEP)
    first = jax.shard_map(
        local,
        mesh=Mesh(devices, ("q", "z")),
        in_specs=(P("q", "z"), P(), P(), P(), P("q", "z")),
        out_specs=P(("q", "z")),
        check_vma=False,
    )
    last = jax.shard_map(
        joined,
        mesh=Mesh(devices.reshape(-1), ("d",)),
        in_specs=P("d"),
        out_specs=P(),
        check_vma=False,
    )
    return lambda *args: last(first(*args))
```

```python
import functools

import jax
import jax.numpy as jnp
from jax import lax
from jax.experimental import pallas as pl
from jax.experimental.pallas import tpu as pltpu
from jax.sharding import Mesh
from jax.sharding import PartitionSpec as P

SLOTS = 8
SIDE = 4
CHIPS = SIDE * SIDE
CORES = 2
DEEP = 8
BLOCK = 512
NEG = -1e30

VMEM = pl.BlockSpec(memory_space=pltpu.VMEM)
HBM = pl.BlockSpec(memory_space=pltpu.HBM)
SMEM = pl.BlockSpec(memory_space=pltpu.SMEM)
MIB = 1 << 20


def limit(mib):
    return pltpu.CompilerParams(vmem_limit_bytes=mib * MIB)


def iota(shape, dim):
    return lax.broadcasted_iota(jnp.int32, shape, dim).astype(jnp.float32)


def total(x, axis):
    return jnp.sum(x, axis=axis, keepdims=True)


def chip_rank(chip):
    x, y = chip // SIDE, chip % SIDE
    return (x + SIDE // 2) % SIDE * SIDE + (y + SIDE // 2) % SIDE


PLANE = sorted(range(CHIPS), key=chip_rank)
COLUMN = [(k + DEEP // 2) % DEEP for k in range(DEEP)]
BOTH = [chip * CORES + core for chip in PLANE for core in (1, 0)]
EACH = [[chip * CORES + core for chip in PLANE] for core in (0, 1)]
HALVES = [[place * DEEP + z for place in group for z in COLUMN] for group in EACH]
PAIRS = [(place, place ^ 1) for place in range(CHIPS * CORES)]


def core_index():
    return lax.axis_index("q") & 1


def chip_index():
    return lax.axis_index("q") >> 1


def modulo(x, n):
    return x - n * jnp.floor(x / n)


def place_rank(place):
    chip = jnp.floor(place / CORES)
    x, y = jnp.floor(chip / SIDE), modulo(chip, SIDE)
    x, y = modulo(x + SIDE // 2, SIDE), modulo(y + SIDE // 2, SIDE)
    return (x * SIDE + y) * CORES + (1.0 - modulo(place, CORES))


def as_column(row):
    n = row.shape[1]
    return total(jnp.where(iota((n, n), 0) == iota((n, n), 1), row, 0.0), 1)


def ends_of(lengths_ref):
    row = lengths_ref[...].astype(jnp.float32)
    n = row.shape[1]
    down, across = iota((n, n), 0), iota((n, n), 1)
    column = total(jnp.where(across <= down, row, 0.0), 1) - 1.0
    return total(jnp.where(down <= across, as_column(row), 0.0), 0) - 1.0, column


def pick_kernel(lengths_ref, *refs):
    *first_ref, hidden_ref, out_ref, more_ref, lengths, hidden, sems = refs
    small = pltpu.make_async_copy(lengths_ref, lengths, sems.at[0])
    large = pltpu.make_async_copy(hidden_ref, hidden, sems.at[1])
    small.start()
    large.start()
    first = first_ref[0][0, 0] if first_ref else jnp.int32(0)
    small.wait()
    n, rows_here = lengths.shape[1], hidden.shape[0]
    ends, _ = ends_of(lengths)
    counts = total(jnp.where(jnp.floor(ends / rows_here) == iota((32, n), 0), 1.0, 0.0), 1)
    most = jnp.max(counts).astype(jnp.int32)
    more_ref[0, 0] = (most > first + SLOTS).astype(jnp.int32)
    base = (lax.axis_index("q") * rows_here).astype(jnp.float32)
    owned = (ends >= base) & (ends < base + rows_here)
    before = total(jnp.where(ends < base, 1.0, 0.0), 1)
    slot = iota((1, n), 1) - before - first.astype(jnp.float32)
    wanted = owned & (slot == iota((SLOTS, n), 0))
    at = total(jnp.where(wanted, ends - base + 1.0, 0.0), 1) - 1.0
    selector = (at == iota((SLOTS, rows_here), 1)).astype(jnp.bfloat16)
    large.wait()
    picked = jnp.dot(selector, hidden[...], preferred_element_type=jnp.float32)
    picked = picked.astype(jnp.bfloat16)
    for peer in range(out_ref.shape[0]):
        out_ref[peer] = picked


def norm_kernel(rows_ref, gain_ref, out_ref):
    parts, _, width = rows_ref.shape
    squares = jnp.zeros((SLOTS, 1), jnp.float32)
    for part in range(parts):
        values = rows_ref[part].astype(jnp.float32)
        squares = squares + total(values * values, 1)
    scale = jnp.sqrt(squares / (parts * width) + 1e-05)
    chips, cores, _, block = out_ref.shape
    for rank, chip in enumerate(PLANE):
        part, at = divmod(chip * block, width)
        part = COLUMN.index(part)
        values = rows_ref[part, :, at : at + block].astype(jnp.float32)
        gain = gain_ref[:, chip * block : (chip + 1) * block]
        normed = (values * gain / scale).astype(jnp.bfloat16)
        for core in range(cores):
            out_ref[rank, core] = normed


def rows_in_order(lengths_ref, found_ref, first=0.0):
    n = lengths_ref.shape[1]
    places = found_ref.shape[0]
    rows = 512
    ends_row, ends = ends_of(lengths_ref)
    owner = jnp.floor(ends / rows)
    before = total(jnp.where(ends_row < owner * rows, 1.0, 0.0), 1)
    slot = iota((n, 1), 0) - before - first
    inside = (slot >= 0.0) & (slot < SLOTS)
    at = jnp.where(inside, place_rank(owner) * SLOTS + slot, -1.0)
    selector = (at == iota((n, places), 1)).astype(jnp.bfloat16)
    return jnp.dot(selector, found_ref[...], preferred_element_type=jnp.float32)


def order_kernel(lengths_ref, first_ref, found_ref, more_ref, next_ref, out_ref):
    next_ref[0, 0] = first_ref[0, 0] + SLOTS
    first = first_ref[0, 0].astype(jnp.float32)
    rows = rows_in_order(lengths_ref, found_ref, first)
    out_ref[...] = more_ref[...] + rows.astype(jnp.bfloat16)


def head_kernel(lengths_ref, found_ref, more_ref, weight_ref, other_ref, out_ref):
    width = weight_ref.shape[1]
    blocks = out_ref.shape[0]
    start = core_index() * (weight_ref.shape[0] - blocks * BLOCK)
    first = core_index() == 0
    rows = rows_in_order(lengths_ref, found_ref).astype(jnp.bfloat16) + more_ref[...]
    low, high = rows[:, :width], rows[:, width:]
    left = jnp.concatenate([jnp.where(first, low, high), jnp.where(first, high, low)], axis=1)
    for block in range(blocks):
        span = pl.ds(pl.multiple_of(start + block * BLOCK, 16), BLOCK)
        weight = jnp.concatenate([weight_ref[span, :], other_ref[span, :]], axis=1)
        part = lax.dot_general(
            left, weight, (((1,), (1,)), ((), ())), preferred_element_type=jnp.float32
        )
        out_ref[block] = part.astype(out_ref.dtype)


def stats_kernel(spare, vocab, logits_ref, targets_ref, out_ref):
    logits = logits_ref[...]
    n, block = logits.shape
    core = core_index()
    chip = chip_index()
    x, y = chip >> 2, chip & (SIDE - 1)
    rank = ((x + SIDE // 2) & (SIDE - 1)) * SIDE + ((y + SIDE // 2) & (SIDE - 1))
    start = (core * spare + rank * block).astype(jnp.float32)
    column = iota((1, block), 1) + start
    half = vocab - spare
    valid = column >= (core * half).astype(jnp.float32)
    shift = (lax.axis_index("z") * vocab).astype(jnp.float32)
    wanted = as_column(targets_ref[...].astype(jnp.float32)) - shift
    found = total(jnp.where(valid & (column == wanted), logits, 0.0), 1)
    logits = jnp.where(valid, logits, NEG)
    top = jnp.max(logits, axis=1, keepdims=True)
    both = top + jnp.log(total(jnp.exp(logits - top), 1))
    down, across = iota((n, 2 * n), 0), iota((n, 2 * n), 1)
    line = jnp.where(across == down, both, 0.0) + jnp.where(across == down + n, found, 0.0)
    out_ref[...] = total(line, 0)


def pair_kernel(mine_ref, theirs_ref, out_ref):
    mine, theirs = mine_ref[...], theirs_ref[...]
    top = jnp.maximum(mine, theirs)
    both = top + jnp.log(jnp.exp(mine - top) + jnp.exp(theirs - top))
    half = iota(mine.shape, 1) < mine.shape[1] // 2
    out_ref[...] = jnp.broadcast_to(jnp.where(half, both, mine + theirs), out_ref.shape)


def join_kernel(found_ref, out_ref):
    n = out_ref.shape[1]
    lines = found_ref[...]
    top = jnp.max(lines, axis=0, keepdims=True)
    both = top + jnp.log(total(jnp.exp(lines - top), 0))
    chosen = total(lines, 0)
    out_ref[...] = chosen[:, n:] - both[:, :n]


def shape(dims, dtype):
    return jax.ShapeDtypeStruct(dims, dtype)


def in_hbm(x):
    return pltpu.with_memory_space_constraint(x, pltpu.HBM)


def exchange(x, axis, groups):
    return lax.all_to_all(
        x, axis, split_axis=0, concat_axis=0, tiled=True, axis_index_groups=groups
    )


def picked(lengths, first, hidden):
    return pl.pallas_call(
        pick_kernel,
        out_shape=(
            shape((DEEP, SLOTS, hidden.shape[1]), hidden.dtype),
            pltpu.SMEM((1, 1), jnp.int32),
        ),
        in_specs=[HBM] + [SMEM] * len(first) + [HBM],
        out_specs=(VMEM, SMEM),
        scratch_shapes=[
            pltpu.VMEM(lengths.shape, lengths.dtype),
            pltpu.VMEM(hidden.shape, hidden.dtype),
            pltpu.SemaphoreType.DMA((2,)),
        ],
        compiler_params=limit(4),
        cost_estimate=pl.CostEstimate(flops=10**10, bytes_accessed=1 << 25, transcendentals=0),
        name="pick",
    )(in_hbm(lengths), *first, in_hbm(hidden))


def spread(rows, gain, after=()):
    chips, cores = CHIPS, CORES
    width = gain.shape[1] // chips
    rows, after = lax.optimization_barrier((exchange(rows, "z", [COLUMN]), after))
    normed = pl.pallas_call(
        norm_kernel,
        out_shape=shape((chips, cores, SLOTS, width), jnp.bfloat16),
        in_specs=[VMEM, VMEM],
        out_specs=VMEM,
        compiler_params=limit(4),
        cost_estimate=pl.CostEstimate(flops=10**10, bytes_accessed=1 << 25, transcendentals=0),
        name="norm",
    )(rows, gain)
    return exchange(normed.reshape(chips * cores * SLOTS, width), "q", [BOTH]), after


def local(hidden, lengths, targets, norm_gain, lm_weight):
    n = lengths.shape[0]
    lengths, targets, gain = lengths[None], targets[None], norm_gain[None]
    weight = lm_weight.T
    vocab, depth = weight.shape
    chips = CHIPS
    half = chips * BLOCK
    start = jnp.zeros((1, 1), jnp.int32)
    rows, some = picked(lengths, (), hidden)

    def again(state):
        _, first, more = state
        rows, some = picked(lengths, (first,), hidden)
        found = spread(rows, gain)[0]
        first, more = pl.pallas_call(
            order_kernel,
            out_shape=(shape(first.shape, first.dtype), shape(more.shape, more.dtype)),
            in_specs=[VMEM, SMEM, VMEM, VMEM],
            out_specs=(SMEM, VMEM),
            input_output_aliases={1: 0, 3: 1},
            compiler_params=limit(4),
            name="order",
        )(lengths, first, found, more)
        return some[0, 0], first, more

    _, _, more = lax.while_loop(
        lambda state: state[0] != 0,
        again,
        (some[0, 0], start + SLOTS, jnp.zeros((n, gain.shape[1] // chips), jnp.bfloat16)),
    )
    rows, more, weight = lax.optimization_barrier((rows, more, weight))
    found, weight = spread(rows, gain, weight)
    other = lax.ppermute(weight, "q", PAIRS)
    own = weight
    parts = pl.pallas_call(
        head_kernel,
        out_shape=shape((chips, n, BLOCK), jnp.float32),
        in_specs=[VMEM] * 5,
        out_specs=VMEM,
        compiler_params=limit(16),
        name="head",
    )(lengths, found, more, own, other)
    logits = jnp.sum(exchange(parts.astype(jnp.float16), "q", EACH).astype(jnp.float32), axis=0)
    line = pl.pallas_call(
        functools.partial(stats_kernel, vocab - half, vocab),
        out_shape=shape((1, 2 * n), jnp.float32),
        in_specs=[VMEM, VMEM],
        out_specs=VMEM,
        compiler_params=limit(4),
        name="stats",
    )(logits, targets)
    return pl.pallas_call(
        pair_kernel,
        out_shape=shape((len(HALVES[0]), 2 * n), jnp.float32),
        in_specs=[VMEM, VMEM],
        out_specs=VMEM,
        compiler_params=limit(4),
        name="pair",
    )(line, lax.ppermute(line, "q", PAIRS))


def joined(line):
    n = line.shape[1] // 2
    out = pl.pallas_call(
        join_kernel,
        out_shape=shape((1, n), jnp.float32),
        in_specs=[VMEM],
        out_specs=VMEM,
        compiler_params=limit(4),
        name="join",
    )(exchange(line, "d", HALVES))
    return out[0]


def solution(mesh):
    devices = mesh.devices.reshape(CHIPS * CORES, DEEP)
    first = jax.shard_map(
        local,
        mesh=Mesh(devices, ("q", "z")),
        in_specs=(P("q", "z"), P(), P(), P(), P("q", "z")),
        out_specs=P(("q", "z")),
        check_vma=False,
    )
    last = jax.shard_map(
        joined,
        mesh=Mesh(devices.reshape(-1), ("d",)),
        in_specs=P("d"),
        out_specs=P(),
        check_vma=False,
    )
    return lambda *args: last(first(*args))
```

```python
import functools

import jax
import jax.numpy as jnp
from jax import lax
from jax.experimental import pallas as pl
from jax.experimental.pallas import tpu as pltpu
from jax.sharding import Mesh
from jax.sharding import PartitionSpec as P

SLOTS = 8
SIDE = 4
CHIPS = SIDE * SIDE
CORES = 2
DEEP = 8
FAR_X, FAR_Y, FAR_Z, FAR_CORE = 2, 2, 4, 1
BLOCK = 512
NEG = -1e30

VMEM = pl.BlockSpec(memory_space=pltpu.VMEM)
HBM = pl.BlockSpec(memory_space=pltpu.HBM)
SMEM = pl.BlockSpec(memory_space=pltpu.SMEM)
MIB = 1 << 20


def limit(mib):
    return pltpu.CompilerParams(vmem_limit_bytes=mib * MIB)


def iota(shape, dim):
    return lax.broadcasted_iota(jnp.int32, shape, dim).astype(jnp.float32)


def total(x, axis):
    return jnp.sum(x, axis=axis, keepdims=True)


def chip_rank(chip):
    x, y = chip // SIDE, chip % SIDE
    return (x - FAR_X) % SIDE * SIDE + (y - FAR_Y) % SIDE


PLANE = sorted(range(CHIPS), key=chip_rank)
COLUMN = [(k + FAR_Z) % DEEP for k in range(DEEP)]
BOTH = [chip * CORES + core for chip in PLANE for core in (FAR_CORE, 1 - FAR_CORE)]
EACH = [[chip * CORES + core for chip in PLANE] for core in (0, 1)]
HALVES = [[place * DEEP + z for place in group for z in COLUMN] for group in EACH]
PAIRS = [(place, place ^ 1) for place in range(CHIPS * CORES)]


def core_index():
    return lax.axis_index("q") & 1


def chip_index():
    return lax.axis_index("q") >> 1


def modulo(x, n):
    return x - n * jnp.floor(x / n)


def place_rank(place):
    chip = jnp.floor(place / CORES)
    x, y = jnp.floor(chip / SIDE), modulo(chip, SIDE)
    x, y = modulo(x - FAR_X, SIDE), modulo(y - FAR_Y, SIDE)
    core = modulo(place, CORES)
    return (x * SIDE + y) * CORES + (core if FAR_CORE == 0 else 1.0 - core)


def as_column(row):
    n = row.shape[1]
    return total(jnp.where(iota((n, n), 0) == iota((n, n), 1), row, 0.0), 1)


def ends_of(lengths_ref):
    row = lengths_ref[...].astype(jnp.float32)
    n = row.shape[1]
    down, across = iota((n, n), 0), iota((n, n), 1)
    column = total(jnp.where(across <= down, row, 0.0), 1) - 1.0
    return total(jnp.where(down <= across, as_column(row), 0.0), 0) - 1.0, column


def order_of(ends, column, rows, first, places):
    n = column.shape[0]
    owner = jnp.floor(column / rows)
    before = total(jnp.where(ends < owner * rows, 1.0, 0.0), 1)
    slot = iota((n, 1), 0) - before - first
    inside = (slot >= 0.0) & (slot < SLOTS)
    at = jnp.where(inside, place_rank(owner) * SLOTS + slot, -1.0)
    return (at == iota((n, places), 1)).astype(jnp.bfloat16)


def pick_kernel(lengths_ref, *refs):
    *first_ref, hidden_ref, out_ref, more_ref, order_ref, lengths, hidden, sems = refs
    small = pltpu.make_async_copy(lengths_ref, lengths, sems.at[0])
    large = pltpu.make_async_copy(hidden_ref, hidden, sems.at[1])
    small.start()
    large.start()
    first = first_ref[0][0, 0] if first_ref else jnp.int32(0)
    small.wait()
    n, rows_here = lengths.shape[1], hidden.shape[0]
    ends, column = ends_of(lengths)
    counts = total(jnp.where(jnp.floor(ends / rows_here) == iota((32, n), 0), 1.0, 0.0), 1)
    most = jnp.max(counts).astype(jnp.int32)
    more_ref[0, 0] = (most > first + SLOTS).astype(jnp.int32)
    base = (lax.axis_index("q") * rows_here).astype(jnp.float32)
    owned = (ends >= base) & (ends < base + rows_here)
    before = total(jnp.where(ends < base, 1.0, 0.0), 1)
    slot = iota((1, n), 1) - before - first.astype(jnp.float32)
    wanted = owned & (slot == iota((SLOTS, n), 0))
    at = total(jnp.where(wanted, ends - base + 1.0, 0.0), 1) - 1.0
    selector = (at == iota((SLOTS, rows_here), 1)).astype(jnp.bfloat16)
    order_ref[...] = order_of(ends, column, rows_here, first.astype(jnp.float32), order_ref.shape[1])
    large.wait()
    picked = jnp.dot(selector, hidden[...], preferred_element_type=jnp.float32)
    picked = picked.astype(jnp.bfloat16)
    for peer in range(out_ref.shape[0]):
        out_ref[peer] = picked


def norm_kernel(rows_ref, gain_ref, out_ref):
    parts, _, width = rows_ref.shape
    squares = jnp.zeros((SLOTS, 1), jnp.float32)
    for part in range(parts):
        values = rows_ref[part].astype(jnp.float32)
        squares = squares + total(values * values, 1)
    scale = jnp.sqrt(squares / (parts * width) + 1e-05)
    chips, cores, _, block = out_ref.shape
    for rank, chip in enumerate(PLANE):
        part, at = divmod(chip * block, width)
        part = COLUMN.index(part)
        values = rows_ref[part, :, at : at + block].astype(jnp.float32)
        gain = gain_ref[:, chip * block : (chip + 1) * block]
        normed = (values * gain / scale).astype(jnp.bfloat16)
        for core in range(cores):
            out_ref[rank, core] = normed


def order_kernel(order_ref, first_ref, found_ref, more_ref, next_ref, out_ref):
    next_ref[0, 0] = first_ref[0, 0] + SLOTS
    rows = jnp.dot(order_ref[...], found_ref[...], preferred_element_type=jnp.float32)
    out_ref[...] = more_ref[...] + rows.astype(jnp.bfloat16)


def head_kernel(order_ref, found_ref, more_ref, weight_ref, other_ref, out_ref):
    width = weight_ref.shape[1]
    blocks = out_ref.shape[0]
    start = core_index() * (weight_ref.shape[0] - blocks * BLOCK)
    first = core_index() == 0
    rows = jnp.dot(order_ref[...], found_ref[...], preferred_element_type=jnp.float32)
    rows = rows.astype(jnp.bfloat16) + more_ref[...]
    low, high = rows[:, :width], rows[:, width:]
    left = jnp.concatenate([jnp.where(first, low, high), jnp.where(first, high, low)], axis=1)
    for block in range(blocks):
        span = pl.ds(pl.multiple_of(start + block * BLOCK, 16), BLOCK)
        weight = jnp.concatenate([weight_ref[span, :], other_ref[span, :]], axis=1)
        part = lax.dot_general(
            left, weight, (((1,), (1,)), ((), ())), preferred_element_type=jnp.float32
        )
        out_ref[block] = part.astype(out_ref.dtype)


def stats_kernel(spare, vocab, logits_ref, targets_ref, out_ref):
    logits = logits_ref[...]
    n, block = logits.shape
    core = core_index()
    chip = chip_index()
    x, y = chip >> 2, chip & (SIDE - 1)
    rank = ((x - FAR_X) & (SIDE - 1)) * SIDE + ((y - FAR_Y) & (SIDE - 1))
    start = (core * spare + rank * block).astype(jnp.float32)
    column = iota((1, block), 1) + start
    half = vocab - spare
    valid = column >= (core * half).astype(jnp.float32)
    shift = (lax.axis_index("z") * vocab).astype(jnp.float32)
    wanted = as_column(targets_ref[...].astype(jnp.float32)) - shift
    found = total(jnp.where(valid & (column == wanted), logits, 0.0), 1)
    logits = jnp.where(valid, logits, NEG)
    top = jnp.max(logits, axis=1, keepdims=True)
    both = top + jnp.log(total(jnp.exp(logits - top), 1))
    down, across = iota((n, 2 * n), 0), iota((n, 2 * n), 1)
    line = jnp.where(across == down, both, 0.0) + jnp.where(across == down + n, found, 0.0)
    out_ref[...] = total(line, 0)


def pair_kernel(mine_ref, theirs_ref, out_ref):
    mine, theirs = mine_ref[...], theirs_ref[...]
    top = jnp.maximum(mine, theirs)
    both = top + jnp.log(jnp.exp(mine - top) + jnp.exp(theirs - top))
    half = iota(mine.shape, 1) < mine.shape[1] // 2
    out_ref[...] = jnp.broadcast_to(jnp.where(half, both, mine + theirs), out_ref.shape)


def join_kernel(found_ref, out_ref):
    n = out_ref.shape[1]
    lines = found_ref[...]
    top = jnp.max(lines, axis=0, keepdims=True)
    both = top + jnp.log(total(jnp.exp(lines - top), 0))
    chosen = total(lines, 0)
    out_ref[...] = chosen[:, n:] - both[:, :n]


def shape(dims, dtype):
    return jax.ShapeDtypeStruct(dims, dtype)


def in_hbm(x):
    return pltpu.with_memory_space_constraint(x, pltpu.HBM)


def exchange(x, axis, groups):
    return lax.all_to_all(
        x, axis, split_axis=0, concat_axis=0, tiled=True, axis_index_groups=groups
    )


def picked(lengths, first, hidden):
    return pl.pallas_call(
        pick_kernel,
        out_shape=(
            shape((DEEP, SLOTS, hidden.shape[1]), hidden.dtype),
            pltpu.SMEM((1, 1), jnp.int32),
            shape((lengths.shape[1], CHIPS * CORES * SLOTS), jnp.bfloat16),
        ),
        in_specs=[HBM] + [SMEM] * len(first) + [HBM],
        out_specs=(VMEM, SMEM, VMEM),
        scratch_shapes=[
            pltpu.VMEM(lengths.shape, lengths.dtype),
            pltpu.VMEM(hidden.shape, hidden.dtype),
            pltpu.SemaphoreType.DMA((2,)),
        ],
        compiler_params=limit(4),
        cost_estimate=pl.CostEstimate(flops=10**10, bytes_accessed=1 << 25, transcendentals=0),
        name="pick",
    )(in_hbm(lengths), *first, in_hbm(hidden))


def spread(rows, gain, after=()):
    chips, cores = CHIPS, CORES
    width = gain.shape[1] // chips
    rows, after = lax.optimization_barrier((exchange(rows, "z", [COLUMN]), after))
    normed = pl.pallas_call(
        norm_kernel,
        out_shape=shape((chips, cores, SLOTS, width), jnp.bfloat16),
        in_specs=[VMEM, VMEM],
        out_specs=VMEM,
        compiler_params=limit(4),
        cost_estimate=pl.CostEstimate(flops=10**10, bytes_accessed=1 << 25, transcendentals=0),
        name="norm",
    )(rows, gain)
    return exchange(normed.reshape(chips * cores * SLOTS, width), "q", [BOTH]), after


def local(hidden, lengths, targets, norm_gain, lm_weight):
    n = lengths.shape[0]
    lengths, targets, gain = lengths[None], targets[None], norm_gain[None]
    weight = lm_weight.T
    vocab, depth = weight.shape
    chips = CHIPS
    half = chips * BLOCK
    start = jnp.zeros((1, 1), jnp.int32)
    rows, some, order = picked(lengths, (), hidden)

    def again(state):
        _, first, more = state
        rows, some, order = picked(lengths, (first,), hidden)
        found = spread(rows, gain)[0]
        first, more = pl.pallas_call(
            order_kernel,
            out_shape=(shape(first.shape, first.dtype), shape(more.shape, more.dtype)),
            in_specs=[VMEM, SMEM, VMEM, VMEM],
            out_specs=(SMEM, VMEM),
            input_output_aliases={1: 0, 3: 1},
            compiler_params=limit(4),
            name="order",
        )(order, first, found, more)
        return some[0, 0], first, more

    _, _, more = lax.while_loop(
        lambda state: state[0] != 0,
        again,
        (some[0, 0], start + SLOTS, jnp.zeros((n, gain.shape[1] // chips), jnp.bfloat16)),
    )
    rows, more, weight = lax.optimization_barrier((rows, more, weight))
    found, weight = spread(rows, gain, weight)
    other = lax.ppermute(weight, "q", PAIRS)
    own = weight
    parts = pl.pallas_call(
        head_kernel,
        out_shape=shape((chips, n, BLOCK), jnp.float32),
        in_specs=[VMEM] * 5,
        out_specs=VMEM,
        compiler_params=limit(16),
        name="head",
    )(order, found, more, own, other)
    logits = jnp.sum(exchange(parts.astype(jnp.float16), "q", EACH).astype(jnp.float32), axis=0)
    line = pl.pallas_call(
        functools.partial(stats_kernel, vocab - half, vocab),
        out_shape=shape((1, 2 * n), jnp.float32),
        in_specs=[VMEM, VMEM],
        out_specs=VMEM,
        compiler_params=limit(4),
        name="stats",
    )(logits, targets)
    return pl.pallas_call(
        pair_kernel,
        out_shape=shape((len(HALVES[0]), 2 * n), jnp.float32),
        in_specs=[VMEM, VMEM],
        out_specs=VMEM,
        compiler_params=limit(4),
        name="pair",
    )(line, lax.ppermute(line, "q", PAIRS))


def joined(line):
    n = line.shape[1] // 2
    out = pl.pallas_call(
        join_kernel,
        out_shape=shape((1, n), jnp.float32),
        in_specs=[VMEM],
        out_specs=VMEM,
        compiler_params=limit(4),
        name="join",
    )(exchange(line, "d", HALVES))
    return out[0]


def solution(mesh):
    devices = mesh.devices.reshape(CHIPS * CORES, DEEP)
    first = jax.shard_map(
        local,
        mesh=Mesh(devices, ("q", "z")),
        in_specs=(P("q", "z"), P(), P(), P(), P("q", "z")),
        out_specs=P(("q", "z")),
        check_vma=False,
    )
    last = jax.shard_map(
        joined,
        mesh=Mesh(devices.reshape(-1), ("d",)),
        in_specs=P("d"),
        out_specs=P(),
        check_vma=False,
    )
    return lambda *args: last(first(*args))
```

```python
import functools

import jax
import jax.numpy as jnp
from jax import lax
from jax.experimental import pallas as pl
from jax.experimental.pallas import tpu as pltpu
from jax.sharding import Mesh
from jax.sharding import PartitionSpec as P

SLOTS = 8
SIDE = 4
CHIPS = SIDE * SIDE
CORES = 2
DEEP = 8
FAR_X, FAR_Y, FAR_Z, FAR_CORE = 2, 2, 4, 1
BLOCK = 512
NEG = -1e30

VMEM = pl.BlockSpec(memory_space=pltpu.VMEM)
HBM = pl.BlockSpec(memory_space=pltpu.HBM)
SMEM = pl.BlockSpec(memory_space=pltpu.SMEM)
MIB = 1 << 20


def limit(mib):
    return pltpu.CompilerParams(vmem_limit_bytes=mib * MIB)


def iota(shape, dim):
    return lax.broadcasted_iota(jnp.int32, shape, dim).astype(jnp.float32)


def total(x, axis):
    return jnp.sum(x, axis=axis, keepdims=True)


def chip_rank(chip):
    x, y = chip // SIDE, chip % SIDE
    return (x - FAR_X) % SIDE * SIDE + (y - FAR_Y) % SIDE


PLANE = sorted(range(CHIPS), key=chip_rank)
COLUMN = [(k + FAR_Z) % DEEP for k in range(DEEP)]
BOTH = [chip * CORES + core for chip in PLANE for core in (FAR_CORE, 1 - FAR_CORE)]
EACH = [[chip * CORES + core for chip in PLANE] for core in (0, 1)]
HALVES = [[place * DEEP + z for place in group for z in COLUMN] for group in EACH]
PAIRS = [(place, place ^ 1) for place in range(CHIPS * CORES)]


def core_index():
    return lax.axis_index("q") & 1


def chip_index():
    return lax.axis_index("q") >> 1


def modulo(x, n):
    return x - n * jnp.floor(x / n)


def place_rank(place):
    chip = jnp.floor(place / CORES)
    x, y = jnp.floor(chip / SIDE), modulo(chip, SIDE)
    x, y = modulo(x - FAR_X, SIDE), modulo(y - FAR_Y, SIDE)
    core = modulo(place, CORES)
    return (x * SIDE + y) * CORES + (core if FAR_CORE == 0 else 1.0 - core)


def as_column(row):
    n = row.shape[1]
    return total(jnp.where(iota((n, n), 0) == iota((n, n), 1), row, 0.0), 1)


def ends_of(lengths_ref):
    row = lengths_ref[...].astype(jnp.float32)
    n = row.shape[1]
    down, across = iota((n, n), 0), iota((n, n), 1)
    column = total(jnp.where(across <= down, row, 0.0), 1) - 1.0
    return total(jnp.where(down <= across, as_column(row), 0.0), 0) - 1.0, column


def order_of(ends, column, rows, first, places):
    n = column.shape[0]
    owner = jnp.floor(column / rows)
    before = total(jnp.where(ends < owner * rows, 1.0, 0.0), 1)
    slot = iota((n, 1), 0) - before - first
    inside = (slot >= 0.0) & (slot < SLOTS)
    at = jnp.where(inside, place_rank(owner) * SLOTS + slot, -1.0)
    return (at == iota((n, places), 1)).astype(jnp.bfloat16)


def pick_kernel(lengths_ref, *refs):
    *first_ref, hidden_ref, out_ref, more_ref, order_ref, lengths, hidden, sems = refs
    small = pltpu.make_async_copy(lengths_ref, lengths, sems.at[0])
    large = pltpu.make_async_copy(hidden_ref, hidden, sems.at[1])
    small.start()
    large.start()
    first = first_ref[0][0, 0] if first_ref else jnp.int32(0)
    small.wait()
    n, rows_here = lengths.shape[1], hidden.shape[0]
    ends, column = ends_of(lengths)
    counts = total(jnp.where(jnp.floor(ends / rows_here) == iota((32, n), 0), 1.0, 0.0), 1)
    most = jnp.max(counts).astype(jnp.int32)
    more_ref[0, 0] = (most > first + SLOTS).astype(jnp.int32)
    base = (lax.axis_index("q") * rows_here).astype(jnp.float32)
    owned = (ends >= base) & (ends < base + rows_here)
    before = total(jnp.where(ends < base, 1.0, 0.0), 1)
    slot = iota((1, n), 1) - before - first.astype(jnp.float32)
    wanted = owned & (slot == iota((SLOTS, n), 0))
    at = total(jnp.where(wanted, ends - base + 1.0, 0.0), 1) - 1.0
    selector = (at == iota((SLOTS, rows_here), 1)).astype(jnp.bfloat16)
    order_ref[...] = order_of(ends, column, rows_here, first.astype(jnp.float32), order_ref.shape[1])
    large.wait()
    picked = jnp.dot(selector, hidden[...], preferred_element_type=jnp.float32)
    picked = picked.astype(jnp.bfloat16)
    for peer in range(out_ref.shape[0]):
        out_ref[peer] = picked


def norm_kernel(rows_ref, gain_ref, out_ref):
    parts, _, width = rows_ref.shape
    squares = jnp.zeros((SLOTS, 1), jnp.float32)
    for part in range(parts):
        values = rows_ref[part].astype(jnp.float32)
        squares = squares + total(values * values, 1)
    scale = jnp.sqrt(squares / (parts * width) + 1e-05)
    chips, cores, _, block = out_ref.shape
    for rank, chip in enumerate(PLANE):
        part, at = divmod(chip * block, width)
        part = COLUMN.index(part)
        values = rows_ref[part, :, at : at + block].astype(jnp.float32)
        gain = gain_ref[:, chip * block : (chip + 1) * block]
        normed = (values * gain / scale).astype(jnp.bfloat16)
        for core in range(cores):
            out_ref[rank, core] = normed


def order_kernel(order_ref, first_ref, found_ref, more_ref, next_ref, out_ref):
    next_ref[0, 0] = first_ref[0, 0] + SLOTS
    rows = jnp.dot(order_ref[...], found_ref[...], preferred_element_type=jnp.float32)
    out_ref[...] = more_ref[...] + rows.astype(jnp.bfloat16)


def head_kernel(order_ref, found_ref, more_ref, weight_ref, other_ref, out_ref):
    width = weight_ref.shape[1]
    blocks = out_ref.shape[0]
    start = core_index() * (weight_ref.shape[0] - blocks * BLOCK)
    first = core_index() == 0
    rows = jnp.dot(order_ref[...], found_ref[...], preferred_element_type=jnp.float32)
    rows = rows.astype(jnp.bfloat16) + more_ref[...]
    low, high = rows[:, :width], rows[:, width:]
    left = jnp.concatenate([jnp.where(first, low, high), jnp.where(first, high, low)], axis=1)
    for block in range(blocks):
        span = pl.ds(pl.multiple_of(start + block * BLOCK, 16), BLOCK)
        weight = jnp.concatenate([weight_ref[span, :], other_ref[span, :]], axis=1)
        part = lax.dot_general(
            weight, left, (((1,), (1,)), ((), ())), preferred_element_type=jnp.float32
        )
        out_ref[block] = part.T.astype(out_ref.dtype)


def stats_kernel(spare, vocab, logits_ref, targets_ref, out_ref):
    logits = logits_ref[...]
    n, block = logits.shape
    core = core_index()
    chip = chip_index()
    x, y = chip >> 2, chip & (SIDE - 1)
    rank = ((x - FAR_X) & (SIDE - 1)) * SIDE + ((y - FAR_Y) & (SIDE - 1))
    start = (core * spare + rank * block).astype(jnp.float32)
    column = iota((1, block), 1) + start
    half = vocab - spare
    valid = column >= (core * half).astype(jnp.float32)
    shift = (lax.axis_index("z") * vocab).astype(jnp.float32)
    wanted = as_column(targets_ref[...].astype(jnp.float32)) - shift
    found = total(jnp.where(valid & (column == wanted), logits, 0.0), 1)
    logits = jnp.where(valid, logits, NEG)
    top = jnp.max(logits, axis=1, keepdims=True)
    both = top + jnp.log(total(jnp.exp(logits - top), 1))
    down, across = iota((n, 2 * n), 0), iota((n, 2 * n), 1)
    line = jnp.where(across == down, both, 0.0) + jnp.where(across == down + n, found, 0.0)
    out_ref[...] = total(line, 0)


def pair_kernel(mine_ref, theirs_ref, out_ref):
    mine, theirs = mine_ref[...], theirs_ref[...]
    top = jnp.maximum(mine, theirs)
    both = top + jnp.log(jnp.exp(mine - top) + jnp.exp(theirs - top))
    half = iota(mine.shape, 1) < mine.shape[1] // 2
    out_ref[...] = jnp.broadcast_to(jnp.where(half, both, mine + theirs), out_ref.shape)


def join_kernel(found_ref, out_ref):
    n = out_ref.shape[1]
    lines = found_ref[...]
    top = jnp.max(lines, axis=0, keepdims=True)
    both = top + jnp.log(total(jnp.exp(lines - top), 0))
    chosen = total(lines, 0)
    out_ref[...] = chosen[:, n:] - both[:, :n]


def shape(dims, dtype):
    return jax.ShapeDtypeStruct(dims, dtype)


def in_hbm(x):
    return pltpu.with_memory_space_constraint(x, pltpu.HBM)


def exchange(x, axis, groups):
    return lax.all_to_all(
        x, axis, split_axis=0, concat_axis=0, tiled=True, axis_index_groups=groups
    )


def picked(lengths, first, hidden):
    return pl.pallas_call(
        pick_kernel,
        out_shape=(
            shape((DEEP, SLOTS, hidden.shape[1]), hidden.dtype),
            pltpu.SMEM((1, 1), jnp.int32),
            shape((lengths.shape[1], CHIPS * CORES * SLOTS), jnp.bfloat16),
        ),
        in_specs=[HBM] + [SMEM] * len(first) + [HBM],
        out_specs=(VMEM, SMEM, VMEM),
        scratch_shapes=[
            pltpu.VMEM(lengths.shape, lengths.dtype),
            pltpu.VMEM(hidden.shape, hidden.dtype),
            pltpu.SemaphoreType.DMA((2,)),
        ],
        compiler_params=limit(4),
        cost_estimate=pl.CostEstimate(flops=10**10, bytes_accessed=1 << 25, transcendentals=0),
        name="pick",
    )(in_hbm(lengths), *first, in_hbm(hidden))


def spread(rows, gain, after=()):
    chips, cores = CHIPS, CORES
    width = gain.shape[1] // chips
    rows, after = lax.optimization_barrier((exchange(rows, "z", [COLUMN]), after))
    normed = pl.pallas_call(
        norm_kernel,
        out_shape=shape((chips, cores, SLOTS, width), jnp.bfloat16),
        in_specs=[VMEM, VMEM],
        out_specs=VMEM,
        compiler_params=limit(4),
        cost_estimate=pl.CostEstimate(flops=10**10, bytes_accessed=1 << 25, transcendentals=0),
        name="norm",
    )(rows, gain)
    return exchange(normed.reshape(chips * cores * SLOTS, width), "q", [BOTH]), after


def local(hidden, lengths, targets, norm_gain, lm_weight):
    n = lengths.shape[0]
    lengths, targets, gain = lengths[None], targets[None], norm_gain[None]
    weight = lm_weight.T
    vocab, depth = weight.shape
    chips = CHIPS
    half = chips * BLOCK
    start = jnp.zeros((1, 1), jnp.int32)
    rows, some, order = picked(lengths, (), hidden)

    def again(state):
        _, first, more = state
        rows, some, order = picked(lengths, (first,), hidden)
        found = spread(rows, gain)[0]
        first, more = pl.pallas_call(
            order_kernel,
            out_shape=(shape(first.shape, first.dtype), shape(more.shape, more.dtype)),
            in_specs=[VMEM, SMEM, VMEM, VMEM],
            out_specs=(SMEM, VMEM),
            input_output_aliases={1: 0, 3: 1},
            compiler_params=limit(4),
            name="order",
        )(order, first, found, more)
        return some[0, 0], first, more

    _, _, more = lax.while_loop(
        lambda state: state[0] != 0,
        again,
        (some[0, 0], start + SLOTS, jnp.zeros((n, gain.shape[1] // chips), jnp.bfloat16)),
    )
    rows, more, weight = lax.optimization_barrier((rows, more, weight))
    found, weight = spread(rows, gain, weight)
    other = lax.ppermute(weight, "q", PAIRS)
    own = weight
    parts = pl.pallas_call(
        head_kernel,
        out_shape=shape((chips, n, BLOCK), jnp.float32),
        in_specs=[VMEM] * 5,
        out_specs=VMEM,
        compiler_params=limit(16),
        name="head",
    )(order, found, more, own, other)
    logits = jnp.sum(exchange(parts.astype(jnp.float16), "q", EACH).astype(jnp.float32), axis=0)
    line = pl.pallas_call(
        functools.partial(stats_kernel, vocab - half, vocab),
        out_shape=shape((1, 2 * n), jnp.float32),
        in_specs=[VMEM, VMEM],
        out_specs=VMEM,
        compiler_params=limit(4),
        name="stats",
    )(logits, targets)
    return pl.pallas_call(
        pair_kernel,
        out_shape=shape((len(HALVES[0]), 2 * n), jnp.float32),
        in_specs=[VMEM, VMEM],
        out_specs=VMEM,
        compiler_params=limit(4),
        name="pair",
    )(line, lax.ppermute(line, "q", PAIRS))


def joined(line):
    n = line.shape[1] // 2
    out = pl.pallas_call(
        join_kernel,
        out_shape=shape((1, n), jnp.float32),
        in_specs=[VMEM],
        out_specs=VMEM,
        compiler_params=limit(4),
        name="join",
    )(exchange(line, "d", HALVES))
    return out[0]


def solution(mesh):
    devices = mesh.devices.reshape(CHIPS * CORES, DEEP)
    first = jax.shard_map(
        local,
        mesh=Mesh(devices, ("q", "z")),
        in_specs=(P("q", "z"), P(), P(), P(), P("q", "z")),
        out_specs=P(("q", "z")),
        check_vma=False,
    )
    last = jax.shard_map(
        joined,
        mesh=Mesh(devices.reshape(-1), ("d",)),
        in_specs=P("d"),
        out_specs=P(),
        check_vma=False,
    )
    return lambda *args: last(first(*args))
```

```python
import functools

import jax
import jax.numpy as jnp
from jax import lax
from jax.experimental import pallas as pl
from jax.experimental.pallas import tpu as pltpu
from jax.sharding import Mesh
from jax.sharding import PartitionSpec as P

SLOTS = 8
SIDE = 4
CHIPS = SIDE * SIDE
CORES = 2
DEEP = 8
FAR_X, FAR_Y, FAR_Z, FAR_CORE = 2, 2, 4, 1
BLOCK = 512
NEG = -1e30

VMEM = pl.BlockSpec(memory_space=pltpu.VMEM)
HBM = pl.BlockSpec(memory_space=pltpu.HBM)
SMEM = pl.BlockSpec(memory_space=pltpu.SMEM)
MIB = 1 << 20


def limit(mib):
    return pltpu.CompilerParams(vmem_limit_bytes=mib * MIB)


def iota(shape, dim):
    return lax.broadcasted_iota(jnp.int32, shape, dim).astype(jnp.float32)


def total(x, axis):
    return jnp.sum(x, axis=axis, keepdims=True)


def chip_rank(chip):
    x, y = chip // SIDE, chip % SIDE
    return (x - FAR_X) % SIDE * SIDE + (y - FAR_Y) % SIDE


PLANE = sorted(range(CHIPS), key=chip_rank)
COLUMN = [(k + FAR_Z + 1) % DEEP for k in range(DEEP)]
BOTH = [chip * CORES + core for chip in PLANE for core in (FAR_CORE, 1 - FAR_CORE)]
EACH = [[chip * CORES + core for chip in PLANE] for core in (0, 1)]
LAST = [(k + FAR_Z) % DEEP for k in range(DEEP)]
HALVES = [[place * DEEP + z for place in group for z in LAST] for group in EACH]
PAIRS = [(place, place ^ 1) for place in range(CHIPS * CORES)]


def core_index():
    return lax.axis_index("q") & 1


def chip_index():
    return lax.axis_index("q") >> 1


def modulo(x, n):
    return x - n * jnp.floor(x / n)


def place_rank(place):
    chip = jnp.floor(place / CORES)
    x, y = jnp.floor(chip / SIDE), modulo(chip, SIDE)
    x, y = modulo(x - FAR_X, SIDE), modulo(y - FAR_Y, SIDE)
    core = modulo(place, CORES)
    return (x * SIDE + y) * CORES + (core if FAR_CORE == 0 else 1.0 - core)


def as_column(row):
    n = row.shape[1]
    return total(jnp.where(iota((n, n), 0) == iota((n, n), 1), row, 0.0), 1)


def ends_of(lengths_ref):
    row = lengths_ref[...].astype(jnp.float32)
    n = row.shape[1]
    down, across = iota((n, n), 0), iota((n, n), 1)
    column = total(jnp.where(across <= down, row, 0.0), 1) - 1.0
    return total(jnp.where(down <= across, as_column(row), 0.0), 0) - 1.0, column


def order_of(ends, column, rows, first, places):
    n = column.shape[0]
    owner = jnp.floor(column / rows)
    before = total(jnp.where(ends < owner * rows, 1.0, 0.0), 1)
    slot = iota((n, 1), 0) - before - first
    inside = (slot >= 0.0) & (slot < SLOTS)
    at = jnp.where(inside, place_rank(owner) * SLOTS + slot, -1.0)
    return (at == iota((n, places), 1)).astype(jnp.bfloat16)


def pick_kernel(lengths_ref, *refs):
    *first_ref, hidden_ref, out_ref, more_ref, order_ref, lengths, hidden, sems = refs
    small = pltpu.make_async_copy(lengths_ref, lengths, sems.at[0])
    large = pltpu.make_async_copy(hidden_ref, hidden, sems.at[1])
    small.start()
    large.start()
    first = first_ref[0][0, 0] if first_ref else jnp.int32(0)
    small.wait()
    n, rows_here = lengths.shape[1], hidden.shape[0]
    ends, column = ends_of(lengths)
    counts = total(jnp.where(jnp.floor(ends / rows_here) == iota((32, n), 0), 1.0, 0.0), 1)
    most = jnp.max(counts).astype(jnp.int32)
    more_ref[0, 0] = (most > first + SLOTS).astype(jnp.int32)
    base = (lax.axis_index("q") * rows_here).astype(jnp.float32)
    owned = (ends >= base) & (ends < base + rows_here)
    before = total(jnp.where(ends < base, 1.0, 0.0), 1)
    slot = iota((1, n), 1) - before - first.astype(jnp.float32)
    wanted = owned & (slot == iota((SLOTS, n), 0))
    at = total(jnp.where(wanted, ends - base + 1.0, 0.0), 1) - 1.0
    selector = (at == iota((SLOTS, rows_here), 1)).astype(jnp.bfloat16)
    order_ref[...] = order_of(ends, column, rows_here, first.astype(jnp.float32), order_ref.shape[1])
    large.wait()
    picked = jnp.dot(selector, hidden[...], preferred_element_type=jnp.float32)
    picked = picked.astype(jnp.bfloat16)
    for peer in range(out_ref.shape[0]):
        out_ref[peer] = picked


def norm_kernel(rows_ref, gain_ref, out_ref):
    parts, _, width = rows_ref.shape
    squares = jnp.zeros((SLOTS, 1), jnp.float32)
    for part in range(parts):
        values = rows_ref[part].astype(jnp.float32)
        squares = squares + total(values * values, 1)
    scale = jnp.sqrt(squares / (parts * width) + 1e-05)
    chips, cores, _, block = out_ref.shape
    for rank, chip in enumerate(PLANE):
        part, at = divmod(chip * block, width)
        part = COLUMN.index(part)
        values = rows_ref[part, :, at : at + block].astype(jnp.float32)
        gain = gain_ref[:, chip * block : (chip + 1) * block]
        normed = (values * gain / scale).astype(jnp.bfloat16)
        for core in range(cores):
            out_ref[rank, core] = normed


def order_kernel(order_ref, first_ref, found_ref, more_ref, next_ref, out_ref):
    next_ref[0, 0] = first_ref[0, 0] + SLOTS
    rows = jnp.dot(order_ref[...], found_ref[...], preferred_element_type=jnp.float32)
    out_ref[...] = more_ref[...] + rows.astype(jnp.bfloat16)


def head_kernel(order_ref, found_ref, more_ref, weight_ref, other_ref, out_ref):
    width = weight_ref.shape[1]
    blocks = out_ref.shape[0]
    start = core_index() * (weight_ref.shape[0] - blocks * BLOCK)
    first = core_index() == 0
    rows = jnp.dot(order_ref[...], found_ref[...], preferred_element_type=jnp.float32)
    rows = rows.astype(jnp.bfloat16) + more_ref[...]
    low, high = rows[:, :width], rows[:, width:]
    left = jnp.concatenate([jnp.where(first, low, high), jnp.where(first, high, low)], axis=1)
    for block in range(blocks):
        span = pl.ds(pl.multiple_of(start + block * BLOCK, 16), BLOCK)
        weight = jnp.concatenate([weight_ref[span, :], other_ref[span, :]], axis=1)
        part = lax.dot_general(
            weight, left, (((1,), (1,)), ((), ())), preferred_element_type=jnp.float32
        )
        out_ref[block] = part.T.astype(out_ref.dtype)


def stats_kernel(spare, vocab, logits_ref, targets_ref, out_ref):
    logits = logits_ref[...]
    n, block = logits.shape
    core = core_index()
    chip = chip_index()
    x, y = chip >> 2, chip & (SIDE - 1)
    rank = ((x - FAR_X) & (SIDE - 1)) * SIDE + ((y - FAR_Y) & (SIDE - 1))
    start = (core * spare + rank * block).astype(jnp.float32)
    column = iota((1, block), 1) + start
    half = vocab - spare
    valid = column >= (core * half).astype(jnp.float32)
    shift = (lax.axis_index("z") * vocab).astype(jnp.float32)
    wanted = as_column(targets_ref[...].astype(jnp.float32)) - shift
    found = total(jnp.where(valid & (column == wanted), logits, 0.0), 1)
    logits = jnp.where(valid, logits, NEG)
    top = jnp.max(logits, axis=1, keepdims=True)
    both = top + jnp.log(total(jnp.exp(logits - top), 1))
    down, across = iota((n, 2 * n), 0), iota((n, 2 * n), 1)
    line = jnp.where(across == down, both, 0.0) + jnp.where(across == down + n, found, 0.0)
    out_ref[...] = total(line, 0)


def pair_kernel(mine_ref, theirs_ref, out_ref):
    mine, theirs = mine_ref[...], theirs_ref[...]
    top = jnp.maximum(mine, theirs)
    both = top + jnp.log(jnp.exp(mine - top) + jnp.exp(theirs - top))
    half = iota(mine.shape, 1) < mine.shape[1] // 2
    out_ref[...] = jnp.broadcast_to(jnp.where(half, both, mine + theirs), out_ref.shape)


def join_kernel(found_ref, out_ref):
    n = out_ref.shape[1]
    lines = found_ref[...]
    top = jnp.max(lines, axis=0, keepdims=True)
    both = top + jnp.log(total(jnp.exp(lines - top), 0))
    chosen = total(lines, 0)
    out_ref[...] = chosen[:, n:] - both[:, :n]


def shape(dims, dtype):
    return jax.ShapeDtypeStruct(dims, dtype)


def in_hbm(x):
    return pltpu.with_memory_space_constraint(x, pltpu.HBM)


def exchange(x, axis, groups):
    return lax.all_to_all(
        x, axis, split_axis=0, concat_axis=0, tiled=True, axis_index_groups=groups
    )


def picked(lengths, first, hidden):
    return pl.pallas_call(
        pick_kernel,
        out_shape=(
            shape((DEEP, SLOTS, hidden.shape[1]), hidden.dtype),
            pltpu.SMEM((1, 1), jnp.int32),
            shape((lengths.shape[1], CHIPS * CORES * SLOTS), jnp.bfloat16),
        ),
        in_specs=[HBM] + [SMEM] * len(first) + [HBM],
        out_specs=(VMEM, SMEM, VMEM),
        scratch_shapes=[
            pltpu.VMEM(lengths.shape, lengths.dtype),
            pltpu.VMEM(hidden.shape, hidden.dtype),
            pltpu.SemaphoreType.DMA((2,)),
        ],
        compiler_params=limit(4),
        cost_estimate=pl.CostEstimate(flops=10**10, bytes_accessed=1 << 25, transcendentals=0),
        name="pick",
    )(in_hbm(lengths), *first, in_hbm(hidden))


def spread(rows, gain, after=()):
    chips, cores = CHIPS, CORES
    width = gain.shape[1] // chips
    rows, after = lax.optimization_barrier((exchange(rows, "z", [COLUMN]), after))
    normed = pl.pallas_call(
        norm_kernel,
        out_shape=shape((chips, cores, SLOTS, width), jnp.bfloat16),
        in_specs=[VMEM, VMEM],
        out_specs=VMEM,
        compiler_params=limit(4),
        cost_estimate=pl.CostEstimate(flops=10**10, bytes_accessed=1 << 25, transcendentals=0),
        name="norm",
    )(rows, gain)
    return exchange(normed.reshape(chips * cores * SLOTS, width), "q", [BOTH]), after


def local(hidden, lengths, targets, norm_gain, lm_weight):
    n = lengths.shape[0]
    lengths, targets, gain = lengths[None], targets[None], norm_gain[None]
    weight = lm_weight.T
    vocab, depth = weight.shape
    chips = CHIPS
    half = chips * BLOCK
    start = jnp.zeros((1, 1), jnp.int32)
    rows, some, order = picked(lengths, (), hidden)

    def again(state):
        _, first, more = state
        rows, some, order = picked(lengths, (first,), hidden)
        found = spread(rows, gain)[0]
        first, more = pl.pallas_call(
            order_kernel,
            out_shape=(shape(first.shape, first.dtype), shape(more.shape, more.dtype)),
            in_specs=[VMEM, SMEM, VMEM, VMEM],
            out_specs=(SMEM, VMEM),
            input_output_aliases={1: 0, 3: 1},
            compiler_params=limit(4),
            name="order",
        )(order, first, found, more)
        return some[0, 0], first, more

    _, _, more = lax.while_loop(
        lambda state: state[0] != 0,
        again,
        (some[0, 0], start + SLOTS, jnp.zeros((n, gain.shape[1] // chips), jnp.bfloat16)),
    )
    rows, more, weight = lax.optimization_barrier((rows, more, weight))
    found, weight = spread(rows, gain, weight)
    other = lax.ppermute(weight, "q", PAIRS)
    own = weight
    parts = pl.pallas_call(
        head_kernel,
        out_shape=shape((chips, n, BLOCK), jnp.float32),
        in_specs=[VMEM] * 5,
        out_specs=VMEM,
        compiler_params=limit(16),
        name="head",
    )(order, found, more, own, other)
    logits = jnp.sum(exchange(parts.astype(jnp.float16), "q", EACH).astype(jnp.float32), axis=0)
    line = pl.pallas_call(
        functools.partial(stats_kernel, vocab - half, vocab),
        out_shape=shape((1, 2 * n), jnp.float32),
        in_specs=[VMEM, VMEM],
        out_specs=VMEM,
        compiler_params=limit(4),
        name="stats",
    )(logits, targets)
    return pl.pallas_call(
        pair_kernel,
        out_shape=shape((len(HALVES[0]), 2 * n), jnp.float32),
        in_specs=[VMEM, VMEM],
        out_specs=VMEM,
        compiler_params=limit(4),
        name="pair",
    )(line, lax.ppermute(line, "q", PAIRS))


def joined(line):
    n = line.shape[1] // 2
    out = pl.pallas_call(
        join_kernel,
        out_shape=shape((1, n), jnp.float32),
        in_specs=[VMEM],
        out_specs=VMEM,
        compiler_params=limit(4),
        name="join",
    )(exchange(line, "d", HALVES))
    return out[0]


def solution(mesh):
    devices = mesh.devices.reshape(CHIPS * CORES, DEEP)
    first = jax.shard_map(
        local,
        mesh=Mesh(devices, ("q", "z")),
        in_specs=(P("q", "z"), P(), P(), P(), P("q", "z")),
        out_specs=P(("q", "z")),
        check_vma=False,
    )
    last = jax.shard_map(
        joined,
        mesh=Mesh(devices.reshape(-1), ("d",)),
        in_specs=P("d"),
        out_specs=P(),
        check_vma=False,
    )
    return lambda *args: last(first(*args))
```
